32 devices in a mesh: fsdp: 8 (over y, x, core), tp: 4 (over z).
Axes of the slice: x: 2, y: 2, z: 4, core: 2. Of those that a mesh axis runs over, the one named last changes fastest.
Arguments:
- inputs: float32 [8192, 768], P(('fsdp', 'tp')), may hold values from -6 to 6
- out_cotangent: float32 [8192, 768], P('fsdp'), may hold values from -6 to 6
- clip_lengths: int32 [6], replicated, may hold values from 384 to 1536, as said below
- norm1_gain: float32 [768], replicated, may hold values from 0.5 to 1.5
- norm1_shift: float32 [768], replicated, may hold values from -3 to 3
- query_weight: bfloat16 [768, 768], P('fsdp', 'tp'), may hold values from -0.21875 to 0.21875
- query_bias: float32 [768], replicated, may hold values from -3 to 3
- key_weight: bfloat16 [768, 768], P('fsdp', 'tp'), may hold values from -0.21875 to 0.21875
- value_weight: bfloat16 [768, 768], P('fsdp', 'tp'), may hold values from -0.21875 to 0.21875
- value_bias: float32 [768], replicated, may hold values from -3 to 3
- out_weight: bfloat16 [768, 768], P('fsdp', 'tp'), may hold values from -0.75 to 0.75
- out_bias: float32 [768], replicated, may hold values from -3 to 3
- norm2_gain: float32 [768], replicated, may hold values from 0.5 to 1.5
- norm2_shift: float32 [768], replicated, may hold values from -3 to 3
- fc1_weight: bfloat16 [3072, 768], P(('fsdp', 'tp')), may hold values from -0.21875 to 0.21875
- fc1_bias: float32 [3072], replicated, may hold values from -3 to 3
- fc2_weight: bfloat16 [3072, 768], P(('fsdp', 'tp')), may hold values from -0.3125 to 0.3125
- fc2_bias: float32 [768], replicated, may hold values from -3 to 3
Outputs:
- outputs: float32 [8192, 768], P(('fsdp', 'tp'))
- inputs_grad: float32 [8192, 768], P(('fsdp', 'tp'))
- norm1_gain_grad: float32 [768], replicated
- norm1_shift_grad: float32 [768], replicated
- query_weight_grad: float32 [768, 768], P('fsdp', 'tp')
- query_bias_grad: float32 [768], replicated
- key_weight_grad: float32 [768, 768], P('fsdp', 'tp')
- value_weight_grad: float32 [768, 768], P('fsdp', 'tp')
- value_bias_grad: float32 [768], replicated
- out_weight_grad: float32 [768, 768], P('fsdp', 'tp')
- out_bias_grad: float32 [768], replicated
- norm2_gain_grad: float32 [768], replicated
- norm2_shift_grad: float32 [768], replicated
- fc1_weight_grad: float32 [3072, 768], P(('fsdp', 'tp'))
- fc1_bias_grad: float32 [3072], replicated
- fc2_weight_grad: float32 [3072, 768], P(('fsdp', 'tp'))
- fc2_bias_grad: float32 [768], replicated
The draws below stay inside these ranges and needn't reach their ends.
Inputs may be any that keep to these rules, and one draw needn't show every extreme that they name: `clip_lengths`: clip c has at most min(1536, 8192 - c * 1536) valid frames; some clip has all 1536 frames valid.
All inputs are finite; a program needn't handle non-finite values.
Results may differ from the reference program's by a relative error of at most 0.03.
Values may be sent and summed in bfloat16 or wider, within the bound.
A program may use at most 128 MiB of HBM per device.

```python
import math
import jax
import jax.numpy as jnp
from jax import lax

D = 768
HEADS = 12
HD = 64
FF = 3072
TOK_DEV = 1024
CLIP = 1536
TOKENS = 8192
CLIPS = 6


def draw_clip_lengths(key, part):
    drawn = jax.random.randint(jax.random.fold_in(key, 21), (CLIPS,), CLIP // 4, CLIP + 1)
    complete = jax.random.randint(jax.random.fold_in(key, 22), (), 0, CLIPS - 1)
    drawn = jnp.where(jnp.arange(CLIPS) == complete, CLIP, drawn)
    room = TOKENS - jnp.arange(CLIPS) * CLIP
    return jnp.minimum(drawn, room).astype(jnp.int32)


def levels(own_key, extent, split, least, high):
    def one(axis_at, shards_of):
        heights = jax.random.uniform(jax.random.fold_in(jax.random.fold_in(own_key, 6), axis_at), (shards_of,), jnp.float32, least / len(split), high / len(split))
        return jnp.repeat(jnp.exp(heights), extent[axis_at] // shards_of).reshape((-1,) + (1,) * (len(extent) - axis_at - 1))

    factor_of = one(*split[0])
    for cut in split[1:]:
        factor_of = factor_of * one(*cut)
    return factor_of


def noise(stream_key, dims, scale, most, pieces=(), kind=jnp.bfloat16):
    values = scale * jax.random.normal(stream_key, dims, jnp.float32)
    if pieces:
        values = values * levels(stream_key, dims, pieces, -0.22, 0.18)
    return jnp.clip(values, -most, most).astype(kind)


def setup_inputs(seed: int = 0) -> dict:
    key_list = jax.random.split(jax.random.key(seed), 19)
    return {
        "inputs": noise(key_list[0], (TOKENS, D), 1.0, 6.0, ((0, 32),), jnp.float32),
        "out_cotangent": noise(key_list[1], (TOKENS, D), 1.0, 6.0, ((0, 8),), jnp.float32),
        "clip_lengths": draw_clip_lengths(jax.random.fold_in(key_list[18], 71), 0),
        "norm1_gain": jnp.clip(1.0 + 0.1 * jax.random.normal(key_list[3], (D,), jnp.float32), 0.5, 1.5),
        "norm1_shift": noise(key_list[4], (D,), 0.5, 3.0, (), jnp.float32),
        "query_weight": noise(key_list[5], (D, D), D ** -0.5, 0.21875, ((0, 8), (1, 4))),
        "query_bias": noise(key_list[6], (D,), 0.5, 3.0, (), jnp.float32),
        "key_weight": noise(key_list[7], (D, D), D ** -0.5, 0.21875, ((0, 8), (1, 4))),
        "value_weight": noise(key_list[8], (D, D), D ** -0.5, 0.21875, ((0, 8), (1, 4))),
        "value_bias": noise(key_list[9], (D,), 0.5, 3.0, (), jnp.float32),
        "out_weight": noise(key_list[10], (D, D), HD ** -0.5, 0.75, ((0, 8), (1, 4))),
        "out_bias": noise(key_list[11], (D,), 0.5, 3.0, (), jnp.float32),
        "norm2_gain": jnp.clip(1.0 + 0.1 * jax.random.normal(key_list[12], (D,), jnp.float32), 0.5, 1.5),
        "norm2_shift": noise(key_list[13], (D,), 0.5, 3.0, (), jnp.float32),
        "fc1_weight": noise(key_list[14], (FF, D), D ** -0.5, 0.21875, ((0, 32),)),
        "fc1_bias": noise(key_list[15], (FF,), 0.5, 3.0, (), jnp.float32),
        "fc2_weight": noise(key_list[16], (FF, D), (FF // 8) ** -0.5, 0.3125, ((0, 32),)),
        "fc2_bias": noise(key_list[17], (D,), 0.5, 3.0, (), jnp.float32),
    }


eps_norm = 1e-05
root_half = 0.7071067811865476
inv_root_tau = 0.3989422804014327
far_negative = -1e+30

def widen(values):
    return lax.optimization_barrier(values).astype(jnp.float32)

def normalize(rows, gain, shift):
    centre = lax.optimization_barrier(jnp.mean(rows, axis=-1, keepdims=True))
    centred = rows - centre
    inv_spread = lax.rsqrt(lax.optimization_barrier(jnp.mean(centred * centred, axis=-1, keepdims=True)) + eps_norm)
    unit_rows = centred * inv_spread
    return (unit_rows, inv_spread, unit_rows * gain + shift)

def norm_back(upstream, unit_rows, inv_spread, gain):
    scaled = upstream * gain
    return inv_spread * (scaled - lax.optimization_barrier(jnp.mean(scaled, axis=-1, keepdims=True)) - unit_rows * lax.optimization_barrier(jnp.mean(scaled * unit_rows, axis=-1, keepdims=True)))

def gelu_exact(values):
    return 0.5 * values * (1.0 + lax.erf(values * root_half))

def gelu_slope(values):
    return 0.5 * (1.0 + lax.erf(values * root_half)) + values * jnp.exp(-0.5 * values * values) * inv_root_tau

def clip_scores(query_clip, key_clip, length):
    score_scale = 1.0 / math.sqrt(HD)
    queries = widen(query_clip).reshape(CLIP, HEADS, HD)
    keys = widen(key_clip).reshape(CLIP, HEADS, HD)
    scores = jnp.einsum('qhe,khe->hqk', queries, keys) * score_scale
    valid = jnp.arange(CLIP) < length
    return jnp.where(valid[None, None, :], scores, far_negative)

def clip_forward(item):
    query_clip, key_clip, value_clip, length = item
    scores = clip_scores(query_clip, key_clip, length)
    highest = lax.optimization_barrier(jnp.max(scores, axis=-1, keepdims=True))
    log_total = highest[..., 0] + jnp.log(lax.optimization_barrier(jnp.sum(jnp.exp(scores - highest), axis=-1)))
    weights = widen(jnp.exp(scores - log_total[..., None]).astype(jnp.bfloat16))
    values = widen(value_clip).reshape(CLIP, HEADS, HD)
    context = jnp.einsum('hqk,khe->qhe', weights, values)
    return (context.reshape(CLIP, D).astype(jnp.bfloat16), log_total)

def clip_backward(item):
    query_clip, key_clip, value_clip, context_clip, grad_clip, log_total, length = item
    score_scale = 1.0 / math.sqrt(HD)
    scores = clip_scores(query_clip, key_clip, length)
    probs = jnp.exp(scores - log_total[..., None])
    queries = widen(query_clip).reshape(CLIP, HEADS, HD)
    keys = widen(key_clip).reshape(CLIP, HEADS, HD)
    values = widen(value_clip).reshape(CLIP, HEADS, HD)
    grads = widen(grad_clip).reshape(CLIP, HEADS, HD)
    delta = lax.optimization_barrier(jnp.sum(grads * widen(context_clip).reshape(CLIP, HEADS, HD), axis=-1)).T
    dprobs = jnp.einsum('qhe,khe->hqk', grads, values)
    dscores = widen((probs * (dprobs - delta[..., None]) * score_scale).astype(jnp.bfloat16))
    dquery = jnp.einsum('hqk,khe->qhe', dscores, keys).reshape(CLIP, D).astype(jnp.bfloat16)
    dkey = jnp.einsum('hqk,qhe->khe', dscores, queries).reshape(CLIP, D).astype(jnp.bfloat16)
    weights = widen(probs.astype(jnp.bfloat16))
    dvalue = jnp.einsum('hqk,qhe->khe', weights, grads).reshape(CLIP, D).astype(jnp.bfloat16)
    return (dquery, dkey, dvalue)

def reference(inputs, out_cotangent, clip_lengths, norm1_gain, norm1_shift, query_weight, query_bias, key_weight, value_weight, value_bias, out_weight, out_bias, norm2_gain, norm2_shift, fc1_weight, fc1_bias, fc2_weight, fc2_bias):
    bf16 = jnp.bfloat16
    f32 = jnp.float32
    unit1, spread1, normed_full = normalize(inputs, norm1_gain, norm1_shift)
    normed = normed_full.astype(bf16)
    query = (jnp.dot(normed, query_weight, preferred_element_type=f32) + query_bias).astype(bf16)
    key = jnp.dot(normed, key_weight, preferred_element_type=f32).astype(bf16)
    value = (jnp.dot(normed, value_weight, preferred_element_type=f32) + value_bias).astype(bf16)
    padding = CLIPS * CLIP - TOKENS

    def by_clip(rows):
        return jnp.pad(rows, ((0, padding), (0, 0))).reshape(CLIPS, CLIP, D)

    def by_row(clips):
        return clips.reshape(CLIPS * CLIP, D)[:TOKENS]
    context_clips, totals = lax.map(clip_forward, (by_clip(query), by_clip(key), by_clip(value), clip_lengths))
    context = by_row(context_clips)
    hidden = inputs + jnp.dot(context, out_weight.T, preferred_element_type=f32) + out_bias
    unit2, spread2, normed2_full = normalize(hidden, norm2_gain, norm2_shift)
    normed2 = normed2_full.astype(bf16)

    def mlp_block(carry, item):
        grad_up, grad_down, grad_upbias = carry
        rows, upstream = item
        preact = jnp.dot(rows, fc1_weight.T, preferred_element_type=f32) + fc1_bias
        activated = gelu_exact(preact).astype(bf16)
        mixed = jnp.dot(activated, fc2_weight, preferred_element_type=f32)
        up_rounded = upstream.astype(bf16)
        dactivated = jnp.dot(up_rounded, fc2_weight.T, preferred_element_type=f32)
        dpreact = (dactivated * gelu_slope(preact)).astype(bf16)
        grad_down = grad_down + jnp.dot(activated.T, up_rounded, preferred_element_type=f32)
        grad_up = grad_up + jnp.dot(dpreact.T, rows, preferred_element_type=f32)
        grad_upbias = grad_upbias + lax.optimization_barrier(jnp.sum(dpreact.astype(f32), axis=0))
        drows = jnp.dot(dpreact, fc1_weight, preferred_element_type=f32)
        return ((grad_up, grad_down, grad_upbias), (mixed, drows))
    zero_matrix = jnp.zeros((FF, D), f32)
    (grad_fc1, grad_fc2, grad_b1), (mixed_rows, dnorm_rows) = lax.scan(mlp_block, (zero_matrix, zero_matrix, jnp.zeros((FF,), f32)), (normed2.reshape(-1, TOK_DEV, D), out_cotangent.reshape(-1, TOK_DEV, D)))
    outputs = hidden + mixed_rows.reshape(TOKENS, D) + fc2_bias
    grad_b2 = lax.optimization_barrier(jnp.sum(out_cotangent, axis=0))
    dnorm2 = dnorm_rows.reshape(TOKENS, D)
    grad_gain2 = lax.optimization_barrier(jnp.sum(dnorm2 * unit2, axis=0))
    grad_shift2 = lax.optimization_barrier(jnp.sum(dnorm2, axis=0))
    dhidden = out_cotangent + norm_back(dnorm2, unit2, spread2, norm2_gain)
    dh_rounded = dhidden.astype(bf16)
    grad_out = jnp.dot(dh_rounded.T, context, preferred_element_type=f32)
    grad_obias = lax.optimization_barrier(jnp.sum(dhidden, axis=0))
    dcontext = jnp.dot(dh_rounded, out_weight, preferred_element_type=f32).astype(bf16)
    dq_clips, dk_clips, dv_clips = lax.map(clip_backward, (by_clip(query), by_clip(key), by_clip(value), by_clip(context), by_clip(dcontext), totals, clip_lengths))
    dquery = by_row(dq_clips)
    dkey = by_row(dk_clips)
    dvalue = by_row(dv_clips)
    grad_query = jnp.dot(normed.T, dquery, preferred_element_type=f32)
    grad_key = jnp.dot(normed.T, dkey, preferred_element_type=f32)
    grad_value = jnp.dot(normed.T, dvalue, preferred_element_type=f32)
    grad_qbias = lax.optimization_barrier(jnp.sum(dquery.astype(f32), axis=0))
    grad_vbias = lax.optimization_barrier(jnp.sum(dvalue.astype(f32), axis=0))
    dnorm1 = jnp.dot(dquery, query_weight.T, preferred_element_type=f32) + jnp.dot(dkey, key_weight.T, preferred_element_type=f32) + jnp.dot(dvalue, value_weight.T, preferred_element_type=f32)
    grad_gain1 = lax.optimization_barrier(jnp.sum(dnorm1 * unit1, axis=0))
    grad_shift1 = lax.optimization_barrier(jnp.sum(dnorm1, axis=0))
    inputs_grad = dhidden + norm_back(dnorm1, unit1, spread1, norm1_gain)
    return (outputs, inputs_grad, grad_gain1, grad_shift1, grad_query, grad_qbias, grad_key, grad_value, grad_vbias, grad_out, grad_obias, grad_gain2, grad_shift2, grad_fc1, grad_b1, grad_fc2, grad_b2)
```

```python
import math

import jax
import jax.numpy as jnp
from jax import lax
from jax.sharding import PartitionSpec as P

HD = 64
CLIP = 1536
QB = 512


eps_norm = 1e-05
root_half = 0.7071067811865476
inv_root_tau = 0.3989422804014327
far_negative = -1e30


def extended(value, sides, width):
    for axis, dim in sides:
        size, length = (lax.axis_size(axis), value.shape[dim])
        up = [(i, (i + 1) % size) for i in range(size - 1)]
        down = [(j, i) for i, j in up]
        last = lax.slice_in_dim(value, length - width, length, axis=dim)
        initial = lax.slice_in_dim(value, 0, width, axis=dim)
        before = lax.ppermute(last, axis, up)
        after = lax.ppermute(initial, axis, down)
        value = jnp.concatenate([before, value, after], axis=dim)
    return value


def normalize(rows, gain, shift):
    centre = jnp.mean(rows, axis=-1, keepdims=True)
    centred = rows - centre
    inv_spread = lax.rsqrt(jnp.mean(centred * centred, axis=-1, keepdims=True) + eps_norm)
    unit_rows = centred * inv_spread
    return (unit_rows, inv_spread, unit_rows * gain + shift)


def norm_back(upstream, unit_rows, inv_spread, gain):
    scaled = upstream * gain
    return inv_spread * (
        scaled
        - jnp.mean(scaled, axis=-1, keepdims=True)
        - unit_rows * jnp.mean(scaled * unit_rows, axis=-1, keepdims=True)
    )


def gelu_exact(values):
    return 0.5 * values * (1.0 + lax.erf(values * root_half))


def gelu_slope(values):
    return (
        0.5 * (1.0 + lax.erf(values * root_half))
        + values * jnp.exp(-0.5 * values * values) * inv_root_tau
    )


def contract_rows(left_rows, right_rows):
    return lax.dot_general(
        left_rows, right_rows, (((0,), (0,)), ((), ())), preferred_element_type=jnp.float32
    )


def contract_cols(left_rows, right_rows):
    return lax.dot_general(
        left_rows, right_rows, (((1,), (1,)), ((), ())), preferred_element_type=jnp.float32
    )


def fetch_attention(query_weight, key_weight, value_weight, out_weight):
    joined = jnp.concatenate([query_weight, key_weight, value_weight, out_weight], axis=1)
    return jnp.split(lax.all_gather(joined, "fsdp", axis=0, tiled=True), 4, axis=1)


def scatter_rows(partial_rows, axis):
    return lax.psum_scatter(
        partial_rows.astype(jnp.bfloat16), axis, scatter_dimension=0, tiled=True
    ).astype(jnp.float32)


def on_device(
    inputs,
    out_cotangent,
    clip_lengths,
    norm1_gain,
    norm1_shift,
    query_weight,
    query_bias,
    key_weight,
    value_weight,
    value_bias,
    out_weight,
    out_bias,
    norm2_gain,
    norm2_shift,
    fc1_weight,
    fc1_bias,
    fc2_weight,
    fc2_bias,
):
    bf16 = jnp.bfloat16
    f32 = jnp.float32
    tp_count = lax.axis_size("tp")
    fsdp_count = lax.axis_size("fsdp")
    tp_index = lax.axis_index("tp")
    fsdp_index = lax.axis_index("fsdp")
    own_rows = inputs.shape[0]
    group_rows = out_cotangent.shape[0]
    score_scale = 1.0 / math.sqrt(HD)
    margin = CLIP - QB
    tp_slot = (jnp.arange(tp_count) == tp_index).astype(f32)
    own_cotangent = lax.dynamic_slice_in_dim(out_cotangent, tp_index * own_rows, own_rows, 0)
    unit1, spread1, normed_own = normalize(inputs, norm1_gain, norm1_shift)
    normed = lax.all_gather(normed_own.astype(bf16), "tp", axis=0, tiled=True)
    query_w, key_w, value_w, out_w = fetch_attention(
        query_weight, key_weight, value_weight, out_weight
    )
    local_width = query_w.shape[1]
    heads_here = local_width // HD
    column_start = tp_index * local_width
    query = (
        jnp.dot(normed, query_w, preferred_element_type=f32)
        + lax.dynamic_slice_in_dim(query_bias, column_start, local_width, 0)
    ).astype(bf16)
    key = jnp.dot(normed, key_w, preferred_element_type=f32).astype(bf16)
    value = (
        jnp.dot(normed, value_w, preferred_element_type=f32)
        + lax.dynamic_slice_in_dim(value_bias, column_start, local_width, 0)
    ).astype(bf16)
    padded = extended(jnp.stack([key, value]), (("fsdp", 1),), margin)
    group_base = fsdp_index * group_rows
    clip_ids = jnp.arange(clip_lengths.shape[0])
    block_count = group_rows // QB

    def block_scores(block_index):
        first_row = block_index * QB
        clip_index = (group_base + first_row) // CLIP
        key_start = clip_index * CLIP - group_base + margin
        length = jnp.sum(jnp.where(clip_ids == clip_index, clip_lengths, 0))
        query_block = lax.dynamic_slice_in_dim(query, first_row, QB, 0).reshape(QB, heads_here, HD)
        pair = lax.dynamic_slice_in_dim(padded, key_start, CLIP, 1).reshape(2, CLIP, heads_here, HD)
        scores = (
            jnp.einsum("qhe,khe->hqk", query_block, pair[0], preferred_element_type=f32)
            * score_scale
        )
        scores = jnp.where((jnp.arange(CLIP) < length)[None, None, :], scores, far_negative)
        return (first_row, key_start, query_block, pair[0], pair[1], scores)

    def attend(block_index, carry):
        context_rows, total_rows = carry
        first_row, key_start, query_block, key_block, value_block, scores = block_scores(
            block_index
        )
        highest = jnp.max(scores, axis=-1, keepdims=True)
        log_total = highest[..., 0] + jnp.log(jnp.sum(jnp.exp(scores - highest), axis=-1))
        weights = jnp.exp(scores - log_total[..., None]).astype(bf16)
        block_out = jnp.einsum("hqk,khe->qhe", weights, value_block, preferred_element_type=f32)
        block_out = block_out.astype(bf16).reshape(QB, local_width)
        context_rows = lax.dynamic_update_slice_in_dim(context_rows, block_out, first_row, 0)
        total_rows = lax.dynamic_update_slice_in_dim(total_rows, log_total, first_row, 1)
        return (context_rows, total_rows)

    context, totals = lax.fori_loop(
        0,
        block_count,
        attend,
        (jnp.zeros((group_rows, local_width), bf16), jnp.zeros((heads_here, group_rows), f32)),
    )
    attended = scatter_rows(contract_cols(context, out_w), "tp")
    hidden = inputs + attended + out_bias
    unit2, spread2, normed2_full = normalize(hidden, norm2_gain, norm2_shift)
    normed2_own = normed2_full.astype(bf16)
    normed2 = lax.all_gather(normed2_own, "tp", axis=0, tiled=True)
    w_up, w_down = jnp.split(
        lax.all_gather(
            jnp.concatenate([fc1_weight, fc2_weight], axis=1), "fsdp", axis=0, tiled=True
        ),
        2,
        axis=1,
    )
    unit_count = fc1_weight.shape[0]
    bias_up = lax.dynamic_index_in_dim(
        fc1_bias.reshape(fsdp_count, tp_count, unit_count), tp_index, 1, False
    ).reshape(-1)
    preact = contract_cols(normed2, w_up) + bias_up
    activated = gelu_exact(preact).astype(bf16)
    mixed = scatter_rows(jnp.dot(activated, w_down, preferred_element_type=f32), "tp")
    outputs = hidden + mixed + fc2_bias
    up_rounded = out_cotangent.astype(bf16)
    dactivated = contract_cols(up_rounded, w_down)
    dpreact = (dactivated * gelu_slope(preact)).astype(bf16)
    grad_up_part = contract_rows(dpreact, normed2)
    grad_down_part = contract_rows(activated, up_rounded)
    upbias_part = jnp.sum(dpreact.astype(f32), axis=0)
    grad_b1 = (upbias_part.reshape(fsdp_count, 1, unit_count) * tp_slot[None, :, None]).reshape(-1)
    dnorm2 = scatter_rows(jnp.dot(dpreact, w_up, preferred_element_type=f32), "tp")
    grad_fc1, grad_fc2 = jnp.split(
        scatter_rows(jnp.concatenate([grad_up_part, grad_down_part], axis=1), "fsdp"), 2, axis=1
    )
    grad_b2 = jnp.sum(own_cotangent, axis=0)
    grad_gain2 = jnp.sum(dnorm2 * unit2, axis=0)
    grad_shift2 = jnp.sum(dnorm2, axis=0)
    dhidden = own_cotangent + norm_back(dnorm2, unit2, spread2, norm2_gain)
    grad_obias = jnp.sum(dhidden, axis=0)
    dh_all = lax.all_gather(dhidden.astype(bf16), "tp", axis=0, tiled=True)
    dcontext = jnp.dot(dh_all, out_w, preferred_element_type=f32).astype(bf16)
    grad_out = contract_rows(dh_all, context)
    delta = jnp.sum(
        (dcontext.astype(f32) * context.astype(f32)).reshape(group_rows, heads_here, HD), axis=-1
    ).T

    def attend_back(block_index, carry):
        dquery_rows, dpair = carry
        first_row, key_start, query_block, key_block, value_block, scores = block_scores(
            block_index
        )
        grad_block = lax.dynamic_slice_in_dim(dcontext, first_row, QB, 0).reshape(
            QB, heads_here, HD
        )
        probs = jnp.exp(scores - lax.dynamic_slice_in_dim(totals, first_row, QB, 1)[..., None])
        delta_block = lax.dynamic_slice_in_dim(delta, first_row, QB, 1)
        dprobs = jnp.einsum("qhe,khe->hqk", grad_block, value_block, preferred_element_type=f32)
        dscores = (probs * (dprobs - delta_block[..., None]) * score_scale).astype(bf16)
        dquery_block = jnp.einsum("hqk,khe->qhe", dscores, key_block, preferred_element_type=f32)
        dquery_block = dquery_block.astype(bf16).reshape(QB, local_width)
        dkey_block = jnp.einsum(
            "hqk,qhe->khe", dscores, query_block, preferred_element_type=f32
        ).reshape(CLIP, local_width)
        dvalue_block = jnp.einsum(
            "hqk,qhe->khe", probs.astype(bf16), grad_block, preferred_element_type=f32
        ).reshape(CLIP, local_width)
        current = lax.dynamic_slice_in_dim(dpair, key_start, CLIP, 1)
        dpair = lax.dynamic_update_slice_in_dim(
            dpair, current + jnp.stack([dkey_block, dvalue_block]), key_start, 1
        )
        dquery_rows = lax.dynamic_update_slice_in_dim(dquery_rows, dquery_block, first_row, 0)
        return (dquery_rows, dpair)

    dquery, dpair = lax.fori_loop(
        0,
        block_count,
        attend_back,
        (jnp.zeros((group_rows, local_width), bf16), jnp.zeros(padded.shape, f32)),
    )
    rims = jnp.concatenate([dpair[:, :margin], dpair[:, margin + group_rows :]], axis=1)
    received = extended(rims, (("fsdp", 1),), margin)
    inner_part = dpair[:, margin : margin + group_rows]
    inner_part = inner_part.at[:, :margin].add(received[:, :margin])
    inner_part = inner_part.at[:, group_rows - margin :].add(received[:, 3 * margin :])
    dkey = inner_part[0].astype(bf16)
    dvalue = inner_part[1].astype(bf16)
    grad_query = contract_rows(normed, dquery)
    grad_key = contract_rows(normed, dkey)
    grad_value = contract_rows(normed, dvalue)
    grad_qbias = (tp_slot[:, None] * jnp.sum(dquery.astype(f32), axis=0)[None, :]).reshape(-1)
    grad_vbias = (tp_slot[:, None] * jnp.sum(dvalue.astype(f32), axis=0)[None, :]).reshape(-1)
    dnorm1 = scatter_rows(
        contract_cols(dquery, query_w)
        + contract_cols(dkey, key_w)
        + contract_cols(dvalue, value_w),
        "tp",
    )
    grad_gain1 = jnp.sum(dnorm1 * unit1, axis=0)
    grad_shift1 = jnp.sum(dnorm1, axis=0)
    inputs_grad = dhidden + norm_back(dnorm1, unit1, spread1, norm1_gain)
    grad_query, grad_key, grad_value, grad_out = jnp.split(
        scatter_rows(
            jnp.concatenate([grad_query, grad_key, grad_value, grad_out], axis=1), "fsdp"
        ),
        4,
        axis=1,
    )
    (
        grad_gain1,
        grad_shift1,
        grad_qbias,
        grad_vbias,
        grad_obias,
        grad_gain2,
        grad_shift2,
        grad_b1,
        grad_b2,
    ) = lax.psum(
        (
            grad_gain1,
            grad_shift1,
            grad_qbias,
            grad_vbias,
            grad_obias,
            grad_gain2,
            grad_shift2,
            grad_b1,
            grad_b2,
        ),
        ("fsdp", "tp"),
    )
    return (
        outputs,
        inputs_grad,
        grad_gain1,
        grad_shift1,
        grad_query,
        grad_qbias,
        grad_key,
        grad_value,
        grad_vbias,
        grad_out,
        grad_obias,
        grad_gain2,
        grad_shift2,
        grad_fc1,
        grad_b1,
        grad_fc2,
        grad_b2,
    )


def solution(mesh):
    in_specs = (
        P(("fsdp", "tp"), None),
        P("fsdp", None),
        P(),
        P(),
        P(),
        P("fsdp", "tp"),
        P(),
        P("fsdp", "tp"),
        P("fsdp", "tp"),
        P(),
        P("fsdp", "tp"),
        P(),
        P(),
        P(),
        P(("fsdp", "tp"), None),
        P(),
        P(("fsdp", "tp"), None),
        P(),
    )
    out_specs = (
        P(("fsdp", "tp"), None),
        P(("fsdp", "tp"), None),
        P(),
        P(),
        P("fsdp", "tp"),
        P(),
        P("fsdp", "tp"),
        P("fsdp", "tp"),
        P(),
        P("fsdp", "tp"),
        P(),
        P(),
        P(),
        P(("fsdp", "tp"), None),
        P(),
        P(("fsdp", "tp"), None),
        P(),
    )
    return jax.shard_map(
        on_device, mesh=mesh, in_specs=in_specs, out_specs=out_specs, check_vma=False
    )
```

```python
import functools
import math

import jax
import jax.numpy as jnp
from jax import lax
from jax.experimental import pallas as pl
from jax.experimental.pallas import tpu as pltpu
from jax.sharding import PartitionSpec as P

HD = 64
CLIP = 1536
QB = 512


eps_norm = 1e-05
root_half = 0.7071067811865476
inv_root_tau = 0.3989422804014327
far_negative = -1e30


def extended(value, sides, width):
    for axis, dim in sides:
        size, length = (lax.axis_size(axis), value.shape[dim])
        up = [(i, (i + 1) % size) for i in range(size - 1)]
        down = [(j, i) for i, j in up]
        last = lax.slice_in_dim(value, length - width, length, axis=dim)
        initial = lax.slice_in_dim(value, 0, width, axis=dim)
        before = lax.ppermute(last, axis, up)
        after = lax.ppermute(initial, axis, down)
        value = jnp.concatenate([before, value, after], axis=dim)
    return value


def normalize(rows, gain, shift):
    centre = jnp.mean(rows, axis=-1, keepdims=True)
    centred = rows - centre
    inv_spread = lax.rsqrt(jnp.mean(centred * centred, axis=-1, keepdims=True) + eps_norm)
    unit_rows = centred * inv_spread
    return (unit_rows, inv_spread, unit_rows * gain + shift)


def norm_back(upstream, unit_rows, inv_spread, gain):
    scaled = upstream * gain
    return inv_spread * (
        scaled
        - jnp.mean(scaled, axis=-1, keepdims=True)
        - unit_rows * jnp.mean(scaled * unit_rows, axis=-1, keepdims=True)
    )


def gelu_exact(values):
    return 0.5 * values * (1.0 + lax.erf(values * root_half))


def gelu_slope(values):
    return (
        0.5 * (1.0 + lax.erf(values * root_half))
        + values * jnp.exp(-0.5 * values * values) * inv_root_tau
    )


def contract_rows(left_rows, right_rows):
    return lax.dot_general(
        left_rows, right_rows, (((0,), (0,)), ((), ())), preferred_element_type=jnp.float32
    )


def contract_cols(left_rows, right_rows):
    return lax.dot_general(
        left_rows, right_rows, (((1,), (1,)), ((), ())), preferred_element_type=jnp.float32
    )


def scatter_rows(partial_rows, axis):
    return lax.psum_scatter(
        partial_rows.astype(jnp.bfloat16), axis, scatter_dimension=0, tiled=True
    ).astype(jnp.float32)


MESH = pl.DeviceIdType.MESH
VMEM_LIMIT = 60 * 1024 * 1024


def remote(source, target, send_sem, recv_sem, fsdp_to, tp_to):
    return pltpu.make_async_remote_copy(
        src_ref=source,
        dst_ref=target,
        send_sem=send_sem,
        recv_sem=recv_sem,
        device_id=(fsdp_to, tp_to),
        device_id_type=MESH,
    )


def greet(fsdp_count, tp_count, f, t):
    barrier = pltpu.get_barrier_semaphore()

    def greet_fsdp(i, carry):
        pl.semaphore_signal(
            barrier, inc=1, device_id=(lax.rem(f + i, fsdp_count), t), device_id_type=MESH
        )
        return carry

    def greet_tp(j, carry):
        pl.semaphore_signal(
            barrier, inc=1, device_id=(f, lax.rem(t + j, tp_count)), device_id_type=MESH
        )
        return carry

    lax.fori_loop(1, fsdp_count, greet_fsdp, 0)
    lax.fori_loop(1, tp_count, greet_tp, 0)
    pl.semaphore_wait(barrier, fsdp_count + tp_count - 2)


def halo_plan(f, fsdp_count):
    phase = lax.rem(f, 3)
    above = f + 1 < fsdp_count
    below = f > 0
    sends = (
        (f + 1, 0, above & (phase == 0)),
        (f + 1, 1, above & (phase < 2)),
        (f - 1, 0, below & (phase > 0)),
        (f - 1, 1, below & (phase == 2)),
    )
    receives = (
        below & (phase == 1),
        below & (phase > 0),
        above & (phase < 2),
        above & (phase == 1),
    )
    return (sends, receives)


def project_kernel(
    fsdp_count,
    tp_count,
    x_ref,
    gain_ref,
    shift_ref,
    weight_ref,
    bias_ref,
    query_ref,
    pair_ref,
    normed_ref,
    full_ref,
    weight_send,
    weight_recv,
    row_send,
    row_recv,
    halo_send,
    halo_recv,
):
    f = lax.axis_index("fsdp")
    t = lax.axis_index("tp")
    rows = x_ref.shape[0]
    depth = weight_ref.shape[0]
    group = rows * tp_count
    width = query_ref.shape[1]
    margin = (pair_ref.shape[0] - group) // 2
    blank = jnp.zeros((256, 2 * width), jnp.bfloat16)

    def clear(i, carry):
        pair_ref[pl.ds(i * 256, 256), :] = blank
        pair_ref[pl.ds(margin + group + i * 256, 256), :] = blank
        return carry

    lax.fori_loop(0, margin // 256, clear, 0)
    greet(fsdp_count, tp_count, f, t)

    def weight_copy(i):
        return remote(
            weight_ref,
            full_ref.at[pl.ds(f * depth, depth)],
            weight_send.at[i],
            weight_recv.at[i],
            lax.rem(f + i, fsdp_count),
            t,
        )

    def weight_start(i, carry):
        weight_copy(i).start()
        return carry

    def weight_done(i, carry):
        weight_copy(i).wait_send()
        source = lax.rem(f + fsdp_count - i, fsdp_count)
        remote(
            weight_ref,
            full_ref.at[pl.ds(source * depth, depth)],
            weight_send.at[i],
            weight_recv.at[i],
            source,
            t,
        ).wait_recv()
        return carry

    _, _, normed = normalize(x_ref[...], gain_ref[...], shift_ref[...])
    normed_ref[t] = normed.astype(jnp.bfloat16)

    def row_copy(source, lane, toward):
        return remote(
            normed_ref.at[source],
            normed_ref.at[source],
            row_send.at[lane],
            row_recv.at[source],
            f,
            toward,
        )

    @pl.when(t > 0)
    def _():
        row_copy(t, tp_count, t - 1).start()

    @pl.when(t < tp_count - 1)
    def _():
        row_copy(t, tp_count + 1, t + 1).start()

    lax.fori_loop(1, fsdp_count, weight_start, 0)
    full_ref[pl.ds(f * depth, depth), :] = weight_ref[...]
    lax.fori_loop(1, fsdp_count, weight_done, 0)

    def compute(source):
        out = jnp.dot(normed_ref[source], full_ref[...], preferred_element_type=jnp.float32)
        out = (out + bias_ref[t]).astype(jnp.bfloat16)
        pair_ref[pl.ds(margin + source * rows, rows), :] = out[:, : 2 * width]
        query_ref[pl.ds(source * rows, rows), :] = out[:, 2 * width :]

    compute(t)

    def arrival(k):
        step = k // 2 + 1
        side = 2 * lax.rem(k, 2) - 1
        source = t + side * step
        onward = t - side
        valid = (source >= 0) & (source < tp_count)
        return (source, onward, valid, valid & (onward >= 0) & (onward < tp_count))

    def receive(k, carry):
        source, onward, valid, forward = arrival(k)

        @pl.when(valid)
        def _():
            row_copy(source, 0, t).wait_recv()

            @pl.when(forward)
            def _():
                row_copy(source, source, onward).start()

            compute(source)

        return carry

    lax.fori_loop(0, 2 * (tp_count - 1), receive, 0)

    sends, receives = halo_plan(f, fsdp_count)
    half = group // 2
    for lane, (toward, part, needed) in enumerate(sends):
        target = (margin + group if lane >= 2 else 0) + part * half

        @pl.when(needed)
        def _(lane=lane, toward=toward, part=part, target=target):
            remote(
                pair_ref.at[pl.ds(margin + part * half, half)],
                pair_ref.at[pl.ds(target, half)],
                halo_send.at[lane],
                halo_recv.at[lane],
                toward,
                t,
            ).start()

    def sent(k, carry):
        source, onward, valid, forward = arrival(k)

        @pl.when(forward)
        def _():
            row_copy(source, source, onward).wait_send()

        return carry

    lax.fori_loop(0, 2 * (tp_count - 1), sent, 0)

    @pl.when(t > 0)
    def _():
        row_copy(t, tp_count, t - 1).wait_send()

    @pl.when(t < tp_count - 1)
    def _():
        row_copy(t, tp_count + 1, t + 1).wait_send()

    for lane, (toward, part, needed) in enumerate(sends):
        target = (margin + group if lane >= 2 else 0) + part * half
        handle = remote(
            pair_ref.at[pl.ds(margin + part * half, half)],
            pair_ref.at[pl.ds(target, half)],
            halo_send.at[lane],
            halo_recv.at[lane],
            toward,
            t,
        )

        @pl.when(needed)
        def _(handle=handle):
            handle.wait_send()

        @pl.when(receives[lane])
        def _(handle=handle):
            handle.wait_recv()


def project(fsdp_count, tp_count, x, gain, shift, weights, bias, margin):
    bf16 = jnp.bfloat16
    rows, features = x.shape
    width = weights.shape[1] // 3
    group = rows * tp_count
    depth = weights.shape[0]
    whole = pl.BlockSpec(memory_space=pltpu.VMEM)
    dma = pltpu.SemaphoreType.DMA
    return pl.pallas_call(
        functools.partial(project_kernel, fsdp_count, tp_count),
        out_shape=(
            jax.ShapeDtypeStruct((group, width), bf16),
            jax.ShapeDtypeStruct((group + 2 * margin, 2 * width), bf16),
            jax.ShapeDtypeStruct((tp_count, rows, features), bf16),
            jax.ShapeDtypeStruct((depth * fsdp_count, 3 * width), bf16),
        ),
        in_specs=[whole] * 5,
        out_specs=(whole,) * 4,
        scratch_shapes=[
            dma((fsdp_count,)),
            dma((fsdp_count,)),
            dma((tp_count + 2,)),
            dma((tp_count,)),
            dma((4,)),
            dma((4,)),
        ],
        compiler_params=pltpu.CompilerParams(
            collective_id=1, has_side_effects=True, vmem_limit_bytes=VMEM_LIMIT
        ),
        name="project",
    )(x, gain, shift, weights, bias)


def on_device(
    inputs,
    out_cotangent,
    clip_lengths,
    norm1_gain,
    norm1_shift,
    query_weight,
    query_bias,
    key_weight,
    value_weight,
    value_bias,
    out_weight,
    out_bias,
    norm2_gain,
    norm2_shift,
    fc1_weight,
    fc1_bias,
    fc2_weight,
    fc2_bias,
):
    bf16 = jnp.bfloat16
    f32 = jnp.float32
    tp_count = lax.axis_size("tp")
    fsdp_count = lax.axis_size("fsdp")
    tp_index = lax.axis_index("tp")
    fsdp_index = lax.axis_index("fsdp")
    own_rows = inputs.shape[0]
    group_rows = out_cotangent.shape[0]
    score_scale = 1.0 / math.sqrt(HD)
    margin = CLIP - QB
    tp_slot = (jnp.arange(tp_count) == tp_index).astype(f32)
    own_cotangent = lax.dynamic_slice_in_dim(out_cotangent, tp_index * own_rows, own_rows, 0)
    unit1, spread1, _ = normalize(inputs, norm1_gain, norm1_shift)
    local_width = query_weight.shape[1]
    heads_here = local_width // HD
    by_tp = lambda bias: bias.reshape(tp_count, 1, local_width)
    attention_bias = jnp.concatenate(
        [jnp.zeros((tp_count, 1, local_width), f32), by_tp(value_bias), by_tp(query_bias)], axis=2
    )
    query, pairs, normed, attention_w = project(
        fsdp_count,
        tp_count,
        inputs,
        norm1_gain.reshape(1, -1),
        norm1_shift.reshape(1, -1),
        jnp.concatenate([key_weight, value_weight, query_weight], axis=1),
        attention_bias,
        margin,
    )
    normed = normed.reshape(group_rows, -1)
    key_w, value_w, query_w = jnp.split(attention_w, 3, axis=1)
    padded = jnp.stack(jnp.split(pairs, 2, axis=1))
    out_w = lax.all_gather(out_weight, "fsdp", axis=0, tiled=True)
    group_base = fsdp_index * group_rows
    clip_ids = jnp.arange(clip_lengths.shape[0])
    block_count = group_rows // QB

    def block_scores(block_index):
        first_row = block_index * QB
        clip_index = (group_base + first_row) // CLIP
        key_start = clip_index * CLIP - group_base + margin
        length = jnp.sum(jnp.where(clip_ids == clip_index, clip_lengths, 0))
        query_block = lax.dynamic_slice_in_dim(query, first_row, QB, 0).reshape(QB, heads_here, HD)
        pair = lax.dynamic_slice_in_dim(padded, key_start, CLIP, 1).reshape(2, CLIP, heads_here, HD)
        scores = (
            jnp.einsum("qhe,khe->hqk", query_block, pair[0], preferred_element_type=f32)
            * score_scale
        )
        scores = jnp.where((jnp.arange(CLIP) < length)[None, None, :], scores, far_negative)
        return (first_row, key_start, query_block, pair[0], pair[1], scores)

    def attend(block_index, carry):
        context_rows, total_rows = carry
        first_row, key_start, query_block, key_block, value_block, scores = block_scores(
            block_index
        )
        highest = jnp.max(scores, axis=-1, keepdims=True)
        log_total = highest[..., 0] + jnp.log(jnp.sum(jnp.exp(scores - highest), axis=-1))
        weights = jnp.exp(scores - log_total[..., None]).astype(bf16)
        block_out = jnp.einsum("hqk,khe->qhe", weights, value_block, preferred_element_type=f32)
        block_out = block_out.astype(bf16).reshape(QB, local_width)
        context_rows = lax.dynamic_update_slice_in_dim(context_rows, block_out, first_row, 0)
        total_rows = lax.dynamic_update_slice_in_dim(total_rows, log_total, first_row, 1)
        return (context_rows, total_rows)

    context, totals = lax.fori_loop(
        0,
        block_count,
        attend,
        (jnp.zeros((group_rows, local_width), bf16), jnp.zeros((heads_here, group_rows), f32)),
    )
    attended = scatter_rows(contract_cols(context, out_w), "tp")
    hidden = inputs + attended + out_bias
    unit2, spread2, normed2_full = normalize(hidden, norm2_gain, norm2_shift)
    normed2_own = normed2_full.astype(bf16)
    normed2 = lax.all_gather(normed2_own, "tp", axis=0, tiled=True)
    w_up, w_down = jnp.split(
        lax.all_gather(
            jnp.concatenate([fc1_weight, fc2_weight], axis=1), "fsdp", axis=0, tiled=True
        ),
        2,
        axis=1,
    )
    unit_count = fc1_weight.shape[0]
    bias_up = lax.dynamic_index_in_dim(
        fc1_bias.reshape(fsdp_count, tp_count, unit_count), tp_index, 1, False
    ).reshape(-1)
    preact = contract_cols(normed2, w_up) + bias_up
    activated = gelu_exact(preact).astype(bf16)
    mixed = scatter_rows(jnp.dot(activated, w_down, preferred_element_type=f32), "tp")
    outputs = hidden + mixed + fc2_bias
    up_rounded = out_cotangent.astype(bf16)
    dactivated = contract_cols(up_rounded, w_down)
    dpreact = (dactivated * gelu_slope(preact)).astype(bf16)
    grad_up_part = contract_rows(dpreact, normed2)
    grad_down_part = contract_rows(activated, up_rounded)
    upbias_part = jnp.sum(dpreact.astype(f32), axis=0)
    grad_b1 = (upbias_part.reshape(fsdp_count, 1, unit_count) * tp_slot[None, :, None]).reshape(-1)
    dnorm2 = scatter_rows(jnp.dot(dpreact, w_up, preferred_element_type=f32), "tp")
    grad_fc1, grad_fc2 = jnp.split(
        scatter_rows(jnp.concatenate([grad_up_part, grad_down_part], axis=1), "fsdp"), 2, axis=1
    )
    grad_b2 = jnp.sum(own_cotangent, axis=0)
    grad_gain2 = jnp.sum(dnorm2 * unit2, axis=0)
    grad_shift2 = jnp.sum(dnorm2, axis=0)
    dhidden = own_cotangent + norm_back(dnorm2, unit2, spread2, norm2_gain)
    grad_obias = jnp.sum(dhidden, axis=0)
    dh_all = lax.all_gather(dhidden.astype(bf16), "tp", axis=0, tiled=True)
    dcontext = jnp.dot(dh_all, out_w, preferred_element_type=f32).astype(bf16)
    grad_out = contract_rows(dh_all, context)
    delta = jnp.sum(
        (dcontext.astype(f32) * context.astype(f32)).reshape(group_rows, heads_here, HD), axis=-1
    ).T

    def attend_back(block_index, carry):
        dquery_rows, dpair = carry
        first_row, key_start, query_block, key_block, value_block, scores = block_scores(
            block_index
        )
        grad_block = lax.dynamic_slice_in_dim(dcontext, first_row, QB, 0).reshape(
            QB, heads_here, HD
        )
        probs = jnp.exp(scores - lax.dynamic_slice_in_dim(totals, first_row, QB, 1)[..., None])
        delta_block = lax.dynamic_slice_in_dim(delta, first_row, QB, 1)
        dprobs = jnp.einsum("qhe,khe->hqk", grad_block, value_block, preferred_element_type=f32)
        dscores = (probs * (dprobs - delta_block[..., None]) * score_scale).astype(bf16)
        dquery_block = jnp.einsum("hqk,khe->qhe", dscores, key_block, preferred_element_type=f32)
        dquery_block = dquery_block.astype(bf16).reshape(QB, local_width)
        dkey_block = jnp.einsum(
            "hqk,qhe->khe", dscores, query_block, preferred_element_type=f32
        ).reshape(CLIP, local_width)
        dvalue_block = jnp.einsum(
            "hqk,qhe->khe", probs.astype(bf16), grad_block, preferred_element_type=f32
        ).reshape(CLIP, local_width)
        current = lax.dynamic_slice_in_dim(dpair, key_start, CLIP, 1)
        dpair = lax.dynamic_update_slice_in_dim(
            dpair, current + jnp.stack([dkey_block, dvalue_block]), key_start, 1
        )
        dquery_rows = lax.dynamic_update_slice_in_dim(dquery_rows, dquery_block, first_row, 0)
        return (dquery_rows, dpair)

    dquery, dpair = lax.fori_loop(
        0,
        block_count,
        attend_back,
        (jnp.zeros((group_rows, local_width), bf16), jnp.zeros(padded.shape, f32)),
    )
    rims = jnp.concatenate([dpair[:, :margin], dpair[:, margin + group_rows :]], axis=1)
    received = extended(rims, (("fsdp", 1),), margin)
    inner_part = dpair[:, margin : margin + group_rows]
    inner_part = inner_part.at[:, :margin].add(received[:, :margin])
    inner_part = inner_part.at[:, group_rows - margin :].add(received[:, 3 * margin :])
    dkey = inner_part[0].astype(bf16)
    dvalue = inner_part[1].astype(bf16)
    grad_query = contract_rows(normed, dquery)
    grad_key = contract_rows(normed, dkey)
    grad_value = contract_rows(normed, dvalue)
    grad_qbias = (tp_slot[:, None] * jnp.sum(dquery.astype(f32), axis=0)[None, :]).reshape(-1)
    grad_vbias = (tp_slot[:, None] * jnp.sum(dvalue.astype(f32), axis=0)[None, :]).reshape(-1)
    dnorm1 = scatter_rows(
        contract_cols(dquery, query_w)
        + contract_cols(dkey, key_w)
        + contract_cols(dvalue, value_w),
        "tp",
    )
    grad_gain1 = jnp.sum(dnorm1 * unit1, axis=0)
    grad_shift1 = jnp.sum(dnorm1, axis=0)
    inputs_grad = dhidden + norm_back(dnorm1, unit1, spread1, norm1_gain)
    grad_query, grad_key, grad_value, grad_out = jnp.split(
        scatter_rows(
            jnp.concatenate([grad_query, grad_key, grad_value, grad_out], axis=1), "fsdp"
        ),
        4,
        axis=1,
    )
    (
        grad_gain1,
        grad_shift1,
        grad_qbias,
        grad_vbias,
        grad_obias,
        grad_gain2,
        grad_shift2,
        grad_b1,
        grad_b2,
    ) = lax.psum(
        (
            grad_gain1,
            grad_shift1,
            grad_qbias,
            grad_vbias,
            grad_obias,
            grad_gain2,
            grad_shift2,
            grad_b1,
            grad_b2,
        ),
        ("fsdp", "tp"),
    )
    return (
        outputs,
        inputs_grad,
        grad_gain1,
        grad_shift1,
        grad_query,
        grad_qbias,
        grad_key,
        grad_value,
        grad_vbias,
        grad_out,
        grad_obias,
        grad_gain2,
        grad_shift2,
        grad_fc1,
        grad_b1,
        grad_fc2,
        grad_b2,
    )


def solution(mesh):
    in_specs = (
        P(("fsdp", "tp"), None),
        P("fsdp", None),
        P(),
        P(),
        P(),
        P("fsdp", "tp"),
        P(),
        P("fsdp", "tp"),
        P("fsdp", "tp"),
        P(),
        P("fsdp", "tp"),
        P(),
        P(),
        P(),
        P(("fsdp", "tp"), None),
        P(),
        P(("fsdp", "tp"), None),
        P(),
    )
    out_specs = (
        P(("fsdp", "tp"), None),
        P(("fsdp", "tp"), None),
        P(),
        P(),
        P("fsdp", "tp"),
        P(),
        P("fsdp", "tp"),
        P("fsdp", "tp"),
        P(),
        P("fsdp", "tp"),
        P(),
        P(),
        P(),
        P(("fsdp", "tp"), None),
        P(),
        P(("fsdp", "tp"), None),
        P(),
    )
    return jax.shard_map(
        on_device, mesh=mesh, in_specs=in_specs, out_specs=out_specs, check_vma=False
    )
```

```python
import functools
import math

import jax
import jax.numpy as jnp
from jax import lax
from jax.experimental import pallas as pl
from jax.experimental.pallas import tpu as pltpu
from jax.sharding import PartitionSpec as P

HD = 64
CLIP = 1536
QB = 512


eps_norm = 1e-05
root_half = 0.7071067811865476
inv_root_tau = 0.3989422804014327
far_negative = -1e30


def extended(value, sides, width):
    for axis, dim in sides:
        size, length = (lax.axis_size(axis), value.shape[dim])
        up = [(i, (i + 1) % size) for i in range(size - 1)]
        down = [(j, i) for i, j in up]
        last = lax.slice_in_dim(value, length - width, length, axis=dim)
        initial = lax.slice_in_dim(value, 0, width, axis=dim)
        before = lax.ppermute(last, axis, up)
        after = lax.ppermute(initial, axis, down)
        value = jnp.concatenate([before, value, after], axis=dim)
    return value


def normalize(rows, gain, shift):
    centre = jnp.mean(rows, axis=-1, keepdims=True)
    centred = rows - centre
    inv_spread = lax.rsqrt(jnp.mean(centred * centred, axis=-1, keepdims=True) + eps_norm)
    unit_rows = centred * inv_spread
    return (unit_rows, inv_spread, unit_rows * gain + shift)


def norm_back(upstream, unit_rows, inv_spread, gain):
    scaled = upstream * gain
    return inv_spread * (
        scaled
        - jnp.mean(scaled, axis=-1, keepdims=True)
        - unit_rows * jnp.mean(scaled * unit_rows, axis=-1, keepdims=True)
    )


def gelu_exact(values):
    return 0.5 * values * (1.0 + lax.erf(values * root_half))


def gelu_slope(values):
    return (
        0.5 * (1.0 + lax.erf(values * root_half))
        + values * jnp.exp(-0.5 * values * values) * inv_root_tau
    )


def contract_rows(left_rows, right_rows):
    return lax.dot_general(
        left_rows, right_rows, (((0,), (0,)), ((), ())), preferred_element_type=jnp.float32
    )


def contract_cols(left_rows, right_rows):
    return lax.dot_general(
        left_rows, right_rows, (((1,), (1,)), ((), ())), preferred_element_type=jnp.float32
    )


def scatter_rows(partial_rows, axis):
    return lax.psum_scatter(
        partial_rows.astype(jnp.bfloat16), axis, scatter_dimension=0, tiled=True
    ).astype(jnp.float32)


MESH = pl.DeviceIdType.MESH
VMEM_LIMIT = 60 * 1024 * 1024
LANES = 128


def remote(source, target, send_sem, recv_sem, fsdp_to, tp_to):
    return pltpu.make_async_remote_copy(
        src_ref=source,
        dst_ref=target,
        send_sem=send_sem,
        recv_sem=recv_sem,
        device_id=(fsdp_to, tp_to),
        device_id_type=MESH,
    )


def greet(fsdp_count, tp_count, f, t):
    barrier = pltpu.get_barrier_semaphore()

    def greet_fsdp(i, carry):
        pl.semaphore_signal(
            barrier, inc=1, device_id=(lax.rem(f + i, fsdp_count), t), device_id_type=MESH
        )
        return carry

    def greet_tp(j, carry):
        pl.semaphore_signal(
            barrier, inc=1, device_id=(f, lax.rem(t + j, tp_count)), device_id_type=MESH
        )
        return carry

    lax.fori_loop(1, fsdp_count, greet_fsdp, 0)
    lax.fori_loop(1, tp_count, greet_tp, 0)
    pl.semaphore_wait(barrier, fsdp_count + tp_count - 2)


def gather_copies(f, t, fsdp_count, sources, targets, depth, sends, recvs):
    partner = f + 1 - 2 * lax.rem(f, 2)

    def piece(target, owner):
        return target.at[:, pl.ds(owner * depth, depth)]

    def copies(owner, toward, lane, first):
        return [
            remote(
                source if first else piece(target, owner),
                piece(target, owner),
                send.at[lane],
                recv.at[owner],
                toward,
                t,
            )
            for source, target, send, recv in zip(sources, targets, sends, recvs)
        ]

    def start():
        def body(i, carry):
            for handle in copies(f, lax.rem(f + 2 * i, fsdp_count), i, True):
                handle.start()
            return carry

        lax.fori_loop(1, fsdp_count // 2, body, 0)
        for handle in copies(f, partner, 0, True):
            handle.start()
        for source, target in zip(sources, targets):
            target[:, pl.ds(f * depth, depth), :] = source[...]

    def relay():
        def body(i, carry):
            owner = lax.rem(f + fsdp_count - 2 * i, fsdp_count)
            for handle in copies(owner, partner, fsdp_count // 2 + i, False):
                handle.wait_recv()
                handle.start()
            return carry

        lax.fori_loop(1, fsdp_count // 2, body, 0)

    def finish():
        def body(i, carry):
            owner = lax.rem(partner + 2 * i, fsdp_count)
            for handle in copies(owner, partner, 0, False):
                handle.wait_recv()
            return carry

        lax.fori_loop(0, fsdp_count // 2, body, 0)

    def drain():
        def body(i, carry):
            for handle in copies(f, lax.rem(f + 2 * i, fsdp_count), i, True):
                handle.wait_send()
            for handle in copies(
                lax.rem(f + fsdp_count - 2 * i, fsdp_count),
                partner,
                fsdp_count // 2 + i,
                False,
            ):
                handle.wait_send()
            return carry

        lax.fori_loop(1, fsdp_count // 2, body, 0)
        for handle in copies(f, partner, 0, True):
            handle.wait_send()

    return (start, relay, finish, drain)


def project_kernel(
    fsdp_count,
    tp_count,
    x_ref,
    gain_ref,
    shift_ref,
    weight_ref,
    bias_ref,
    mlp_ref,
    out_ref,
    query_ref,
    pair_ref,
    normed_ref,
    full_ref,
    mlp_full,
    heads_ref,
    side_send,
    side_recv,
    weight_send,
    weight_recv,
    mlp_send,
    mlp_recv,
    row_send,
    row_recv,
    halo_send,
    halo_recv,
):
    f = lax.axis_index("fsdp")
    t = lax.axis_index("tp")
    rows = x_ref.shape[0]
    depth = weight_ref.shape[1]
    group = rows * tp_count
    pair_width = pair_ref.shape[1]
    margin = (pair_ref.shape[0] - group) // 2
    per_half = tp_count // 2
    phase = lax.rem(f, 3)
    above = f + 1 < fsdp_count
    below = f > 0
    blank = jnp.zeros((256, pair_width), jnp.bfloat16)

    def clear(i, carry):
        pair_ref[pl.ds(i * 256, 256), :] = blank
        pair_ref[pl.ds(margin + group + i * 256, 256), :] = blank
        return carry

    lax.fori_loop(0, margin // 256, clear, 0)
    greet(fsdp_count, tp_count, f, t)
    start_weights, relay_weights, finish_weights, drain_weights = gather_copies(
        f, t, fsdp_count, (weight_ref,), (full_ref,), depth, (weight_send,), (weight_recv,)
    )
    start_mlp, relay_mlp, finish_mlp, drain_mlp = gather_copies(
        f, t, fsdp_count, (mlp_ref,), (mlp_full,), depth, (mlp_send,), (mlp_recv,)
    )
    start_weights()
    _, _, normed = normalize(x_ref[...], gain_ref[...], shift_ref[...])
    normed_ref[t] = normed.astype(jnp.bfloat16)

    def row_copy(source, lane, toward):
        return remote(
            normed_ref.at[source],
            normed_ref.at[source],
            row_send.at[lane],
            row_recv.at[source],
            f,
            toward,
        )

    @pl.when(t > 0)
    def _():
        row_copy(t, tp_count, t - 1).start()

    @pl.when(t < tp_count - 1)
    def _():
        row_copy(t, tp_count + 1, t + 1).start()

    def heads_copy(j):
        return remote(
            out_ref,
            heads_ref.at[t],
            side_send.at[j],
            side_recv.at[j],
            f,
            lax.rem(t + j, tp_count),
        )

    def heads_start(j, carry):
        heads_copy(j).start()
        return carry

    def heads_done(j, carry):
        heads_copy(j).wait_send()
        source = lax.rem(t + tp_count - j, tp_count)
        remote(
            out_ref, heads_ref.at[source], side_send.at[j], side_recv.at[j], f, source
        ).wait_recv()
        return carry

    heads_ref[t] = out_ref[...]
    lax.fori_loop(1, tp_count, heads_start, 0)
    relay_weights()
    start_mlp()
    finish_weights()

    def halo_copy(source, side):
        return remote(
            pair_ref.at[pl.ds(margin + source * rows, rows)],
            pair_ref.at[pl.ds((0 if side == 0 else margin + group) + source * rows, rows)],
            halo_send.at[side, source],
            halo_recv.at[side, source],
            f + 1 if side == 0 else f - 1,
            t,
        )

    def halo_sends(source):
        late = source >= per_half
        return (
            above & ((phase == 0) | ((phase == 1) & late)),
            below & ((phase == 2) | ((phase == 1) & jnp.logical_not(late))),
        )

    def halo_receives(source):
        late = source >= per_half
        return (
            below & ((phase == 1) | ((phase == 2) & late)),
            above & ((phase == 1) | ((phase == 0) & jnp.logical_not(late))),
        )

    def compute(source):
        out = jnp.dot(normed_ref[source], full_ref[0], preferred_element_type=jnp.float32)
        out = (out + bias_ref[t]).astype(jnp.bfloat16)
        pair_ref[pl.ds(margin + source * rows, rows), :] = out[:, :pair_width]
        for side, needed in enumerate(halo_sends(source)):

            @pl.when(needed)
            def _(side=side):
                halo_copy(source, side).start()

        query_ref[pl.ds(source * rows, rows), :] = out[:, pair_width:]

    compute(t)

    def arrival(k):
        step = k // 2 + 1
        side = 2 * lax.rem(k, 2) - 1
        source = t + side * step
        onward = t - side
        valid = (source >= 0) & (source < tp_count)
        return (source, onward, valid, valid & (onward >= 0) & (onward < tp_count))

    def receive(k, carry):
        source, onward, valid, forward = arrival(k)

        @pl.when(valid)
        def _():
            row_copy(source, 0, t).wait_recv()

            @pl.when(forward)
            def _():
                row_copy(source, source, onward).start()

            compute(source)

        return carry

    lax.fori_loop(0, 2 * (tp_count - 1), receive, 0)
    relay_mlp()
    lax.fori_loop(1, tp_count, heads_done, 0)

    def sent(k, carry):
        source, onward, valid, forward = arrival(k)

        @pl.when(forward)
        def _():
            row_copy(source, source, onward).wait_send()

        return carry

    lax.fori_loop(0, 2 * (tp_count - 1), sent, 0)

    @pl.when(t > 0)
    def _():
        row_copy(t, tp_count, t - 1).wait_send()

    @pl.when(t < tp_count - 1)
    def _():
        row_copy(t, tp_count + 1, t + 1).wait_send()

    def halo_done(source, carry):
        for side, (sends, receives) in enumerate(zip(halo_sends(source), halo_receives(source))):

            @pl.when(sends)
            def _(side=side):
                halo_copy(source, side).wait_send()

            @pl.when(receives)
            def _(side=side):
                halo_copy(source, side).wait_recv()

        return carry

    lax.fori_loop(0, tp_count, halo_done, 0)
    drain_weights()
    finish_mlp()
    drain_mlp()


def whole_specs(count):
    return [pl.BlockSpec(memory_space=pltpu.VMEM)] * count


def project(fsdp_count, tp_count, x, gain, shift, weights, bias, mlp, out_weight, pair_width, margin):
    bf16 = jnp.bfloat16
    rows, features = x.shape
    group = rows * tp_count
    depth = weights.shape[1]
    dma = pltpu.SemaphoreType.DMA
    return pl.pallas_call(
        functools.partial(project_kernel, fsdp_count, tp_count),
        out_shape=(
            jax.ShapeDtypeStruct((group, weights.shape[2] - pair_width), bf16),
            jax.ShapeDtypeStruct((group + 2 * margin, pair_width), bf16),
            jax.ShapeDtypeStruct((tp_count, rows, features), bf16),
            jax.ShapeDtypeStruct((1, depth * fsdp_count, weights.shape[2]), bf16),
            jax.ShapeDtypeStruct((2, depth * fsdp_count, features), bf16),
            jax.ShapeDtypeStruct((tp_count, *out_weight.shape), bf16),
        ),
        in_specs=whole_specs(7),
        out_specs=tuple(whole_specs(6)),
        scratch_shapes=[
            dma((tp_count,)),
            dma((tp_count,)),
            dma((fsdp_count,)),
            dma((fsdp_count,)),
            dma((fsdp_count,)),
            dma((fsdp_count,)),
            dma((tp_count + 2,)),
            dma((tp_count,)),
            dma((2, tp_count)),
            dma((2, tp_count)),
        ],
        compiler_params=pltpu.CompilerParams(
            collective_id=1, has_side_effects=True, vmem_limit_bytes=VMEM_LIMIT
        ),
        name="project",
    )(x, gain, shift, weights, bias, mlp, out_weight)


def block_clip(f, part, margin):
    phase = lax.rem(f, 3)
    start = jnp.where(
        phase == 0,
        margin,
        jnp.where(phase == 2, margin - QB, jnp.where(part == 0, 0, margin + QB)),
    )
    return (pl.multiple_of(start, QB), (2 * f + part) // 3)


def head_tiles(pair, length):
    lane = lax.broadcasted_iota(jnp.int32, pair.shape, 1)
    row = lax.broadcasted_iota(jnp.int32, pair.shape, 0)
    extra = jnp.where(
        lane == HD,
        jnp.where(row < length, 0.0, far_negative),
        jnp.where(lane <= HD + 3, 1.0, 0.0),
    )
    return jnp.where(lane < HD, pair, extra)


def spread_heads(rows, head):
    tile = rows[:, (head // 2) * LANES : (head // 2 + 1) * LANES]
    return pltpu.roll(tile, HD, axis=1) if head % 2 else tile


def three_parts(column):
    high = column.astype(jnp.bfloat16).astype(jnp.float32)
    rest = column - high
    middle = rest.astype(jnp.bfloat16).astype(jnp.float32)
    return (high, middle, rest - middle)


def attend_kernel(
    fsdp_count,
    tp_count,
    lengths_ref,
    query_ref,
    pair_ref,
    mlp_ref,
    out_ref,
    spread_ref,
    context_ref,
    wide_ref,
    mlp_full,
    out_full,
    mate_ref,
    key_tiles,
    value_tiles,
    mate_send,
    mate_recv,
    context_send,
    context_recv,
    mlp_send,
    mlp_recv,
    out_send,
    out_recv,
):
    f = lax.axis_index("fsdp")
    t = lax.axis_index("tp")
    bf16 = jnp.bfloat16
    f32 = jnp.float32
    rows = spread_ref.shape[1]
    heads = wide_ref.shape[0]
    group = rows * tp_count
    margin = (pair_ref.shape[0] - group) // 2
    greet(fsdp_count, tp_count, f, t)
    depth = mlp_ref.shape[1]
    start_out, relay_out, finish_out, drain_out = gather_copies(
        f, t, fsdp_count, (out_ref,), (out_full,), depth, (out_send,), (out_recv,)
    )
    start_mlp, relay_mlp, finish_mlp, drain_mlp = gather_copies(
        f, t, fsdp_count, (mate_ref,), (mlp_full,), depth, (mlp_send,), (mlp_recv,)
    )
    mate_copy = remote(
        mlp_ref, mate_ref, mate_send, mate_recv, f, lax.rem(t + tp_count // 2, tp_count)
    )
    mate_copy.start()
    start_out()
    per_half = tp_count // 2

    def context_copy(toward):
        return remote(
            context_ref.at[pl.ds(toward * rows, rows)],
            spread_ref.at[t],
            context_send.at[toward],
            context_recv.at[t],
            f,
            toward,
        )

    lane = lax.broadcasted_iota(jnp.int32, (rows, LANES), 1)
    row = lax.broadcasted_iota(jnp.int32, (LANES, rows), 0)
    tall = lax.broadcasted_iota(jnp.int32, (LANES, CLIP), 0)

    def half(step, carry):
        part = lax.rem(t // per_half + 1 + step, 2)
        first, clip = block_clip(f, part, margin)
        length = lengths_ref[clip]
        for head in range(heads):
            pair = pair_ref[pl.ds(first, CLIP), head * LANES : (head + 1) * LANES].astype(f32)
            key_tiles[head] = head_tiles(pair, length).astype(bf16)
            value_tiles[head] = jnp.where(tall < HD, 1.0, pair.T).astype(bf16)

        def block(i, inner):
            within = lax.rem(lax.rem(t, per_half) + 1 + i, per_half)
            index = part * per_half + within
            here = pl.ds(pl.multiple_of(index * rows, rows), rows)
            query = query_ref[here, :].astype(f32) * (1.0 / math.sqrt(HD))
            parts = []
            for head in range(heads):
                wide = jnp.where(
                    lane < HD, spread_heads(query, head), jnp.where(lane == HD, 1.0, 0.0)
                )
                scores = lax.dot_general(
                    key_tiles[head],
                    wide.astype(bf16),
                    (((1,), (1,)), ((), ())),
                    preferred_element_type=f32,
                )
                highest = jnp.max(scores, axis=0, keepdims=True)
                weights = jnp.exp(scores - highest).astype(bf16)
                summed = jnp.dot(value_tiles[head], weights, preferred_element_type=f32)
                total = summed[0:1, :]
                log_total = highest + jnp.log(total)
                turned = jnp.where(row == 0, log_total, summed * (1.0 / total)).T
                high, middle, low = three_parts(turned[:, 0:1])
                wide_ref[head, here, :] = jnp.where(
                    lane == HD + 1,
                    -high,
                    jnp.where(lane == HD + 2, -middle, jnp.where(lane == HD + 3, -low, wide)),
                ).astype(bf16)
                parts.append(turned)
            context_ref[here, 0:LANES] = jnp.where(
                lane < HD, pltpu.roll(parts[0], HD, axis=1), parts[1]
            ).astype(bf16)
            context_ref[here, LANES : LANES + HD] = pltpu.roll(parts[2], HD, axis=1)[
                :, :HD
            ].astype(bf16)

            @pl.when(index == t)
            def _():
                spread_ref[t] = context_ref[here, :]

            @pl.when(index != t)
            def _():
                context_copy(index).start()

            return inner

        lax.fori_loop(0, per_half, block, 0)

        @pl.when(step == 0)
        def _():
            mate_copy.wait()
            start_mlp()
            relay_out()

        return carry

    lax.fori_loop(0, 2, half, 0)
    relay_mlp()

    def settle(j, carry):
        toward = lax.rem(t + j, tp_count)
        context_copy(toward).wait_send()
        remote(
            context_ref.at[pl.ds(0, rows)],
            spread_ref.at[toward],
            context_send.at[toward],
            context_recv.at[toward],
            f,
            toward,
        ).wait_recv()
        return carry

    lax.fori_loop(1, tp_count, settle, 0)
    finish_out()
    finish_mlp()
    drain_out()
    drain_mlp()


def attend(fsdp_count, tp_count, lengths, query, pairs, mlp, out_weights, heads):
    bf16 = jnp.bfloat16
    group = query.shape[0]
    rows = group // tp_count
    width = heads * HD
    dma = pltpu.SemaphoreType.DMA
    depth = mlp.shape[1]
    return pl.pallas_call(
        functools.partial(attend_kernel, fsdp_count, tp_count),
        out_shape=(
            jax.ShapeDtypeStruct((tp_count, rows, width), bf16),
            jax.ShapeDtypeStruct((group, width), bf16),
            jax.ShapeDtypeStruct((heads, group, LANES), bf16),
            jax.ShapeDtypeStruct((mlp.shape[0], depth * fsdp_count, mlp.shape[2]), bf16),
            jax.ShapeDtypeStruct((tp_count, depth * fsdp_count, width), bf16),
        ),
        in_specs=[pl.BlockSpec(memory_space=pltpu.SMEM)] + whole_specs(4),
        out_specs=tuple(whole_specs(5)),
        scratch_shapes=[
            pltpu.VMEM(mlp.shape, bf16),
            pltpu.VMEM((heads, CLIP, LANES), bf16),
            pltpu.VMEM((heads, LANES, CLIP), bf16),
            dma,
            dma,
            dma((tp_count,)),
            dma((tp_count,)),
            dma((fsdp_count,)),
            dma((fsdp_count,)),
            dma((fsdp_count,)),
            dma((fsdp_count,)),
        ],
        compiler_params=pltpu.CompilerParams(
            collective_id=2, has_side_effects=True, vmem_limit_bytes=VMEM_LIMIT
        ),
        name="attend",
    )(lengths, query, pairs, mlp, out_weights)


def column_sum(rows):
    return jnp.sum(rows, axis=0, keepdims=True)


def rows_kernel(
    fsdp_count,
    tp_count,
    x_ref,
    spread_ref,
    heads_ref,
    vector_ref,
    bias_ref,
    own_ref,
    mate_ref,
    cotangent_ref,
    gradient_ref,
    outputs_ref,
    mixed_ref,
    context_ref,
    own_grad,
    mate_grad,
    heads_grad,
    bias_grad,
    sums_ref,
    upstream,
    rounded,
    hidden_ref,
    unit_ref,
    normed_ref,
    active_ref,
    slope_ref,
    mixed_sum,
    norm_sum,
    norm_out,
    norm_in,
    load_sem,
    row_send,
    row_recv,
    norm_send,
    norm_recv,
):
    f = lax.axis_index("fsdp")
    t = lax.axis_index("tp")
    bf16 = jnp.bfloat16
    f32 = jnp.float32
    rows = x_ref.shape[0]
    tile = 256
    side = lax.rem(t, 2)
    peer = t + 1 - 2 * side
    load = pltpu.make_async_copy(
        cotangent_ref.at[pl.ds((t - side) * rows, 2 * rows)], upstream, load_sem
    )
    load.start()
    barrier = pltpu.get_barrier_semaphore()
    pl.semaphore_signal(barrier, inc=1, device_id=(f, peer), device_id_type=MESH)
    pl.semaphore_wait(barrier, 1)

    hidden = x_ref[...] + vector_ref[0:1, :]
    for j in range(tp_count):
        hidden = hidden + lax.dot_general(
            spread_ref[j], heads_ref[j], (((1,), (1,)), ((), ())), preferred_element_type=f32
        )
    hidden_ref[...] = hidden
    unit, spread, normed = normalize(hidden, vector_ref[1:2, :], vector_ref[2:3, :])
    unit_ref[...] = unit
    normed_ref[side] = normed.astype(bf16)
    row_copy = remote(normed_ref.at[side], normed_ref.at[side], row_send, row_recv, f, peer)
    row_copy.start()
    load.wait()

    def rounding(i, carry):
        rounded[pl.ds(i * rows, rows), :] = upstream[pl.ds(i * rows, rows), :].astype(bf16)
        return carry

    lax.fori_loop(0, 2, rounding, 0)
    mixed_sum[...] = jnp.zeros(mixed_sum.shape, f32)
    norm_sum[...] = jnp.zeros(norm_sum.shape, f32)
    chunks = own_ref.shape[1] // tile
    mate = lax.rem(t + tp_count // 2, tp_count)

    def feed_forward(turn, carry):
        which = lax.rem(side + turn, 2)

        @pl.when(turn == 1)
        def _():
            row_copy.wait_recv()

        here = pl.ds(pl.multiple_of(which * rows, rows), rows)
        normed_rows = normed_ref[which]
        upstream_rows = rounded[here, :]

        for level, (weights, owner) in enumerate(((own_ref, t), (mate_ref, mate))):

            def chunk(c, inner, weights=weights, owner=owner, level=level):
                units = pl.ds(pl.multiple_of(c * tile, tile), tile)
                up = weights[0, units, :]
                down = weights[1, units, :]
                preact = (
                    lax.dot_general(
                        normed_rows, up, (((1,), (1,)), ((), ())), preferred_element_type=f32
                    )
                    + bias_ref[owner, c]
                )
                cdf = 0.5 * (1.0 + lax.erf(preact * root_half))
                active = (preact * cdf).astype(bf16)
                slope = cdf + preact * jnp.exp(-0.5 * preact * preact) * inv_root_tau
                dactive = lax.dot_general(
                    upstream_rows, down, (((1,), (1,)), ((), ())), preferred_element_type=f32
                )
                dpreact = (dactive * slope).astype(bf16)
                active_ref[level, c, here, :] = active
                slope_ref[level, c, here, :] = dpreact
                norm_sum[which] += jnp.dot(dpreact, up, preferred_element_type=f32)
                mixed_sum[which] += jnp.dot(active, down, preferred_element_type=f32)
                return inner

            lax.fori_loop(0, chunks, chunk, 0)
        return carry

    lax.fori_loop(0, 2, feed_forward, 0)
    norm_out[...] = norm_sum[1 - side].astype(bf16)
    norm_copy = remote(norm_out, norm_in, norm_send, norm_recv, f, peer)
    norm_copy.start()
    mixed_ref[...] = mixed_sum[1 - side].astype(bf16)
    outputs_ref[...] = hidden_ref[...] + mixed_sum[side] + vector_ref[3:4, :]

    for level, grad in enumerate((own_grad, mate_grad)):

        def weight_grads(c, carry, level=level, grad=grad):
            units = pl.ds(pl.multiple_of(c * tile, tile), tile)
            slopes = slope_ref[level, c]
            both = jnp.concatenate([normed_ref[0], normed_ref[1]], axis=0)
            grad[0, units, :] = contract_rows(slopes, both).astype(bf16)
            grad[1, units, :] = contract_rows(active_ref[level, c], rounded[...]).astype(bf16)
            bias_grad[level, c] = column_sum(slopes.astype(f32))
            return carry

        lax.fori_loop(0, chunks, weight_grads, 0)

    norm_copy.wait()
    dnorm = norm_sum[side] + norm_in[...].astype(f32)
    unit = unit_ref[...]
    cotangent = upstream[pl.ds(pl.multiple_of(side * rows, rows), rows), :]
    gradient = cotangent + norm_back(dnorm, unit, spread, vector_ref[1:2, :])
    gradient_ref[...] = gradient
    sums_ref[0:1, :] = column_sum(dnorm * unit)
    sums_ref[1:2, :] = column_sum(dnorm)
    sums_ref[2:3, :] = column_sum(gradient)
    sums_ref[3:4, :] = column_sum(cotangent)
    gradient = gradient.astype(bf16)
    for j in range(tp_count):
        context_ref[j] = jnp.dot(gradient, heads_ref[j], preferred_element_type=f32).astype(bf16)
        heads_grad[j] = contract_rows(gradient, spread_ref[j]).astype(bf16)
    row_copy.wait_send()


def by_rows(fsdp_count, tp_count, x, spread, heads, vectors, bias, own, mate, cotangent):
    bf16 = jnp.bfloat16
    f32 = jnp.float32
    rows, features = x.shape
    units = own.shape[1]
    chunks = units // 256
    dma = pltpu.SemaphoreType.DMA
    return pl.pallas_call(
        functools.partial(rows_kernel, fsdp_count, tp_count),
        out_shape=(
            jax.ShapeDtypeStruct((rows, features), f32),
            jax.ShapeDtypeStruct((rows, features), f32),
            jax.ShapeDtypeStruct((rows, features), bf16),
            jax.ShapeDtypeStruct(spread.shape, bf16),
            jax.ShapeDtypeStruct(own.shape, bf16),
            jax.ShapeDtypeStruct(own.shape, bf16),
            jax.ShapeDtypeStruct(heads.shape, bf16),
            jax.ShapeDtypeStruct((2, chunks, 1, 256), f32),
            jax.ShapeDtypeStruct((4, features), f32),
        ),
        in_specs=whole_specs(7) + [pl.BlockSpec(memory_space=pl.ANY)],
        out_specs=tuple(whole_specs(9)),
        scratch_shapes=[
            pltpu.VMEM((2 * rows, features), f32),
            pltpu.VMEM((2 * rows, features), bf16),
            pltpu.VMEM((rows, features), f32),
            pltpu.VMEM((rows, features), f32),
            pltpu.VMEM((2, rows, features), bf16),
            pltpu.VMEM((2, chunks, 2 * rows, 256), bf16),
            pltpu.VMEM((2, chunks, 2 * rows, 256), bf16),
            pltpu.VMEM((2, rows, features), f32),
            pltpu.VMEM((2, rows, features), f32),
            pltpu.VMEM((rows, features), bf16),
            pltpu.VMEM((rows, features), bf16),
            dma,
            dma,
            dma,
            dma,
            dma,
        ],
        compiler_params=pltpu.CompilerParams(
            collective_id=4, has_side_effects=True, vmem_limit_bytes=VMEM_LIMIT
        ),
        name="by_rows",
    )(x, spread, heads, vectors, bias, own, mate, cotangent)


def pack_columns(key, value, query):
    lead = key.shape[:-1]
    heads = key.shape[-1] // HD
    pairs = jnp.stack([key.reshape(*lead, heads, HD), value.reshape(*lead, heads, HD)], axis=-2)
    spare = jnp.zeros((*lead, -key.shape[-1] % LANES), key.dtype)
    return jnp.concatenate([pairs.reshape(*lead, -1), query, spare], axis=-1)


def on_device(
    inputs,
    out_cotangent,
    clip_lengths,
    norm1_gain,
    norm1_shift,
    query_weight,
    query_bias,
    key_weight,
    value_weight,
    value_bias,
    out_weight,
    out_bias,
    norm2_gain,
    norm2_shift,
    fc1_weight,
    fc1_bias,
    fc2_weight,
    fc2_bias,
):
    bf16 = jnp.bfloat16
    f32 = jnp.float32
    tp_count = lax.axis_size("tp")
    fsdp_count = lax.axis_size("fsdp")
    tp_index = lax.axis_index("tp")
    fsdp_index = lax.axis_index("fsdp")
    own_rows = inputs.shape[0]
    group_rows = out_cotangent.shape[0]
    score_scale = 1.0 / math.sqrt(HD)
    margin = CLIP - QB
    tp_slot = (jnp.arange(tp_count) == tp_index).astype(f32)
    unit1, spread1, _ = normalize(inputs, norm1_gain, norm1_shift)
    local_width = query_weight.shape[1]
    heads_here = local_width // HD
    unit_count = fc1_weight.shape[0]
    by_tp = lambda bias: bias.reshape(tp_count, 1, local_width)
    pair_width = 2 * local_width
    mlp_own = jnp.stack([fc1_weight, fc2_weight])
    query, pairs, normed, attention_w, mlp_w, out_parts = project(
        fsdp_count,
        tp_count,
        inputs,
        norm1_gain.reshape(1, -1),
        norm1_shift.reshape(1, -1),
        pack_columns(key_weight, value_weight, query_weight)[None],
        pack_columns(jnp.zeros((tp_count, 1, local_width), f32), by_tp(value_bias), by_tp(query_bias)),
        mlp_own,
        out_weight,
        pair_width,
        margin,
    )
    attention_w = attention_w[0]
    spread, context, wide, mlp_other, out_full = attend(
        fsdp_count, tp_count, clip_lengths, query, pairs, mlp_own, out_parts, heads_here
    )
    totals = -jnp.sum(wide[:, :, HD + 1 : HD + 4].astype(f32), axis=2)
    query = query[:, :local_width]
    normed = normed.reshape(group_rows, -1)
    key_w, value_w = jnp.moveaxis(attention_w[:, :pair_width].reshape(-1, heads_here, 2, HD), 2, 0)
    key_w = key_w.reshape(-1, local_width)
    value_w = value_w.reshape(-1, local_width)
    query_w = attention_w[:, pair_width : pair_width + local_width]
    padded = jnp.moveaxis(pairs.reshape(-1, heads_here, 2, HD), 2, 0).reshape(2, -1, local_width)
    out_w = lax.dynamic_index_in_dim(out_full, tp_index, 0, False)
    w_up, w_down = mlp_w
    group_base = fsdp_index * group_rows
    clip_ids = jnp.arange(clip_lengths.shape[0])
    block_count = group_rows // QB

    def block_scores(block_index):
        first_row = block_index * QB
        clip_index = (group_base + first_row) // CLIP
        key_start = clip_index * CLIP - group_base + margin
        length = jnp.sum(jnp.where(clip_ids == clip_index, clip_lengths, 0))
        query_block = lax.dynamic_slice_in_dim(query, first_row, QB, 0).reshape(QB, heads_here, HD)
        pair = lax.dynamic_slice_in_dim(padded, key_start, CLIP, 1).reshape(2, CLIP, heads_here, HD)
        scores = (
            jnp.einsum("qhe,khe->hqk", query_block, pair[0], preferred_element_type=f32)
            * score_scale
        )
        scores = jnp.where((jnp.arange(CLIP) < length)[None, None, :], scores, far_negative)
        return (first_row, key_start, query_block, pair[0], pair[1], scores)

    unit_bias = jnp.swapaxes(fc1_bias.reshape(fsdp_count, tp_count, unit_count), 0, 1)
    dhidden, outputs, mixed, dspread, own_grad, mate_grad, heads_grad, bias_part, sums = by_rows(
        fsdp_count,
        tp_count,
        inputs,
        spread,
        out_full,
        jnp.stack([out_bias, norm2_gain, norm2_shift, fc2_bias]),
        unit_bias.reshape(tp_count, -1, 1, 256),
        mlp_w,
        mlp_other,
        out_cotangent,
    )
    outputs = outputs + lax.ppermute(
        mixed, "tp", [(i, i ^ 1) for i in range(tp_count)]
    ).astype(f32)
    halves = [(i, (i + tp_count // 2) % tp_count) for i in range(tp_count)]
    grad_both = lax.psum_scatter(
        jnp.concatenate([*own_grad, *mate_grad], axis=1),
        "fsdp",
        scatter_dimension=0,
        tiled=True,
    )
    grad_own, grad_mate = jnp.split(grad_both, 2, axis=1)
    grad_own = grad_own.astype(f32) + lax.ppermute(grad_mate, "tp", halves).astype(f32)
    grad_fc1, grad_fc2 = jnp.split(grad_own, 2, axis=1)
    grad_out = lax.psum_scatter(heads_grad, "fsdp", scatter_dimension=1, tiled=True)
    grad_out = lax.psum_scatter(grad_out, "tp", scatter_dimension=0, tiled=True)[0].astype(f32)
    grad_gain2, grad_shift2, grad_obias, grad_b2 = sums
    mate_index = (tp_index + tp_count // 2) % tp_count
    mate_slot = (jnp.arange(tp_count) == mate_index).astype(f32)
    bias_part = bias_part.reshape(2, -1)
    by_tp_sum = tp_slot[:, None] * bias_part[0] + mate_slot[:, None] * bias_part[1]
    grad_b1 = jnp.swapaxes(by_tp_sum.reshape(tp_count, fsdp_count, unit_count), 0, 1).reshape(-1)
    dcontext = lax.all_to_all(dspread, "tp", 0, 0, tiled=False).reshape(group_rows, local_width)
    delta = jnp.sum(
        (dcontext.astype(f32) * context.astype(f32)).reshape(group_rows, heads_here, HD), axis=-1
    ).T

    def attend_back(block_index, carry):
        dquery_rows, dpair = carry
        first_row, key_start, query_block, key_block, value_block, scores = block_scores(
            block_index
        )
        grad_block = lax.dynamic_slice_in_dim(dcontext, first_row, QB, 0).reshape(
            QB, heads_here, HD
        )
        probs = jnp.exp(scores - lax.dynamic_slice_in_dim(totals, first_row, QB, 1)[..., None])
        delta_block = lax.dynamic_slice_in_dim(delta, first_row, QB, 1)
        dprobs = jnp.einsum("qhe,khe->hqk", grad_block, value_block, preferred_element_type=f32)
        dscores = (probs * (dprobs - delta_block[..., None]) * score_scale).astype(bf16)
        dquery_block = jnp.einsum("hqk,khe->qhe", dscores, key_block, preferred_element_type=f32)
        dquery_block = dquery_block.astype(bf16).reshape(QB, local_width)
        dkey_block = jnp.einsum(
            "hqk,qhe->khe", dscores, query_block, preferred_element_type=f32
        ).reshape(CLIP, local_width)
        dvalue_block = jnp.einsum(
            "hqk,qhe->khe", probs.astype(bf16), grad_block, preferred_element_type=f32
        ).reshape(CLIP, local_width)
        current = lax.dynamic_slice_in_dim(dpair, key_start, CLIP, 1)
        dpair = lax.dynamic_update_slice_in_dim(
            dpair, current + jnp.stack([dkey_block, dvalue_block]), key_start, 1
        )
        dquery_rows = lax.dynamic_update_slice_in_dim(dquery_rows, dquery_block, first_row, 0)
        return (dquery_rows, dpair)

    dquery, dpair = lax.fori_loop(
        0,
        block_count,
        attend_back,
        (jnp.zeros((group_rows, local_width), bf16), jnp.zeros(padded.shape, f32)),
    )
    rims = jnp.concatenate([dpair[:, :margin], dpair[:, margin + group_rows :]], axis=1)
    received = extended(rims, (("fsdp", 1),), margin)
    inner_part = dpair[:, margin : margin + group_rows]
    inner_part = inner_part.at[:, :margin].add(received[:, :margin])
    inner_part = inner_part.at[:, group_rows - margin :].add(received[:, 3 * margin :])
    dkey = inner_part[0].astype(bf16)
    dvalue = inner_part[1].astype(bf16)
    grad_query = contract_rows(normed, dquery)
    grad_key = contract_rows(normed, dkey)
    grad_value = contract_rows(normed, dvalue)
    grad_qbias = (tp_slot[:, None] * jnp.sum(dquery.astype(f32), axis=0)[None, :]).reshape(-1)
    grad_vbias = (tp_slot[:, None] * jnp.sum(dvalue.astype(f32), axis=0)[None, :]).reshape(-1)
    dnorm1 = scatter_rows(
        contract_cols(dquery, query_w)
        + contract_cols(dkey, key_w)
        + contract_cols(dvalue, value_w),
        "tp",
    )
    grad_gain1 = jnp.sum(dnorm1 * unit1, axis=0)
    grad_shift1 = jnp.sum(dnorm1, axis=0)
    inputs_grad = dhidden + norm_back(dnorm1, unit1, spread1, norm1_gain)
    grad_query, grad_key, grad_value = jnp.split(
        scatter_rows(jnp.concatenate([grad_query, grad_key, grad_value], axis=1), "fsdp"),
        3,
        axis=1,
    )
    (
        grad_gain1,
        grad_shift1,
        grad_qbias,
        grad_vbias,
        grad_obias,
        grad_gain2,
        grad_shift2,
        grad_b1,
        grad_b2,
    ) = lax.psum(
        (
            grad_gain1,
            grad_shift1,
            grad_qbias,
            grad_vbias,
            grad_obias,
            grad_gain2,
            grad_shift2,
            grad_b1,
            grad_b2,
        ),
        ("fsdp", "tp"),
    )
    return (
        outputs,
        inputs_grad,
        grad_gain1,
        grad_shift1,
        grad_query,
        grad_qbias,
        grad_key,
        grad_value,
        grad_vbias,
        grad_out,
        grad_obias,
        grad_gain2,
        grad_shift2,
        grad_fc1,
        grad_b1,
        grad_fc2,
        grad_b2,
    )


def solution(mesh):
    in_specs = (
        P(("fsdp", "tp"), None),
        P("fsdp", None),
        P(),
        P(),
        P(),
        P("fsdp", "tp"),
        P(),
        P("fsdp", "tp"),
        P("fsdp", "tp"),
        P(),
        P("fsdp", "tp"),
        P(),
        P(),
        P(),
        P(("fsdp", "tp"), None),
        P(),
        P(("fsdp", "tp"), None),
        P(),
    )
    out_specs = (
        P(("fsdp", "tp"), None),
        P(("fsdp", "tp"), None),
        P(),
        P(),
        P("fsdp", "tp"),
        P(),
        P("fsdp", "tp"),
        P("fsdp", "tp"),
        P(),
        P("fsdp", "tp"),
        P(),
        P(),
        P(),
        P(("fsdp", "tp"), None),
        P(),
        P(("fsdp", "tp"), None),
        P(),
    )
    return jax.shard_map(
        on_device, mesh=mesh, in_specs=in_specs, out_specs=out_specs, check_vma=False
    )
```

```python
import functools
import math

import jax
import jax.numpy as jnp
from jax import lax
from jax.experimental import pallas as pl
from jax.experimental.pallas import tpu as pltpu
from jax.sharding import PartitionSpec as P

HD = 64
CLIP = 1536
QB = 512


eps_norm = 1e-05
root_half = 0.7071067811865476
inv_root_tau = 0.3989422804014327
far_negative = -1e30


def extended(value, sides, width):
    for axis, dim in sides:
        size, length = (lax.axis_size(axis), value.shape[dim])
        up = [(i, (i + 1) % size) for i in range(size - 1)]
        down = [(j, i) for i, j in up]
        last = lax.slice_in_dim(value, length - width, length, axis=dim)
        initial = lax.slice_in_dim(value, 0, width, axis=dim)
        before = lax.ppermute(last, axis, up)
        after = lax.ppermute(initial, axis, down)
        value = jnp.concatenate([before, value, after], axis=dim)
    return value


def normalize(rows, gain, shift):
    centre = jnp.mean(rows, axis=-1, keepdims=True)
    centred = rows - centre
    inv_spread = lax.rsqrt(jnp.mean(centred * centred, axis=-1, keepdims=True) + eps_norm)
    unit_rows = centred * inv_spread
    return (unit_rows, inv_spread, unit_rows * gain + shift)


def norm_back(upstream, unit_rows, inv_spread, gain):
    scaled = upstream * gain
    return inv_spread * (
        scaled
        - jnp.mean(scaled, axis=-1, keepdims=True)
        - unit_rows * jnp.mean(scaled * unit_rows, axis=-1, keepdims=True)
    )


def gelu_exact(values):
    return 0.5 * values * (1.0 + lax.erf(values * root_half))


def gelu_slope(values):
    return (
        0.5 * (1.0 + lax.erf(values * root_half))
        + values * jnp.exp(-0.5 * values * values) * inv_root_tau
    )


def contract_rows(left_rows, right_rows):
    return lax.dot_general(
        left_rows, right_rows, (((0,), (0,)), ((), ())), preferred_element_type=jnp.float32
    )


def contract_cols(left_rows, right_rows):
    return lax.dot_general(
        left_rows, right_rows, (((1,), (1,)), ((), ())), preferred_element_type=jnp.float32
    )


def scatter_rows(partial_rows, axis):
    return lax.psum_scatter(
        partial_rows.astype(jnp.bfloat16), axis, scatter_dimension=0, tiled=True
    ).astype(jnp.float32)


MESH = pl.DeviceIdType.MESH
VMEM_LIMIT = 60 * 1024 * 1024
LANES = 128


def remote(source, target, send_sem, recv_sem, fsdp_to, tp_to):
    return pltpu.make_async_remote_copy(
        src_ref=source,
        dst_ref=target,
        send_sem=send_sem,
        recv_sem=recv_sem,
        device_id=(fsdp_to, tp_to),
        device_id_type=MESH,
    )


def greet(fsdp_count, tp_count, f, t):
    barrier = pltpu.get_barrier_semaphore()

    def greet_fsdp(i, carry):
        pl.semaphore_signal(
            barrier, inc=1, device_id=(lax.rem(f + i, fsdp_count), t), device_id_type=MESH
        )
        return carry

    def greet_tp(j, carry):
        pl.semaphore_signal(
            barrier, inc=1, device_id=(f, lax.rem(t + j, tp_count)), device_id_type=MESH
        )
        return carry

    lax.fori_loop(1, fsdp_count, greet_fsdp, 0)
    lax.fori_loop(1, tp_count, greet_tp, 0)
    pl.semaphore_wait(barrier, fsdp_count + tp_count - 2)


def gather_copies(f, t, fsdp_count, sources, targets, depth, sends, recvs):
    partner = f + 1 - 2 * lax.rem(f, 2)

    def piece(target, owner):
        return target.at[:, pl.ds(owner * depth, depth)]

    def copies(owner, toward, lane, first):
        return [
            remote(
                source if first else piece(target, owner),
                piece(target, owner),
                send.at[lane],
                recv.at[owner],
                toward,
                t,
            )
            for source, target, send, recv in zip(sources, targets, sends, recvs)
        ]

    def start():
        def body(i, carry):
            for handle in copies(f, lax.rem(f + 2 * i, fsdp_count), i, True):
                handle.start()
            return carry

        lax.fori_loop(1, fsdp_count // 2, body, 0)
        for handle in copies(f, partner, 0, True):
            handle.start()
        for source, target in zip(sources, targets):
            target[:, pl.ds(f * depth, depth), :] = source[...]

    def relay():
        def body(i, carry):
            owner = lax.rem(f + fsdp_count - 2 * i, fsdp_count)
            for handle in copies(owner, partner, fsdp_count // 2 + i, False):
                handle.wait_recv()
                handle.start()
            return carry

        lax.fori_loop(1, fsdp_count // 2, body, 0)

    def finish():
        def body(i, carry):
            owner = lax.rem(partner + 2 * i, fsdp_count)
            for handle in copies(owner, partner, 0, False):
                handle.wait_recv()
            return carry

        lax.fori_loop(0, fsdp_count // 2, body, 0)

    def drain():
        def body(i, carry):
            for handle in copies(f, lax.rem(f + 2 * i, fsdp_count), i, True):
                handle.wait_send()
            for handle in copies(
                lax.rem(f + fsdp_count - 2 * i, fsdp_count),
                partner,
                fsdp_count // 2 + i,
                False,
            ):
                handle.wait_send()
            return carry

        lax.fori_loop(1, fsdp_count // 2, body, 0)
        for handle in copies(f, partner, 0, True):
            handle.wait_send()

    return (start, relay, finish, drain)


def project_kernel(
    fsdp_count,
    tp_count,
    x_ref,
    gain_ref,
    shift_ref,
    weight_ref,
    bias_ref,
    mlp_ref,
    out_ref,
    query_ref,
    pair_ref,
    normed_ref,
    full_ref,
    mlp_full,
    heads_ref,
    side_send,
    side_recv,
    weight_send,
    weight_recv,
    mlp_send,
    mlp_recv,
    row_send,
    row_recv,
    halo_send,
    halo_recv,
):
    f = lax.axis_index("fsdp")
    t = lax.axis_index("tp")
    rows = x_ref.shape[0]
    depth = weight_ref.shape[1]
    group = rows * tp_count
    pair_width = pair_ref.shape[1]
    margin = (pair_ref.shape[0] - group) // 2
    per_half = tp_count // 2
    phase = lax.rem(f, 3)
    above = f + 1 < fsdp_count
    below = f > 0
    blank = jnp.zeros((256, pair_width), jnp.bfloat16)

    def clear(i, carry):
        pair_ref[pl.ds(i * 256, 256), :] = blank
        pair_ref[pl.ds(margin + group + i * 256, 256), :] = blank
        return carry

    lax.fori_loop(0, margin // 256, clear, 0)
    greet(fsdp_count, tp_count, f, t)
    start_weights, relay_weights, finish_weights, drain_weights = gather_copies(
        f, t, fsdp_count, (weight_ref,), (full_ref,), depth, (weight_send,), (weight_recv,)
    )
    start_mlp, relay_mlp, finish_mlp, drain_mlp = gather_copies(
        f, t, fsdp_count, (mlp_ref,), (mlp_full,), depth, (mlp_send,), (mlp_recv,)
    )
    start_weights()
    _, _, normed = normalize(x_ref[...], gain_ref[...], shift_ref[...])
    normed_ref[t] = normed.astype(jnp.bfloat16)

    def row_copy(source, lane, toward):
        return remote(
            normed_ref.at[source],
            normed_ref.at[source],
            row_send.at[lane],
            row_recv.at[source],
            f,
            toward,
        )

    @pl.when(t > 0)
    def _():
        row_copy(t, tp_count, t - 1).start()

    @pl.when(t < tp_count - 1)
    def _():
        row_copy(t, tp_count + 1, t + 1).start()

    def heads_copy(j):
        return remote(
            out_ref,
            heads_ref.at[t],
            side_send.at[j],
            side_recv.at[j],
            f,
            lax.rem(t + j, tp_count),
        )

    def heads_start(j, carry):
        heads_copy(j).start()
        return carry

    def heads_done(j, carry):
        heads_copy(j).wait_send()
        source = lax.rem(t + tp_count - j, tp_count)
        remote(
            out_ref, heads_ref.at[source], side_send.at[j], side_recv.at[j], f, source
        ).wait_recv()
        return carry

    heads_ref[t] = out_ref[...]
    lax.fori_loop(1, tp_count, heads_start, 0)
    relay_weights()
    start_mlp()
    finish_weights()

    def halo_copy(source, side):
        return remote(
            pair_ref.at[pl.ds(margin + source * rows, rows)],
            pair_ref.at[pl.ds((0 if side == 0 else margin + group) + source * rows, rows)],
            halo_send.at[side, source],
            halo_recv.at[side, source],
            f + 1 if side == 0 else f - 1,
            t,
        )

    def halo_sends(source):
        late = source >= per_half
        return (
            above & ((phase == 0) | ((phase == 1) & late)),
            below & ((phase == 2) | ((phase == 1) & jnp.logical_not(late))),
        )

    def halo_receives(source):
        late = source >= per_half
        return (
            below & ((phase == 1) | ((phase == 2) & late)),
            above & ((phase == 1) | ((phase == 0) & jnp.logical_not(late))),
        )

    def compute(source):
        out = jnp.dot(normed_ref[source], full_ref[0], preferred_element_type=jnp.float32)
        out = (out + bias_ref[t]).astype(jnp.bfloat16)
        pair_ref[pl.ds(margin + source * rows, rows), :] = out[:, :pair_width]
        for side, needed in enumerate(halo_sends(source)):

            @pl.when(needed)
            def _(side=side):
                halo_copy(source, side).start()

        query_ref[pl.ds(source * rows, rows), :] = out[:, pair_width:]

    compute(t)

    def arrival(k):
        step = k // 2 + 1
        side = 2 * lax.rem(k, 2) - 1
        source = t + side * step
        onward = t - side
        valid = (source >= 0) & (source < tp_count)
        return (source, onward, valid, valid & (onward >= 0) & (onward < tp_count))

    def receive(k, carry):
        source, onward, valid, forward = arrival(k)

        @pl.when(valid)
        def _():
            row_copy(source, 0, t).wait_recv()

            @pl.when(forward)
            def _():
                row_copy(source, source, onward).start()

            compute(source)

        return carry

    lax.fori_loop(0, 2 * (tp_count - 1), receive, 0)
    relay_mlp()
    lax.fori_loop(1, tp_count, heads_done, 0)

    def sent(k, carry):
        source, onward, valid, forward = arrival(k)

        @pl.when(forward)
        def _():
            row_copy(source, source, onward).wait_send()

        return carry

    lax.fori_loop(0, 2 * (tp_count - 1), sent, 0)

    @pl.when(t > 0)
    def _():
        row_copy(t, tp_count, t - 1).wait_send()

    @pl.when(t < tp_count - 1)
    def _():
        row_copy(t, tp_count + 1, t + 1).wait_send()

    def halo_done(source, carry):
        for side, (sends, receives) in enumerate(zip(halo_sends(source), halo_receives(source))):

            @pl.when(sends)
            def _(side=side):
                halo_copy(source, side).wait_send()

            @pl.when(receives)
            def _(side=side):
                halo_copy(source, side).wait_recv()

        return carry

    lax.fori_loop(0, tp_count, halo_done, 0)
    drain_weights()
    finish_mlp()
    drain_mlp()


def whole_specs(count):
    return [pl.BlockSpec(memory_space=pltpu.VMEM)] * count


def project(fsdp_count, tp_count, x, gain, shift, weights, bias, mlp, out_weight, pair_width, margin):
    bf16 = jnp.bfloat16
    rows, features = x.shape
    group = rows * tp_count
    depth = weights.shape[1]
    dma = pltpu.SemaphoreType.DMA
    return pl.pallas_call(
        functools.partial(project_kernel, fsdp_count, tp_count),
        out_shape=(
            jax.ShapeDtypeStruct((group, weights.shape[2] - pair_width), bf16),
            jax.ShapeDtypeStruct((group + 2 * margin, pair_width), bf16),
            jax.ShapeDtypeStruct((tp_count, rows, features), bf16),
            jax.ShapeDtypeStruct((1, depth * fsdp_count, weights.shape[2]), bf16),
            jax.ShapeDtypeStruct((2, depth * fsdp_count, features), bf16),
            jax.ShapeDtypeStruct((tp_count, *out_weight.shape), bf16),
        ),
        in_specs=whole_specs(7),
        out_specs=tuple(whole_specs(6)),
        scratch_shapes=[
            dma((tp_count,)),
            dma((tp_count,)),
            dma((fsdp_count,)),
            dma((fsdp_count,)),
            dma((fsdp_count,)),
            dma((fsdp_count,)),
            dma((tp_count + 2,)),
            dma((tp_count,)),
            dma((2, tp_count)),
            dma((2, tp_count)),
        ],
        compiler_params=pltpu.CompilerParams(
            collective_id=1, has_side_effects=True, vmem_limit_bytes=VMEM_LIMIT
        ),
        name="project",
    )(x, gain, shift, weights, bias, mlp, out_weight)


def block_clip(f, part, margin):
    phase = lax.rem(f, 3)
    start = jnp.where(
        phase == 0,
        margin,
        jnp.where(phase == 2, margin - QB, jnp.where(part == 0, 0, margin + QB)),
    )
    return (pl.multiple_of(start, QB), (2 * f + part) // 3)


def head_tiles(pair, length):
    lane = lax.broadcasted_iota(jnp.int32, pair.shape, 1)
    row = lax.broadcasted_iota(jnp.int32, pair.shape, 0)
    extra = jnp.where(
        lane == HD,
        jnp.where(row < length, 0.0, far_negative),
        jnp.where(lane <= HD + 3, 1.0, 0.0),
    )
    return jnp.where(lane < HD, pair, extra)


def spread_heads(rows, head):
    tile = rows[:, (head // 2) * LANES : (head // 2 + 1) * LANES]
    return pltpu.roll(tile, HD, axis=1) if head % 2 else tile


def three_parts(column):
    high = column.astype(jnp.bfloat16).astype(jnp.float32)
    rest = column - high
    middle = rest.astype(jnp.bfloat16).astype(jnp.float32)
    return (high, middle, rest - middle)


def attend_kernel(
    fsdp_count,
    tp_count,
    lengths_ref,
    query_ref,
    pair_ref,
    mlp_ref,
    out_ref,
    spread_ref,
    context_ref,
    wide_ref,
    mlp_full,
    out_full,
    mate_ref,
    key_tiles,
    value_tiles,
    mate_send,
    mate_recv,
    context_send,
    context_recv,
    mlp_send,
    mlp_recv,
    out_send,
    out_recv,
):
    f = lax.axis_index("fsdp")
    t = lax.axis_index("tp")
    bf16 = jnp.bfloat16
    f32 = jnp.float32
    rows = spread_ref.shape[1]
    heads = wide_ref.shape[0]
    group = rows * tp_count
    margin = (pair_ref.shape[0] - group) // 2
    greet(fsdp_count, tp_count, f, t)
    depth = mlp_ref.shape[1]
    start_out, relay_out, finish_out, drain_out = gather_copies(
        f, t, fsdp_count, (out_ref,), (out_full,), depth, (out_send,), (out_recv,)
    )
    start_mlp, relay_mlp, finish_mlp, drain_mlp = gather_copies(
        f, t, fsdp_count, (mate_ref,), (mlp_full,), depth, (mlp_send,), (mlp_recv,)
    )
    mate_copy = remote(
        mlp_ref, mate_ref, mate_send, mate_recv, f, lax.rem(t + tp_count // 2, tp_count)
    )
    mate_copy.start()
    start_out()
    per_half = tp_count // 2

    def context_copy(toward):
        return remote(
            context_ref.at[pl.ds(toward * rows, rows)],
            spread_ref.at[t],
            context_send.at[toward],
            context_recv.at[t],
            f,
            toward,
        )

    lane = lax.broadcasted_iota(jnp.int32, (rows, LANES), 1)
    row = lax.broadcasted_iota(jnp.int32, (LANES, rows), 0)
    tall = lax.broadcasted_iota(jnp.int32, (LANES, CLIP), 0)

    def half(step, carry):
        part = lax.rem(t // per_half + 1 + step, 2)
        first, clip = block_clip(f, part, margin)
        length = lengths_ref[clip]
        for head in range(heads):
            pair = pair_ref[pl.ds(first, CLIP), head * LANES : (head + 1) * LANES].astype(f32)
            key_tiles[head] = head_tiles(pair, length).astype(bf16)
            value_tiles[head] = jnp.where(tall < HD, 1.0, pair.T).astype(bf16)

        def block(i, inner):
            within = lax.rem(lax.rem(t, per_half) + 1 + i, per_half)
            index = part * per_half + within
            here = pl.ds(pl.multiple_of(index * rows, rows), rows)
            query = query_ref[here, :].astype(f32) * (1.0 / math.sqrt(HD))
            parts = []
            for head in range(heads):
                wide = jnp.where(
                    lane < HD, spread_heads(query, head), jnp.where(lane == HD, 1.0, 0.0)
                )
                scores = lax.dot_general(
                    key_tiles[head],
                    wide.astype(bf16),
                    (((1,), (1,)), ((), ())),
                    preferred_element_type=f32,
                )
                highest = jnp.max(scores, axis=0, keepdims=True)
                weights = jnp.exp(scores - highest).astype(bf16)
                summed = jnp.dot(value_tiles[head], weights, preferred_element_type=f32)
                total = summed[0:1, :]
                log_total = highest + jnp.log(total)
                turned = jnp.where(row == 0, log_total, summed * (1.0 / total)).T
                high, middle, low = three_parts(turned[:, 0:1])
                wide_ref[head, here, :] = jnp.where(
                    lane == HD + 1,
                    -high,
                    jnp.where(lane == HD + 2, -middle, jnp.where(lane == HD + 3, -low, wide)),
                ).astype(bf16)
                parts.append(turned)
            context_ref[here, 0:LANES] = jnp.where(
                lane < HD, pltpu.roll(parts[0], HD, axis=1), parts[1]
            ).astype(bf16)
            context_ref[here, LANES : LANES + HD] = pltpu.roll(parts[2], HD, axis=1)[
                :, :HD
            ].astype(bf16)

            @pl.when(index == t)
            def _():
                spread_ref[t] = context_ref[here, :]

            @pl.when(index != t)
            def _():
                context_copy(index).start()

            return inner

        lax.fori_loop(0, per_half, block, 0)

        @pl.when(step == 0)
        def _():
            mate_copy.wait()
            start_mlp()
            relay_out()

        return carry

    lax.fori_loop(0, 2, half, 0)
    relay_mlp()

    def settle(j, carry):
        toward = lax.rem(t + j, tp_count)
        context_copy(toward).wait_send()
        remote(
            context_ref.at[pl.ds(0, rows)],
            spread_ref.at[toward],
            context_send.at[toward],
            context_recv.at[toward],
            f,
            toward,
        ).wait_recv()
        return carry

    lax.fori_loop(1, tp_count, settle, 0)
    finish_out()
    finish_mlp()
    drain_out()
    drain_mlp()


def attend(fsdp_count, tp_count, lengths, query, pairs, mlp, out_weights, heads):
    bf16 = jnp.bfloat16
    group = query.shape[0]
    rows = group // tp_count
    width = heads * HD
    dma = pltpu.SemaphoreType.DMA
    depth = mlp.shape[1]
    return pl.pallas_call(
        functools.partial(attend_kernel, fsdp_count, tp_count),
        out_shape=(
            jax.ShapeDtypeStruct((tp_count, rows, width), bf16),
            jax.ShapeDtypeStruct((group, width), bf16),
            jax.ShapeDtypeStruct((heads, group, LANES), bf16),
            jax.ShapeDtypeStruct((mlp.shape[0], depth * fsdp_count, mlp.shape[2]), bf16),
            jax.ShapeDtypeStruct((tp_count, depth * fsdp_count, width), bf16),
        ),
        in_specs=[pl.BlockSpec(memory_space=pltpu.SMEM)] + whole_specs(4),
        out_specs=tuple(whole_specs(5)),
        scratch_shapes=[
            pltpu.VMEM(mlp.shape, bf16),
            pltpu.VMEM((heads, CLIP, LANES), bf16),
            pltpu.VMEM((heads, LANES, CLIP), bf16),
            dma,
            dma,
            dma((tp_count,)),
            dma((tp_count,)),
            dma((fsdp_count,)),
            dma((fsdp_count,)),
            dma((fsdp_count,)),
            dma((fsdp_count,)),
        ],
        compiler_params=pltpu.CompilerParams(
            collective_id=2, has_side_effects=True, vmem_limit_bytes=VMEM_LIMIT
        ),
        name="attend",
    )(lengths, query, pairs, mlp, out_weights)


def column_sum(rows):
    return jnp.sum(rows, axis=0, keepdims=True)


def rows_kernel(
    fsdp_count,
    tp_count,
    x_ref,
    spread_ref,
    heads_ref,
    vector_ref,
    bias_ref,
    own_ref,
    mate_ref,
    cotangent_ref,
    gradient_ref,
    outputs_ref,
    mixed_ref,
    context_ref,
    mlp_grad,
    heads_grad,
    bias_grad,
    sums_ref,
    upstream,
    rounded,
    hidden_ref,
    unit_ref,
    normed_ref,
    active_ref,
    slope_ref,
    mixed_sum,
    norm_sum,
    norm_out,
    norm_in,
    load_sem,
    row_send,
    row_recv,
    norm_send,
    norm_recv,
):
    f = lax.axis_index("fsdp")
    t = lax.axis_index("tp")
    bf16 = jnp.bfloat16
    f32 = jnp.float32
    rows = x_ref.shape[0]
    tile = 256
    side = lax.rem(t, 2)
    peer = t + 1 - 2 * side
    load = pltpu.make_async_copy(
        cotangent_ref.at[pl.ds((t - side) * rows, 2 * rows)], upstream, load_sem
    )
    load.start()
    barrier = pltpu.get_barrier_semaphore()
    pl.semaphore_signal(barrier, inc=1, device_id=(f, peer), device_id_type=MESH)
    pl.semaphore_wait(barrier, 1)

    hidden = x_ref[...] + vector_ref[0:1, :]
    for j in range(tp_count):
        hidden = hidden + lax.dot_general(
            spread_ref[j], heads_ref[j], (((1,), (1,)), ((), ())), preferred_element_type=f32
        )
    hidden_ref[...] = hidden
    unit, spread, normed = normalize(hidden, vector_ref[1:2, :], vector_ref[2:3, :])
    unit_ref[...] = unit
    normed_ref[side] = normed.astype(bf16)
    row_copy = remote(normed_ref.at[side], normed_ref.at[side], row_send, row_recv, f, peer)
    row_copy.start()
    load.wait()

    def rounding(i, carry):
        rounded[pl.ds(i * rows, rows), :] = upstream[pl.ds(i * rows, rows), :].astype(bf16)
        return carry

    lax.fori_loop(0, 2, rounding, 0)
    mixed_sum[...] = jnp.zeros(mixed_sum.shape, f32)
    norm_sum[...] = jnp.zeros(norm_sum.shape, f32)
    chunks = own_ref.shape[1] // tile
    mate = lax.rem(t + tp_count // 2, tp_count)

    def feed_forward(turn, carry):
        which = lax.rem(side + turn, 2)

        @pl.when(turn == 1)
        def _():
            row_copy.wait_recv()

        here = pl.ds(pl.multiple_of(which * rows, rows), rows)
        normed_rows = normed_ref[which]
        upstream_rows = rounded[here, :]

        for level, (weights, owner) in enumerate(((own_ref, t), (mate_ref, mate))):

            def chunk(c, inner, weights=weights, owner=owner, level=level):
                units = pl.ds(pl.multiple_of(c * tile, tile), tile)
                up = weights[0, units, :]
                down = weights[1, units, :]
                preact = (
                    lax.dot_general(
                        normed_rows, up, (((1,), (1,)), ((), ())), preferred_element_type=f32
                    )
                    + bias_ref[owner, c]
                )
                cdf = 0.5 * (1.0 + lax.erf(preact * root_half))
                active = (preact * cdf).astype(bf16)
                slope = cdf + preact * jnp.exp(-0.5 * preact * preact) * inv_root_tau
                dactive = lax.dot_general(
                    upstream_rows, down, (((1,), (1,)), ((), ())), preferred_element_type=f32
                )
                dpreact = (dactive * slope).astype(bf16)
                active_ref[level, c, here, :] = active
                slope_ref[level, c, here, :] = dpreact
                norm_sum[which] += jnp.dot(dpreact, up, preferred_element_type=f32)
                mixed_sum[which] += jnp.dot(active, down, preferred_element_type=f32)
                return inner

            lax.fori_loop(0, chunks, chunk, 0)
        return carry

    lax.fori_loop(0, 2, feed_forward, 0)
    norm_out[...] = norm_sum[1 - side].astype(bf16)
    norm_copy = remote(norm_out, norm_in, norm_send, norm_recv, f, peer)
    norm_copy.start()
    mixed_ref[...] = mixed_sum[1 - side].astype(bf16)
    outputs_ref[...] = hidden_ref[...] + mixed_sum[side] + vector_ref[3:4, :]

    for level in range(2):

        def weight_grads(c, carry, level=level):
            units = pl.ds(pl.multiple_of(c * tile, tile), tile)
            slopes = slope_ref[level, c]
            both = jnp.concatenate([normed_ref[0], normed_ref[1]], axis=0)
            mlp_grad[2 * level, units, :] = contract_rows(slopes, both).astype(bf16)
            mlp_grad[2 * level + 1, units, :] = contract_rows(active_ref[level, c], rounded[...]).astype(bf16)
            bias_grad[level, c] = column_sum(slopes.astype(f32))
            return carry

        lax.fori_loop(0, chunks, weight_grads, 0)

    norm_copy.wait()
    dnorm = norm_sum[side] + norm_in[...].astype(f32)
    unit = unit_ref[...]
    cotangent = upstream[pl.ds(pl.multiple_of(side * rows, rows), rows), :]
    gradient = cotangent + norm_back(dnorm, unit, spread, vector_ref[1:2, :])
    gradient_ref[...] = gradient
    sums_ref[0:1, :] = column_sum(dnorm * unit)
    sums_ref[1:2, :] = column_sum(dnorm)
    sums_ref[2:3, :] = column_sum(gradient)
    sums_ref[3:4, :] = column_sum(cotangent)
    gradient = gradient.astype(bf16)
    for j in range(tp_count):
        context_ref[j] = jnp.dot(gradient, heads_ref[j], preferred_element_type=f32).astype(bf16)
        heads_grad[j] = contract_rows(gradient, spread_ref[j]).astype(bf16)
    row_copy.wait_send()


def by_rows(fsdp_count, tp_count, x, spread, heads, vectors, bias, own, mate, cotangent):
    bf16 = jnp.bfloat16
    f32 = jnp.float32
    rows, features = x.shape
    units = own.shape[1]
    chunks = units // 256
    dma = pltpu.SemaphoreType.DMA
    return pl.pallas_call(
        functools.partial(rows_kernel, fsdp_count, tp_count),
        out_shape=(
            jax.ShapeDtypeStruct((rows, features), f32),
            jax.ShapeDtypeStruct((rows, features), f32),
            jax.ShapeDtypeStruct((rows, features), bf16),
            jax.ShapeDtypeStruct(spread.shape, bf16),
            jax.ShapeDtypeStruct((4, units, features), bf16),
            jax.ShapeDtypeStruct(heads.shape, bf16),
            jax.ShapeDtypeStruct((2, chunks, 1, 256), f32),
            jax.ShapeDtypeStruct((4, features), f32),
        ),
        in_specs=whole_specs(7) + [pl.BlockSpec(memory_space=pl.ANY)],
        out_specs=tuple(whole_specs(8)),
        scratch_shapes=[
            pltpu.VMEM((2 * rows, features), f32),
            pltpu.VMEM((2 * rows, features), bf16),
            pltpu.VMEM((rows, features), f32),
            pltpu.VMEM((rows, features), f32),
            pltpu.VMEM((2, rows, features), bf16),
            pltpu.VMEM((2, chunks, 2 * rows, 256), bf16),
            pltpu.VMEM((2, chunks, 2 * rows, 256), bf16),
            pltpu.VMEM((2, rows, features), f32),
            pltpu.VMEM((2, rows, features), f32),
            pltpu.VMEM((rows, features), bf16),
            pltpu.VMEM((rows, features), bf16),
            dma,
            dma,
            dma,
            dma,
            dma,
        ],
        compiler_params=pltpu.CompilerParams(
            collective_id=4, has_side_effects=True, vmem_limit_bytes=VMEM_LIMIT
        ),
        name="by_rows",
    )(x, spread, heads, vectors, bias, own, mate, cotangent)


def margin_plan(f, fsdp_count, part):
    phase = lax.rem(f, 3)
    above = f + 1 < fsdp_count
    below = f > 0
    sends = (
        below & ((phase == 1) | ((phase == 2) & (part == 1))),
        above & ((phase == 1) | ((phase == 0) & (part == 0))),
    )
    receives = (
        above & ((phase == 0) | ((phase == 1) & (part == 1))),
        below & ((phase == 2) | ((phase == 1) & (part == 0))),
    )
    return (sends, receives)


def scatter_copies(f, t, fsdp_count, grads, firsts, seconds, one_send, one_recv, sends, recvs):
    parity = lax.rem(f, 2)
    partner = f + 1 - 2 * parity
    place = f // 2
    count = fsdp_count // 2

    def first_copies():
        return [
            remote(
                grad.at[:, :, 1 - parity], first, one_send.at[i], one_recv.at[i], partner, t
            )
            for i, (grad, first) in enumerate(zip(grads, firsts))
        ]

    def second_copies(i):
        toward = lax.rem(f + 2 * i, fsdp_count)
        return [
            remote(
                first.at[:, toward // 2],
                second.at[place],
                send.at[toward // 2],
                recv.at[place],
                toward,
                t,
            )
            for first, second, send, recv in zip(firsts, seconds, sends, recvs)
        ]

    def start():
        for handle in first_copies():
            handle.start()

    def add_first():
        for handle in first_copies():
            handle.wait_recv()
        for grad, first in zip(grads, firsts):

            def body(k, carry, grad=grad, first=first):
                i, j = (k // count, lax.rem(k, count))
                mine = grad[i, j, parity].astype(jnp.float32)
                first[i, j] = (mine + first[i, j].astype(jnp.float32)).astype(jnp.bfloat16)
                return carry

            lax.fori_loop(0, grad.shape[0] * count, body, 0)

        def send(i, carry):
            for handle in second_copies(i):
                handle.start()
            return carry

        lax.fori_loop(1, count, send, 0)

    def finish(totals):
        for first, total in zip(firsts, totals):
            total[...] = first[:, place].astype(jnp.float32)

        def body(i, carry):
            source = lax.rem(f + fsdp_count - 2 * i, fsdp_count)
            for first, second, send, recv, total in zip(firsts, seconds, sends, recvs, totals):
                remote(
                    first.at[:, place],
                    second.at[source // 2],
                    send.at[0],
                    recv.at[source // 2],
                    source,
                    t,
                ).wait_recv()
                total[...] += second[source // 2].astype(jnp.float32)
            return carry

        lax.fori_loop(1, count, body, 0)

        def drain(i, carry):
            for handle in second_copies(i):
                handle.wait_send()
            return carry

        lax.fori_loop(1, count, drain, 0)
        for handle in first_copies():
            handle.wait_send()

    return (start, add_first, finish)


def attend_back_kernel(
    fsdp_count,
    tp_count,
    lengths_ref,
    dspread_ref,
    wide_ref,
    pair_ref,
    context_ref,
    mlp_grad,
    heads_grad,
    mixed_ref,
    dproj_ref,
    mlp_total,
    heads_total,
    mixed_in,
    sums_ref,
    dcontext,
    key_tiles,
    value_tiles,
    turned_tiles,
    totals,
    halo_out,
    halo_in,
    mlp_first,
    mlp_second,
    heads_first,
    heads_second,
    context_send,
    context_recv,
    mixed_send,
    mixed_recv,
    halo_send,
    halo_recv,
    one_send,
    one_recv,
    mlp_send,
    mlp_recv,
    heads_send,
    heads_recv,
):
    f = lax.axis_index("fsdp")
    t = lax.axis_index("tp")
    bf16 = jnp.bfloat16
    f32 = jnp.float32
    rows = dspread_ref.shape[1]
    heads = wide_ref.shape[0]
    group = rows * tp_count
    margin = (pair_ref.shape[0] - group) // 2
    per_half = tp_count // 2
    pair_width = heads * LANES
    scale = 1.0 / math.sqrt(HD)
    greet(fsdp_count, tp_count, f, t)

    def context_copy(j):
        toward = lax.rem(t + j, tp_count)
        return remote(
            dspread_ref.at[toward],
            dcontext.at[t],
            context_send.at[j],
            context_recv.at[t],
            f,
            toward,
        )

    def context_start(j, carry):
        context_copy(j).start()
        return carry

    lax.fori_loop(1, tp_count, context_start, 0)
    start_grads, add_grads, finish_grads = scatter_copies(
        f,
        t,
        fsdp_count,
        (mlp_grad, heads_grad),
        (mlp_first, heads_first),
        (mlp_second, heads_second),
        one_send,
        one_recv,
        (mlp_send, heads_send),
        (mlp_recv, heads_recv),
    )
    start_grads()
    dcontext[t] = dspread_ref[t]
    mixed_copy = remote(
        mixed_ref, mixed_in, mixed_send, mixed_recv, f, t + 1 - 2 * lax.rem(t, 2)
    )

    def clear(i, carry):
        for head in range(heads):
            totals[head, pl.ds(i * QB, QB), :] = jnp.zeros((QB, LANES), f32)
        return carry

    lax.fori_loop(0, pair_ref.shape[0] // QB, clear, 0)
    add_grads()
    lane = lax.broadcasted_iota(jnp.int32, (rows, LANES), 1)
    tall = lax.broadcasted_iota(jnp.int32, (CLIP, LANES), 1)

    def half(step, carry):
        part = lax.rem(t // per_half + step, 2)
        first, clip = block_clip(f, part, margin)
        length = lengths_ref[clip]
        for head in range(heads):
            pair = pair_ref[pl.ds(first, CLIP), head * LANES : (head + 1) * LANES].astype(f32)
            key_tiles[head] = head_tiles(pair, length).astype(bf16)
            value_tiles[head] = jnp.where(
                tall < HD, jnp.where(tall < 3, 1.0, 0.0), pair
            ).astype(bf16)
            turned_tiles[head] = pair.T.astype(bf16)

        def block(i, inner):
            within = lax.rem(lax.rem(t, per_half) + i, per_half)
            index = part * per_half + within

            @pl.when(index != t)
            def _():
                remote(
                    dspread_ref.at[0],
                    dcontext.at[index],
                    context_send.at[0],
                    context_recv.at[index],
                    f,
                    index,
                ).wait_recv()

            here = pl.ds(pl.multiple_of(index * rows, rows), rows)
            empty = jnp.zeros((rows, HD), f32)

            def two_tiles(ref, at):
                return (
                    ref[at + (slice(0, LANES),)].astype(f32),
                    jnp.concatenate(
                        [ref[at + (slice(LANES, LANES + HD),)].astype(f32), empty], axis=1
                    ),
                )

            upstream = two_tiles(dcontext, (index, slice(None)))
            forward = two_tiles(context_ref, (here,))
            queries = []
            for head in range(heads):
                tile = upstream[head // 2]
                odd = head % 2
                kept = jnp.where((lane >= HD) if odd else (lane < HD), tile * forward[head // 2], 0.0)
                delta = jnp.sum(kept, axis=1, keepdims=True) * scale
                high, middle, low = three_parts(delta)
                grad = (tile if odd else pltpu.roll(tile, HD, axis=1)) * scale
                grad = jnp.where(
                    lane >= HD,
                    grad,
                    jnp.where(
                        lane == 0,
                        -high,
                        jnp.where(lane == 1, -middle, jnp.where(lane == 2, -low, 0.0)),
                    ),
                ).astype(bf16)
                wide = wide_ref[head, here, :]
                probs = jnp.exp(contract_cols(key_tiles[head], wide))
                dscores = (probs * contract_cols(value_tiles[head], grad)).astype(bf16)
                both = jnp.concatenate([dscores, probs.astype(bf16)], axis=1)
                fold = jnp.concatenate(
                    [
                        jnp.where(lane < HD, wide.astype(f32), 0.0),
                        jnp.where(lane < HD, 0.0, grad.astype(f32)),
                    ],
                    axis=0,
                ).astype(bf16)
                totals[head, pl.ds(first, CLIP), :] += jnp.dot(
                    both, fold, preferred_element_type=f32
                )
                queries.append(
                    jnp.dot(turned_tiles[head], dscores, preferred_element_type=f32).T
                )
            dproj_ref[here, pair_width : pair_width + LANES] = jnp.where(
                lane < HD, queries[0], pltpu.roll(queries[1], HD, axis=1)
            ).astype(bf16)
            dproj_ref[here, pair_width + LANES :] = jnp.where(lane < HD, queries[2], 0.0).astype(
                bf16
            )
            return inner

        lax.fori_loop(0, per_half, block, 0)

        @pl.when(step == 0)
        def _():
            mixed_copy.start()

        return carry

    lax.fori_loop(0, 2, half, 0)

    def halo_copy(side, part):
        return remote(
            halo_out.at[side, part],
            halo_in.at[side, part],
            halo_send.at[side, part],
            halo_recv.at[side, part],
            f - 1 if side == 0 else f + 1,
            t,
        )

    halves = group // QB
    for part in range(halves):
        sends, _ = margin_plan(f, fsdp_count, part)
        for side in range(2):

            @pl.when(sends[side])
            def _(side=side, part=part):
                base = (0 if side == 0 else margin + group) + part * QB
                for head in range(heads):
                    halo_out[side, part, head] = totals[head, pl.ds(base, QB), :].astype(bf16)
                halo_copy(side, part).start()

    for part in range(halves):
        _, receives = margin_plan(f, fsdp_count, part)
        here = pl.ds(margin + part * QB, QB)
        for side in range(2):

            @pl.when(receives[side])
            def _(side=side, part=part, here=here):
                halo_copy(side, part).wait_recv()
                for head in range(heads):
                    totals[head, here, :] += halo_in[side, part, head].astype(f32)

        for head in range(heads):
            dproj_ref[part * QB : (part + 1) * QB, head * LANES : (head + 1) * LANES] = (
                totals[head, here, :] * (1.0 / scale)
            ).astype(bf16)

    def add_rows(i, carry):
        return carry + column_sum(dproj_ref[pl.ds(i * rows, rows), :].astype(f32))

    sums_ref[...] = lax.fori_loop(
        0, tp_count, add_rows, jnp.zeros((1, dproj_ref.shape[1]), f32)
    )
    finish_grads((mlp_total, heads_total))
    mixed_copy.wait()

    def settle(j, carry):
        context_copy(j).wait_send()
        return carry

    lax.fori_loop(1, tp_count, settle, 0)
    for part in range(halves):
        sends, _ = margin_plan(f, fsdp_count, part)
        for side in range(2):

            @pl.when(sends[side])
            def _(side=side, part=part):
                halo_copy(side, part).wait_send()


def attend_back(
    fsdp_count, tp_count, lengths, dspread, wide, pairs, context, mlp_grad, heads_grad, mixed
):
    bf16 = jnp.bfloat16
    f32 = jnp.float32
    heads, group, _ = wide.shape
    _, rows, width = dspread.shape
    count = fsdp_count // 2
    depth, features = mlp_grad.shape[3:]
    dma = pltpu.SemaphoreType.DMA
    mlp_kinds = mlp_grad.shape[0]
    return pl.pallas_call(
        functools.partial(attend_back_kernel, fsdp_count, tp_count),
        out_shape=(
            jax.ShapeDtypeStruct((group, heads * LANES + 2 * LANES), bf16),
            jax.ShapeDtypeStruct((mlp_kinds, depth, features), f32),
            jax.ShapeDtypeStruct((tp_count, depth, width), f32),
            jax.ShapeDtypeStruct(mixed.shape, bf16),
            jax.ShapeDtypeStruct((1, heads * LANES + 2 * LANES), f32),
        ),
        in_specs=[pl.BlockSpec(memory_space=pltpu.SMEM)] + whole_specs(7),
        out_specs=tuple(whole_specs(5)),
        scratch_shapes=[
            pltpu.VMEM((tp_count, rows, width), bf16),
            pltpu.VMEM((heads, CLIP, LANES), bf16),
            pltpu.VMEM((heads, CLIP, LANES), bf16),
            pltpu.VMEM((heads, LANES, CLIP), bf16),
            pltpu.VMEM((heads, pairs.shape[0], LANES), f32),
            pltpu.VMEM((2, group // QB, heads, QB, LANES), bf16),
            pltpu.VMEM((2, group // QB, heads, QB, LANES), bf16),
            pltpu.VMEM((mlp_kinds, count, depth, features), bf16),
            pltpu.VMEM((count, mlp_kinds, depth, features), bf16),
            pltpu.VMEM((tp_count, count, depth, width), bf16),
            pltpu.VMEM((count, tp_count, depth, width), bf16),
            dma((tp_count,)),
            dma((tp_count,)),
            dma,
            dma,
            dma((2, group // QB)),
            dma((2, group // QB)),
            dma((2,)),
            dma((2,)),
            dma((count,)),
            dma((count,)),
            dma((count,)),
            dma((count,)),
        ],
        compiler_params=pltpu.CompilerParams(
            collective_id=5, has_side_effects=True, vmem_limit_bytes=VMEM_LIMIT
        ),
        name="attend_back",
    )(lengths, dspread, wide, pairs, context, mlp_grad, heads_grad, mixed)


def pack_columns(key, value, query):
    lead = key.shape[:-1]
    heads = key.shape[-1] // HD
    pairs = jnp.stack([key.reshape(*lead, heads, HD), value.reshape(*lead, heads, HD)], axis=-2)
    spare = jnp.zeros((*lead, -key.shape[-1] % LANES), key.dtype)
    return jnp.concatenate([pairs.reshape(*lead, -1), query, spare], axis=-1)


def on_device(
    inputs,
    out_cotangent,
    clip_lengths,
    norm1_gain,
    norm1_shift,
    query_weight,
    query_bias,
    key_weight,
    value_weight,
    value_bias,
    out_weight,
    out_bias,
    norm2_gain,
    norm2_shift,
    fc1_weight,
    fc1_bias,
    fc2_weight,
    fc2_bias,
):
    bf16 = jnp.bfloat16
    f32 = jnp.float32
    tp_count = lax.axis_size("tp")
    fsdp_count = lax.axis_size("fsdp")
    tp_index = lax.axis_index("tp")
    fsdp_index = lax.axis_index("fsdp")
    own_rows = inputs.shape[0]
    group_rows = out_cotangent.shape[0]
    score_scale = 1.0 / math.sqrt(HD)
    margin = CLIP - QB
    tp_slot = (jnp.arange(tp_count) == tp_index).astype(f32)
    unit1, spread1, _ = normalize(inputs, norm1_gain, norm1_shift)
    local_width = query_weight.shape[1]
    heads_here = local_width // HD
    unit_count = fc1_weight.shape[0]
    by_tp = lambda bias: bias.reshape(tp_count, 1, local_width)
    pair_width = 2 * local_width
    mlp_own = jnp.stack([fc1_weight, fc2_weight])
    query, pairs, normed, attention_w, mlp_w, out_parts = project(
        fsdp_count,
        tp_count,
        inputs,
        norm1_gain.reshape(1, -1),
        norm1_shift.reshape(1, -1),
        pack_columns(key_weight, value_weight, query_weight)[None],
        pack_columns(jnp.zeros((tp_count, 1, local_width), f32), by_tp(value_bias), by_tp(query_bias)),
        mlp_own,
        out_weight,
        pair_width,
        margin,
    )
    attention_w = attention_w[0]
    spread, context, wide, mlp_other, out_full = attend(
        fsdp_count, tp_count, clip_lengths, query, pairs, mlp_own, out_parts, heads_here
    )
    normed = normed.reshape(group_rows, -1)
    key_w, value_w = jnp.moveaxis(attention_w[:, :pair_width].reshape(-1, heads_here, 2, HD), 2, 0)
    key_w = key_w.reshape(-1, local_width)
    value_w = value_w.reshape(-1, local_width)
    query_w = attention_w[:, pair_width : pair_width + local_width]
    unit_bias = jnp.swapaxes(fc1_bias.reshape(fsdp_count, tp_count, unit_count), 0, 1)
    dhidden, outputs, mixed, dspread, mlp_grad, heads_grad, bias_part, sums = by_rows(
        fsdp_count,
        tp_count,
        inputs,
        spread,
        out_full,
        jnp.stack([out_bias, norm2_gain, norm2_shift, fc2_bias]),
        unit_bias.reshape(tp_count, -1, 1, 256),
        mlp_w,
        mlp_other,
        out_cotangent,
    )
    count = fsdp_count // 2
    dproj, mlp_total, heads_total, mixed, proj_sums = attend_back(
        fsdp_count,
        tp_count,
        clip_lengths,
        dspread,
        wide,
        pairs,
        context,
        mlp_grad.reshape(4, count, 2, unit_count, -1),
        heads_grad.reshape(tp_count, count, 2, unit_count, -1),
        mixed,
    )
    outputs = outputs + mixed.astype(f32)
    halves = [(i, (i + tp_count // 2) % tp_count) for i in range(tp_count)]
    grad_fc1, grad_fc2 = mlp_total[:2] + lax.ppermute(
        mlp_total[2:].astype(bf16), "tp", halves
    ).astype(f32)
    grad_out = lax.psum_scatter(
        heads_total.astype(bf16), "tp", scatter_dimension=0, tiled=True
    )[0].astype(f32)
    grad_gain2, grad_shift2, grad_obias, grad_b2 = sums
    mate_index = (tp_index + tp_count // 2) % tp_count
    mate_slot = (jnp.arange(tp_count) == mate_index).astype(f32)
    bias_part = bias_part.reshape(2, -1)
    by_tp_sum = tp_slot[:, None] * bias_part[0] + mate_slot[:, None] * bias_part[1]
    grad_b1 = jnp.swapaxes(by_tp_sum.reshape(tp_count, fsdp_count, unit_count), 0, 1).reshape(-1)
    dquery = dproj[:, pair_width : pair_width + local_width]
    dkey, dvalue = jnp.moveaxis(dproj[:, :pair_width].reshape(-1, heads_here, 2, HD), 2, 0).reshape(
        2, -1, local_width
    )
    grad_query = contract_rows(normed, dquery)
    grad_key = contract_rows(normed, dkey)
    grad_value = contract_rows(normed, dvalue)
    grad_qbias = (tp_slot[:, None] * jnp.sum(dquery.astype(f32), axis=0)[None, :]).reshape(-1)
    grad_vbias = (tp_slot[:, None] * jnp.sum(dvalue.astype(f32), axis=0)[None, :]).reshape(-1)
    dnorm1 = scatter_rows(
        contract_cols(dquery, query_w)
        + contract_cols(dkey, key_w)
        + contract_cols(dvalue, value_w),
        "tp",
    )
    grad_gain1 = jnp.sum(dnorm1 * unit1, axis=0)
    grad_shift1 = jnp.sum(dnorm1, axis=0)
    inputs_grad = dhidden + norm_back(dnorm1, unit1, spread1, norm1_gain)
    grad_query, grad_key, grad_value = jnp.split(
        scatter_rows(jnp.concatenate([grad_query, grad_key, grad_value], axis=1), "fsdp"),
        3,
        axis=1,
    )
    (
        grad_gain1,
        grad_shift1,
        grad_qbias,
        grad_vbias,
        grad_obias,
        grad_gain2,
        grad_shift2,
        grad_b1,
        grad_b2,
    ) = lax.psum(
        (
            grad_gain1,
            grad_shift1,
            grad_qbias,
            grad_vbias,
            grad_obias,
            grad_gain2,
            grad_shift2,
            grad_b1,
            grad_b2,
        ),
        ("fsdp", "tp"),
    )
    return (
        outputs,
        inputs_grad,
        grad_gain1,
        grad_shift1,
        grad_query,
        grad_qbias,
        grad_key,
        grad_value,
        grad_vbias,
        grad_out,
        grad_obias,
        grad_gain2,
        grad_shift2,
        grad_fc1,
        grad_b1,
        grad_fc2,
        grad_b2,
    )


def solution(mesh):
    in_specs = (
        P(("fsdp", "tp"), None),
        P("fsdp", None),
        P(),
        P(),
        P(),
        P("fsdp", "tp"),
        P(),
        P("fsdp", "tp"),
        P("fsdp", "tp"),
        P(),
        P("fsdp", "tp"),
        P(),
        P(),
        P(),
        P(("fsdp", "tp"), None),
        P(),
        P(("fsdp", "tp"), None),
        P(),
    )
    out_specs = (
        P(("fsdp", "tp"), None),
        P(("fsdp", "tp"), None),
        P(),
        P(),
        P("fsdp", "tp"),
        P(),
        P("fsdp", "tp"),
        P("fsdp", "tp"),
        P(),
        P("fsdp", "tp"),
        P(),
        P(),
        P(),
        P(("fsdp", "tp"), None),
        P(),
        P(("fsdp", "tp"), None),
        P(),
    )
    return jax.shard_map(
        on_device, mesh=mesh, in_specs=in_specs, out_specs=out_specs, check_vma=False
    )
```

```python
import functools
import math

import jax
import jax.numpy as jnp
from jax import lax
from jax.experimental import pallas as pl
from jax.experimental.pallas import tpu as pltpu
from jax.sharding import PartitionSpec as P

HD = 64
CLIP = 1536
QB = 512


eps_norm = 1e-05
root_half = 0.7071067811865476
inv_root_tau = 0.3989422804014327
far_negative = -1e30


def normalize(rows, gain, shift):
    centre = jnp.mean(rows, axis=-1, keepdims=True)
    centred = rows - centre
    inv_spread = lax.rsqrt(jnp.mean(centred * centred, axis=-1, keepdims=True) + eps_norm)
    unit_rows = centred * inv_spread
    return (unit_rows, inv_spread, unit_rows * gain + shift)


def norm_back(upstream, unit_rows, inv_spread, gain):
    scaled = upstream * gain
    return inv_spread * (
        scaled
        - jnp.mean(scaled, axis=-1, keepdims=True)
        - unit_rows * jnp.mean(scaled * unit_rows, axis=-1, keepdims=True)
    )


def contract_rows(left_rows, right_rows):
    return lax.dot_general(
        left_rows, right_rows, (((0,), (0,)), ((), ())), preferred_element_type=jnp.float32
    )


def contract_cols(left_rows, right_rows):
    return lax.dot_general(
        left_rows, right_rows, (((1,), (1,)), ((), ())), preferred_element_type=jnp.float32
    )


MESH = pl.DeviceIdType.MESH
VMEM_LIMIT = 60 * 1024 * 1024
LANES = 128


def remote(source, target, send_sem, recv_sem, fsdp_to, tp_to):
    return pltpu.make_async_remote_copy(
        src_ref=source,
        dst_ref=target,
        send_sem=send_sem,
        recv_sem=recv_sem,
        device_id=(fsdp_to, tp_to),
        device_id_type=MESH,
    )


def greet(fsdp_count, tp_count, f, t):
    barrier = pltpu.get_barrier_semaphore()

    def greet_fsdp(i, carry):
        pl.semaphore_signal(
            barrier, inc=1, device_id=(lax.rem(f + i, fsdp_count), t), device_id_type=MESH
        )
        return carry

    def greet_tp(j, carry):
        pl.semaphore_signal(
            barrier, inc=1, device_id=(f, lax.rem(t + j, tp_count)), device_id_type=MESH
        )
        return carry

    lax.fori_loop(1, fsdp_count, greet_fsdp, 0)
    lax.fori_loop(1, tp_count, greet_tp, 0)
    pl.semaphore_wait(barrier, fsdp_count + tp_count - 2)


def gather_copies(f, t, fsdp_count, sources, targets, depth, sends, recvs):
    partner = f + 1 - 2 * lax.rem(f, 2)

    def piece(target, owner):
        return target.at[:, pl.ds(owner * depth, depth)]

    def copies(owner, toward, lane, first):
        return [
            remote(
                source if first else piece(target, owner),
                piece(target, owner),
                send.at[lane],
                recv.at[owner],
                toward,
                t,
            )
            for source, target, send, recv in zip(sources, targets, sends, recvs)
        ]

    def start():
        def body(i, carry):
            for handle in copies(f, lax.rem(f + 2 * i, fsdp_count), i, True):
                handle.start()
            return carry

        lax.fori_loop(1, fsdp_count // 2, body, 0)
        for handle in copies(f, partner, 0, True):
            handle.start()
        for source, target in zip(sources, targets):
            target[:, pl.ds(f * depth, depth), :] = source[...]

    def relay():
        def body(i, carry):
            owner = lax.rem(f + fsdp_count - 2 * i, fsdp_count)
            for handle in copies(owner, partner, fsdp_count // 2 + i, False):
                handle.wait_recv()
                handle.start()
            return carry

        lax.fori_loop(1, fsdp_count // 2, body, 0)

    def finish():
        def body(i, carry):
            owner = lax.rem(partner + 2 * i, fsdp_count)
            for handle in copies(owner, partner, 0, False):
                handle.wait_recv()
            return carry

        lax.fori_loop(0, fsdp_count // 2, body, 0)

    def drain():
        def body(i, carry):
            for handle in copies(f, lax.rem(f + 2 * i, fsdp_count), i, True):
                handle.wait_send()
            for handle in copies(
                lax.rem(f + fsdp_count - 2 * i, fsdp_count),
                partner,
                fsdp_count // 2 + i,
                False,
            ):
                handle.wait_send()
            return carry

        lax.fori_loop(1, fsdp_count // 2, body, 0)
        for handle in copies(f, partner, 0, True):
            handle.wait_send()

    return (start, relay, finish, drain)


def project_kernel(
    fsdp_count,
    tp_count,
    x_ref,
    gain_ref,
    shift_ref,
    weight_ref,
    bias_ref,
    mlp_ref,
    out_ref,
    query_ref,
    pair_ref,
    normed_ref,
    full_ref,
    mlp_full,
    heads_ref,
    side_send,
    side_recv,
    weight_send,
    weight_recv,
    mlp_send,
    mlp_recv,
    row_send,
    row_recv,
    halo_send,
    halo_recv,
):
    f = lax.axis_index("fsdp")
    t = lax.axis_index("tp")
    rows = x_ref.shape[0]
    depth = weight_ref.shape[1]
    group = rows * tp_count
    pair_width = pair_ref.shape[1]
    margin = (pair_ref.shape[0] - group) // 2
    per_half = tp_count // 2
    phase = lax.rem(f, 3)
    above = f + 1 < fsdp_count
    below = f > 0
    blank = jnp.zeros((256, pair_width), jnp.bfloat16)

    def clear(i, carry):
        pair_ref[pl.ds(i * 256, 256), :] = blank
        pair_ref[pl.ds(margin + group + i * 256, 256), :] = blank
        return carry

    lax.fori_loop(0, margin // 256, clear, 0)
    greet(fsdp_count, tp_count, f, t)
    start_weights, relay_weights, finish_weights, drain_weights = gather_copies(
        f, t, fsdp_count, (weight_ref,), (full_ref,), depth, (weight_send,), (weight_recv,)
    )
    start_mlp, relay_mlp, finish_mlp, drain_mlp = gather_copies(
        f, t, fsdp_count, (mlp_ref,), (mlp_full,), depth, (mlp_send,), (mlp_recv,)
    )
    start_weights()
    _, _, normed = normalize(x_ref[...], gain_ref[...], shift_ref[...])
    normed_ref[t] = normed.astype(jnp.bfloat16)

    def row_copy(source, lane, toward):
        return remote(
            normed_ref.at[source],
            normed_ref.at[source],
            row_send.at[lane],
            row_recv.at[source],
            f,
            toward,
        )

    @pl.when(t > 0)
    def _():
        row_copy(t, tp_count, t - 1).start()

    @pl.when(t < tp_count - 1)
    def _():
        row_copy(t, tp_count + 1, t + 1).start()

    def heads_copy(j):
        return remote(
            out_ref,
            heads_ref.at[t],
            side_send.at[j],
            side_recv.at[j],
            f,
            lax.rem(t + j, tp_count),
        )

    def heads_start(j, carry):
        heads_copy(j).start()
        return carry

    def heads_done(j, carry):
        heads_copy(j).wait_send()
        source = lax.rem(t + tp_count - j, tp_count)
        remote(
            out_ref, heads_ref.at[source], side_send.at[j], side_recv.at[j], f, source
        ).wait_recv()
        return carry

    heads_ref[t] = out_ref[...]
    lax.fori_loop(1, tp_count, heads_start, 0)
    relay_weights()
    start_mlp()
    finish_weights()

    def halo_copy(source, side):
        return remote(
            pair_ref.at[pl.ds(margin + source * rows, rows)],
            pair_ref.at[pl.ds((0 if side == 0 else margin + group) + source * rows, rows)],
            halo_send.at[side, source],
            halo_recv.at[side, source],
            f + 1 if side == 0 else f - 1,
            t,
        )

    def halo_sends(source):
        late = source >= per_half
        return (
            above & ((phase == 0) | ((phase == 1) & late)),
            below & ((phase == 2) | ((phase == 1) & jnp.logical_not(late))),
        )

    def halo_receives(source):
        late = source >= per_half
        return (
            below & ((phase == 1) | ((phase == 2) & late)),
            above & ((phase == 1) | ((phase == 0) & jnp.logical_not(late))),
        )

    def compute(source):
        out = jnp.dot(normed_ref[source], full_ref[0], preferred_element_type=jnp.float32)
        out = (out + bias_ref[t]).astype(jnp.bfloat16)
        pair_ref[pl.ds(margin + source * rows, rows), :] = out[:, :pair_width]
        for side, needed in enumerate(halo_sends(source)):

            @pl.when(needed)
            def _(side=side):
                halo_copy(source, side).start()

        query_ref[pl.ds(source * rows, rows), :] = out[:, pair_width:]

    compute(t)

    def arrival(k):
        step = k // 2 + 1
        side = 2 * lax.rem(k, 2) - 1
        source = t + side * step
        onward = t - side
        valid = (source >= 0) & (source < tp_count)
        return (source, onward, valid, valid & (onward >= 0) & (onward < tp_count))

    def receive(k, carry):
        source, onward, valid, forward = arrival(k)

        @pl.when(valid)
        def _():
            row_copy(source, 0, t).wait_recv()

            @pl.when(forward)
            def _():
                row_copy(source, source, onward).start()

            compute(source)

        return carry

    lax.fori_loop(0, 2 * (tp_count - 1), receive, 0)
    relay_mlp()
    lax.fori_loop(1, tp_count, heads_done, 0)

    def sent(k, carry):
        source, onward, valid, forward = arrival(k)

        @pl.when(forward)
        def _():
            row_copy(source, source, onward).wait_send()

        return carry

    lax.fori_loop(0, 2 * (tp_count - 1), sent, 0)

    @pl.when(t > 0)
    def _():
        row_copy(t, tp_count, t - 1).wait_send()

    @pl.when(t < tp_count - 1)
    def _():
        row_copy(t, tp_count + 1, t + 1).wait_send()

    def halo_done(source, carry):
        for side, (sends, receives) in enumerate(zip(halo_sends(source), halo_receives(source))):

            @pl.when(sends)
            def _(side=side):
                halo_copy(source, side).wait_send()

            @pl.when(receives)
            def _(side=side):
                halo_copy(source, side).wait_recv()

        return carry

    lax.fori_loop(0, tp_count, halo_done, 0)
    drain_weights()
    finish_mlp()
    drain_mlp()


def whole_specs(count):
    return [pl.BlockSpec(memory_space=pltpu.VMEM)] * count


def project(fsdp_count, tp_count, x, gain, shift, weights, bias, mlp, out_weight, pair_width, margin):
    bf16 = jnp.bfloat16
    rows, features = x.shape
    group = rows * tp_count
    depth = weights.shape[1]
    dma = pltpu.SemaphoreType.DMA
    return pl.pallas_call(
        functools.partial(project_kernel, fsdp_count, tp_count),
        out_shape=(
            jax.ShapeDtypeStruct((group, weights.shape[2] - pair_width), bf16),
            jax.ShapeDtypeStruct((group + 2 * margin, pair_width), bf16),
            jax.ShapeDtypeStruct((tp_count, rows, features), bf16),
            jax.ShapeDtypeStruct((1, depth * fsdp_count, weights.shape[2]), bf16),
            jax.ShapeDtypeStruct((2, depth * fsdp_count, features), bf16),
            jax.ShapeDtypeStruct((tp_count, *out_weight.shape), bf16),
        ),
        in_specs=whole_specs(7),
        out_specs=tuple(whole_specs(6)),
        scratch_shapes=[
            dma((tp_count,)),
            dma((tp_count,)),
            dma((fsdp_count,)),
            dma((fsdp_count,)),
            dma((fsdp_count,)),
            dma((fsdp_count,)),
            dma((tp_count + 2,)),
            dma((tp_count,)),
            dma((2, tp_count)),
            dma((2, tp_count)),
        ],
        compiler_params=pltpu.CompilerParams(
            collective_id=1, has_side_effects=True, vmem_limit_bytes=VMEM_LIMIT
        ),
        name="project",
    )(x, gain, shift, weights, bias, mlp, out_weight)


def block_clip(f, part, margin):
    phase = lax.rem(f, 3)
    start = jnp.where(
        phase == 0,
        margin,
        jnp.where(phase == 2, margin - QB, jnp.where(part == 0, 0, margin + QB)),
    )
    return (pl.multiple_of(start, QB), (2 * f + part) // 3)


def head_tiles(pair, length):
    lane = lax.broadcasted_iota(jnp.int32, pair.shape, 1)
    row = lax.broadcasted_iota(jnp.int32, pair.shape, 0)
    extra = jnp.where(
        lane == HD,
        jnp.where(row < length, 0.0, far_negative),
        jnp.where(lane <= HD + 3, 1.0, 0.0),
    )
    return jnp.where(lane < HD, pair, extra)


def spread_heads(rows, head):
    tile = rows[:, (head // 2) * LANES : (head // 2 + 1) * LANES]
    return pltpu.roll(tile, HD, axis=1) if head % 2 else tile


def three_parts(column):
    high = column.astype(jnp.bfloat16).astype(jnp.float32)
    rest = column - high
    middle = rest.astype(jnp.bfloat16).astype(jnp.float32)
    return (high, middle, rest - middle)


def attend_kernel(
    fsdp_count,
    tp_count,
    lengths_ref,
    query_ref,
    pair_ref,
    mlp_ref,
    out_ref,
    spread_ref,
    context_ref,
    wide_ref,
    mlp_full,
    out_full,
    mate_ref,
    key_tiles,
    value_tiles,
    mate_send,
    mate_recv,
    context_send,
    context_recv,
    mlp_send,
    mlp_recv,
    out_send,
    out_recv,
):
    f = lax.axis_index("fsdp")
    t = lax.axis_index("tp")
    bf16 = jnp.bfloat16
    f32 = jnp.float32
    rows = spread_ref.shape[1]
    heads = wide_ref.shape[0]
    group = rows * tp_count
    margin = (pair_ref.shape[0] - group) // 2
    greet(fsdp_count, tp_count, f, t)
    depth = mlp_ref.shape[1]
    start_out, relay_out, finish_out, drain_out = gather_copies(
        f, t, fsdp_count, (out_ref,), (out_full,), depth, (out_send,), (out_recv,)
    )
    start_mlp, relay_mlp, finish_mlp, drain_mlp = gather_copies(
        f, t, fsdp_count, (mate_ref,), (mlp_full,), depth, (mlp_send,), (mlp_recv,)
    )
    mate_copy = remote(
        mlp_ref, mate_ref, mate_send, mate_recv, f, lax.rem(t + tp_count // 2, tp_count)
    )
    mate_copy.start()
    start_out()
    per_half = tp_count // 2

    def context_copy(toward):
        return remote(
            context_ref.at[pl.ds(toward * rows, rows)],
            spread_ref.at[t],
            context_send.at[toward],
            context_recv.at[t],
            f,
            toward,
        )

    lane = lax.broadcasted_iota(jnp.int32, (rows, LANES), 1)
    row = lax.broadcasted_iota(jnp.int32, (LANES, rows), 0)
    tall = lax.broadcasted_iota(jnp.int32, (LANES, CLIP), 0)

    def half(step, carry):
        part = lax.rem(t // per_half + 1 + step, 2)
        first, clip = block_clip(f, part, margin)
        length = lengths_ref[clip]
        for head in range(heads):
            pair = pair_ref[pl.ds(first, CLIP), head * LANES : (head + 1) * LANES].astype(f32)
            key_tiles[head] = head_tiles(pair, length).astype(bf16)
            value_tiles[head] = jnp.where(tall < HD, 1.0, pair.T).astype(bf16)

        def block(i, inner):
            within = lax.rem(lax.rem(t, per_half) + 1 + i, per_half)
            index = part * per_half + within
            here = pl.ds(pl.multiple_of(index * rows, rows), rows)
            query = query_ref[here, :].astype(f32) * (1.0 / math.sqrt(HD))
            parts = []
            for head in range(heads):
                wide = jnp.where(
                    lane < HD, spread_heads(query, head), jnp.where(lane == HD, 1.0, 0.0)
                )
                scores = lax.dot_general(
                    key_tiles[head],
                    wide.astype(bf16),
                    (((1,), (1,)), ((), ())),
                    preferred_element_type=f32,
                )
                highest = jnp.max(scores, axis=0, keepdims=True)
                weights = jnp.exp(scores - highest).astype(bf16)
                summed = jnp.dot(value_tiles[head], weights, preferred_element_type=f32)
                total = summed[0:1, :]
                log_total = highest + jnp.log(total)
                turned = jnp.where(row == 0, log_total, summed * (1.0 / total)).T
                high, middle, low = three_parts(turned[:, 0:1])
                wide_ref[head, here, :] = jnp.where(
                    lane == HD + 1,
                    -high,
                    jnp.where(lane == HD + 2, -middle, jnp.where(lane == HD + 3, -low, wide)),
                ).astype(bf16)
                parts.append(turned)
            context_ref[here, 0:LANES] = jnp.where(
                lane < HD, pltpu.roll(parts[0], HD, axis=1), parts[1]
            ).astype(bf16)
            context_ref[here, LANES : LANES + HD] = pltpu.roll(parts[2], HD, axis=1)[
                :, :HD
            ].astype(bf16)

            @pl.when(index == t)
            def _():
                spread_ref[t] = context_ref[here, :]

            @pl.when(index != t)
            def _():
                context_copy(index).start()

            return inner

        lax.fori_loop(0, per_half, block, 0)

        @pl.when(step == 0)
        def _():
            mate_copy.wait()
            start_mlp()
            relay_out()

        return carry

    lax.fori_loop(0, 2, half, 0)
    relay_mlp()

    def settle(j, carry):
        toward = lax.rem(t + j, tp_count)
        context_copy(toward).wait_send()
        remote(
            context_ref.at[pl.ds(0, rows)],
            spread_ref.at[toward],
            context_send.at[toward],
            context_recv.at[toward],
            f,
            toward,
        ).wait_recv()
        return carry

    lax.fori_loop(1, tp_count, settle, 0)
    finish_out()
    finish_mlp()
    drain_out()
    drain_mlp()


def attend(fsdp_count, tp_count, lengths, query, pairs, mlp, out_weights, heads):
    bf16 = jnp.bfloat16
    group = query.shape[0]
    rows = group // tp_count
    width = heads * HD
    dma = pltpu.SemaphoreType.DMA
    depth = mlp.shape[1]
    return pl.pallas_call(
        functools.partial(attend_kernel, fsdp_count, tp_count),
        out_shape=(
            jax.ShapeDtypeStruct((tp_count, rows, width), bf16),
            jax.ShapeDtypeStruct((group, width), bf16),
            jax.ShapeDtypeStruct((heads, group, LANES), bf16),
            jax.ShapeDtypeStruct((mlp.shape[0], depth * fsdp_count, mlp.shape[2]), bf16),
            jax.ShapeDtypeStruct((tp_count, depth * fsdp_count, width), bf16),
        ),
        in_specs=[pl.BlockSpec(memory_space=pltpu.SMEM)] + whole_specs(4),
        out_specs=tuple(whole_specs(5)),
        scratch_shapes=[
            pltpu.VMEM(mlp.shape, bf16),
            pltpu.VMEM((heads, CLIP, LANES), bf16),
            pltpu.VMEM((heads, LANES, CLIP), bf16),
            dma,
            dma,
            dma((tp_count,)),
            dma((tp_count,)),
            dma((fsdp_count,)),
            dma((fsdp_count,)),
            dma((fsdp_count,)),
            dma((fsdp_count,)),
        ],
        compiler_params=pltpu.CompilerParams(
            collective_id=2, has_side_effects=True, vmem_limit_bytes=VMEM_LIMIT
        ),
        name="attend",
    )(lengths, query, pairs, mlp, out_weights)


def column_sum(rows):
    return jnp.sum(rows, axis=0, keepdims=True)


def rows_kernel(
    fsdp_count,
    tp_count,
    x_ref,
    spread_ref,
    heads_ref,
    vector_ref,
    bias_ref,
    own_ref,
    mate_ref,
    cotangent_ref,
    gradient_ref,
    outputs_ref,
    mixed_ref,
    context_ref,
    mlp_grad,
    heads_grad,
    bias_grad,
    sums_ref,
    upstream,
    rounded,
    hidden_ref,
    unit_ref,
    normed_ref,
    active_ref,
    slope_ref,
    mixed_sum,
    norm_sum,
    norm_out,
    norm_in,
    load_sem,
    row_send,
    row_recv,
    norm_send,
    norm_recv,
):
    f = lax.axis_index("fsdp")
    t = lax.axis_index("tp")
    bf16 = jnp.bfloat16
    f32 = jnp.float32
    rows = x_ref.shape[0]
    tile = 256
    side = lax.rem(t, 2)
    peer = t + 1 - 2 * side
    load = pltpu.make_async_copy(
        cotangent_ref.at[pl.ds((t - side) * rows, 2 * rows)], upstream, load_sem
    )
    load.start()
    barrier = pltpu.get_barrier_semaphore()
    pl.semaphore_signal(barrier, inc=1, device_id=(f, peer), device_id_type=MESH)
    pl.semaphore_wait(barrier, 1)

    hidden = x_ref[...] + vector_ref[0:1, :]
    for j in range(tp_count):
        hidden = hidden + lax.dot_general(
            spread_ref[j], heads_ref[j], (((1,), (1,)), ((), ())), preferred_element_type=f32
        )
    hidden_ref[...] = hidden
    unit, spread, normed = normalize(hidden, vector_ref[1:2, :], vector_ref[2:3, :])
    unit_ref[...] = unit
    normed_ref[side] = normed.astype(bf16)
    row_copy = remote(normed_ref.at[side], normed_ref.at[side], row_send, row_recv, f, peer)
    row_copy.start()
    load.wait()

    def rounding(i, carry):
        rounded[pl.ds(i * rows, rows), :] = upstream[pl.ds(i * rows, rows), :].astype(bf16)
        return carry

    lax.fori_loop(0, 2, rounding, 0)
    mixed_sum[...] = jnp.zeros(mixed_sum.shape, f32)
    norm_sum[...] = jnp.zeros(norm_sum.shape, f32)
    chunks = own_ref.shape[1] // tile
    mate = lax.rem(t + tp_count // 2, tp_count)

    def feed_forward(turn, carry):
        which = lax.rem(side + turn, 2)

        @pl.when(turn == 1)
        def _():
            row_copy.wait_recv()

        here = pl.ds(pl.multiple_of(which * rows, rows), rows)
        normed_rows = normed_ref[which]
        upstream_rows = rounded[here, :]

        for level, (weights, owner) in enumerate(((own_ref, t), (mate_ref, mate))):

            def chunk(c, inner, weights=weights, owner=owner, level=level):
                units = pl.ds(pl.multiple_of(c * tile, tile), tile)
                up = weights[0, units, :]
                down = weights[1, units, :]
                preact = (
                    lax.dot_general(
                        normed_rows, up, (((1,), (1,)), ((), ())), preferred_element_type=f32
                    )
                    + bias_ref[owner, c]
                )
                cdf = 0.5 * (1.0 + lax.erf(preact * root_half))
                active = (preact * cdf).astype(bf16)
                slope = cdf + preact * jnp.exp(-0.5 * preact * preact) * inv_root_tau
                dactive = lax.dot_general(
                    upstream_rows, down, (((1,), (1,)), ((), ())), preferred_element_type=f32
                )
                dpreact = (dactive * slope).astype(bf16)
                active_ref[level, c, here, :] = active
                slope_ref[level, c, here, :] = dpreact
                norm_sum[which] += jnp.dot(dpreact, up, preferred_element_type=f32)
                mixed_sum[which] += jnp.dot(active, down, preferred_element_type=f32)
                return inner

            lax.fori_loop(0, chunks, chunk, 0)
        return carry

    lax.fori_loop(0, 2, feed_forward, 0)
    norm_out[...] = norm_sum[1 - side].astype(bf16)
    norm_copy = remote(norm_out, norm_in, norm_send, norm_recv, f, peer)
    norm_copy.start()
    mixed_ref[...] = mixed_sum[1 - side].astype(bf16)
    outputs_ref[...] = hidden_ref[...] + mixed_sum[side] + vector_ref[3:4, :]

    for level in range(2):

        def weight_grads(c, carry, level=level):
            units = pl.ds(pl.multiple_of(c * tile, tile), tile)
            slopes = slope_ref[level, c]
            both = jnp.concatenate([normed_ref[0], normed_ref[1]], axis=0)
            mlp_grad[2 * level, units, :] = contract_rows(slopes, both).astype(bf16)
            mlp_grad[2 * level + 1, units, :] = contract_rows(active_ref[level, c], rounded[...]).astype(bf16)
            bias_grad[level, c] = column_sum(slopes.astype(f32))
            return carry

        lax.fori_loop(0, chunks, weight_grads, 0)

    norm_copy.wait()
    dnorm = norm_sum[side] + norm_in[...].astype(f32)
    unit = unit_ref[...]
    cotangent = upstream[pl.ds(pl.multiple_of(side * rows, rows), rows), :]
    gradient = cotangent + norm_back(dnorm, unit, spread, vector_ref[1:2, :])
    gradient_ref[...] = gradient
    sums_ref[0:1, :] = column_sum(dnorm * unit)
    sums_ref[1:2, :] = column_sum(dnorm)
    sums_ref[2:3, :] = column_sum(gradient)
    sums_ref[3:4, :] = column_sum(cotangent)
    gradient = gradient.astype(bf16)
    for j in range(tp_count):
        context_ref[j] = jnp.dot(gradient, heads_ref[j], preferred_element_type=f32).astype(bf16)
        heads_grad[j] = contract_rows(gradient, spread_ref[j]).astype(bf16)
    row_copy.wait_send()


def by_rows(fsdp_count, tp_count, x, spread, heads, vectors, bias, own, mate, cotangent):
    bf16 = jnp.bfloat16
    f32 = jnp.float32
    rows, features = x.shape
    units = own.shape[1]
    chunks = units // 256
    dma = pltpu.SemaphoreType.DMA
    return pl.pallas_call(
        functools.partial(rows_kernel, fsdp_count, tp_count),
        out_shape=(
            jax.ShapeDtypeStruct((rows, features), f32),
            jax.ShapeDtypeStruct((rows, features), f32),
            jax.ShapeDtypeStruct((rows, features), bf16),
            jax.ShapeDtypeStruct(spread.shape, bf16),
            jax.ShapeDtypeStruct((4, units, features), bf16),
            jax.ShapeDtypeStruct(heads.shape, bf16),
            jax.ShapeDtypeStruct((2, chunks, 1, 256), f32),
            jax.ShapeDtypeStruct((4, features), f32),
        ),
        in_specs=whole_specs(7) + [pl.BlockSpec(memory_space=pl.ANY)],
        out_specs=tuple(whole_specs(8)),
        scratch_shapes=[
            pltpu.VMEM((2 * rows, features), f32),
            pltpu.VMEM((2 * rows, features), bf16),
            pltpu.VMEM((rows, features), f32),
            pltpu.VMEM((rows, features), f32),
            pltpu.VMEM((2, rows, features), bf16),
            pltpu.VMEM((2, chunks, 2 * rows, 256), bf16),
            pltpu.VMEM((2, chunks, 2 * rows, 256), bf16),
            pltpu.VMEM((2, rows, features), f32),
            pltpu.VMEM((2, rows, features), f32),
            pltpu.VMEM((rows, features), bf16),
            pltpu.VMEM((rows, features), bf16),
            dma,
            dma,
            dma,
            dma,
            dma,
        ],
        compiler_params=pltpu.CompilerParams(
            collective_id=4, has_side_effects=True, vmem_limit_bytes=VMEM_LIMIT
        ),
        name="by_rows",
    )(x, spread, heads, vectors, bias, own, mate, cotangent)


def margin_plan(f, fsdp_count, part):
    phase = lax.rem(f, 3)
    above = f + 1 < fsdp_count
    below = f > 0
    sends = (
        below & ((phase == 1) | ((phase == 2) & (part == 1))),
        above & ((phase == 1) | ((phase == 0) & (part == 0))),
    )
    receives = (
        above & ((phase == 0) | ((phase == 1) & (part == 1))),
        below & ((phase == 2) | ((phase == 1) & (part == 0))),
    )
    return (sends, receives)


def scatter_copies(f, t, fsdp_count, grads, firsts, seconds, one_send, one_recv, sends, recvs):
    parity = lax.rem(f, 2)
    partner = f + 1 - 2 * parity
    place = f // 2
    count = fsdp_count // 2

    def first_copies():
        return [
            remote(
                grad.at[:, :, 1 - parity], first, one_send.at[i], one_recv.at[i], partner, t
            )
            for i, (grad, first) in enumerate(zip(grads, firsts))
        ]

    def second_copies(i):
        toward = lax.rem(f + 2 * i, fsdp_count)
        return [
            remote(
                first.at[:, toward // 2],
                second.at[place],
                send.at[toward // 2],
                recv.at[place],
                toward,
                t,
            )
            for first, second, send, recv in zip(firsts, seconds, sends, recvs)
        ]

    def start():
        for handle in first_copies():
            handle.start()

    def add_first():
        for handle in first_copies():
            handle.wait_recv()
        for grad, first in zip(grads, firsts):

            def body(k, carry, grad=grad, first=first):
                i, j = (k // count, lax.rem(k, count))
                mine = grad[i, j, parity].astype(jnp.float32)
                first[i, j] = (mine + first[i, j].astype(jnp.float32)).astype(jnp.bfloat16)
                return carry

            lax.fori_loop(0, grad.shape[0] * count, body, 0)

        def send(i, carry):
            for handle in second_copies(i):
                handle.start()
            return carry

        lax.fori_loop(1, count, send, 0)

    def finish(totals):
        for first, total in zip(firsts, totals):
            total[...] = first[:, place].astype(jnp.float32)

        def body(i, carry):
            source = lax.rem(f + fsdp_count - 2 * i, fsdp_count)
            for first, second, send, recv, total in zip(firsts, seconds, sends, recvs, totals):
                remote(
                    first.at[:, place],
                    second.at[source // 2],
                    send.at[0],
                    recv.at[source // 2],
                    source,
                    t,
                ).wait_recv()
                total[...] += second[source // 2].astype(jnp.float32)
            return carry

        lax.fori_loop(1, count, body, 0)

        def drain(i, carry):
            for handle in second_copies(i):
                handle.wait_send()
            return carry

        lax.fori_loop(1, count, drain, 0)
        for handle in first_copies():
            handle.wait_send()

    return (start, add_first, finish)


def attend_back_kernel(
    fsdp_count,
    tp_count,
    lengths_ref,
    dspread_ref,
    wide_ref,
    pair_ref,
    context_ref,
    mlp_grad,
    heads_grad,
    mixed_ref,
    dproj_ref,
    mlp_total,
    heads_total,
    mixed_in,
    sums_ref,
    dcontext,
    key_tiles,
    value_tiles,
    turned_tiles,
    totals,
    halo_out,
    halo_in,
    mlp_first,
    mlp_second,
    heads_first,
    heads_second,
    context_send,
    context_recv,
    mixed_send,
    mixed_recv,
    halo_send,
    halo_recv,
    one_send,
    one_recv,
    mlp_send,
    mlp_recv,
    heads_send,
    heads_recv,
):
    f = lax.axis_index("fsdp")
    t = lax.axis_index("tp")
    bf16 = jnp.bfloat16
    f32 = jnp.float32
    rows = dspread_ref.shape[1]
    heads = wide_ref.shape[0]
    group = rows * tp_count
    margin = (pair_ref.shape[0] - group) // 2
    per_half = tp_count // 2
    pair_width = heads * LANES
    scale = 1.0 / math.sqrt(HD)
    greet(fsdp_count, tp_count, f, t)

    def context_copy(j):
        toward = lax.rem(t + j, tp_count)
        return remote(
            dspread_ref.at[toward],
            dcontext.at[t],
            context_send.at[j],
            context_recv.at[t],
            f,
            toward,
        )

    def context_start(j, carry):
        context_copy(j).start()
        return carry

    lax.fori_loop(1, tp_count, context_start, 0)
    start_grads, add_grads, finish_grads = scatter_copies(
        f,
        t,
        fsdp_count,
        (mlp_grad, heads_grad),
        (mlp_first, heads_first),
        (mlp_second, heads_second),
        one_send,
        one_recv,
        (mlp_send, heads_send),
        (mlp_recv, heads_recv),
    )
    start_grads()
    dcontext[t] = dspread_ref[t]
    mixed_copy = remote(
        mixed_ref, mixed_in, mixed_send, mixed_recv, f, t + 1 - 2 * lax.rem(t, 2)
    )

    def clear(i, carry):
        for head in range(heads):
            totals[head, pl.ds(i * QB, QB), :] = jnp.zeros((QB, LANES), f32)
        return carry

    lax.fori_loop(0, pair_ref.shape[0] // QB, clear, 0)
    add_grads()
    lane = lax.broadcasted_iota(jnp.int32, (rows, LANES), 1)
    tall = lax.broadcasted_iota(jnp.int32, (CLIP, LANES), 1)

    def half(step, carry):
        part = lax.rem(t // per_half + step, 2)
        first, clip = block_clip(f, part, margin)
        length = lengths_ref[clip]
        for head in range(heads):
            pair = pair_ref[pl.ds(first, CLIP), head * LANES : (head + 1) * LANES].astype(f32)
            key_tiles[head] = head_tiles(pair, length).astype(bf16)
            value_tiles[head] = jnp.where(
                tall < HD, jnp.where(tall < 3, 1.0, 0.0), pair
            ).astype(bf16)
            turned_tiles[head] = pair.T.astype(bf16)

        def block(i, inner):
            within = lax.rem(lax.rem(t, per_half) + i, per_half)
            index = part * per_half + within

            @pl.when(index != t)
            def _():
                remote(
                    dspread_ref.at[0],
                    dcontext.at[index],
                    context_send.at[0],
                    context_recv.at[index],
                    f,
                    index,
                ).wait_recv()

            here = pl.ds(pl.multiple_of(index * rows, rows), rows)
            empty = jnp.zeros((rows, HD), f32)

            def two_tiles(ref, at):
                return (
                    ref[at + (slice(0, LANES),)].astype(f32),
                    jnp.concatenate(
                        [ref[at + (slice(LANES, LANES + HD),)].astype(f32), empty], axis=1
                    ),
                )

            upstream = two_tiles(dcontext, (index, slice(None)))
            forward = two_tiles(context_ref, (here,))
            queries = []
            for head in range(heads):
                tile = upstream[head // 2]
                odd = head % 2
                kept = jnp.where((lane >= HD) if odd else (lane < HD), tile * forward[head // 2], 0.0)
                delta = jnp.sum(kept, axis=1, keepdims=True) * scale
                high, middle, low = three_parts(delta)
                grad = (tile if odd else pltpu.roll(tile, HD, axis=1)) * scale
                grad = jnp.where(
                    lane >= HD,
                    grad,
                    jnp.where(
                        lane == 0,
                        -high,
                        jnp.where(lane == 1, -middle, jnp.where(lane == 2, -low, 0.0)),
                    ),
                ).astype(bf16)
                wide = wide_ref[head, here, :]
                probs = jnp.exp(contract_cols(key_tiles[head], wide))
                dscores = (probs * contract_cols(value_tiles[head], grad)).astype(bf16)
                both = jnp.concatenate([dscores, probs.astype(bf16)], axis=1)
                fold = jnp.concatenate(
                    [
                        jnp.where(lane < HD, wide.astype(f32), 0.0),
                        jnp.where(lane < HD, 0.0, grad.astype(f32)),
                    ],
                    axis=0,
                ).astype(bf16)
                totals[head, pl.ds(first, CLIP), :] += jnp.dot(
                    both, fold, preferred_element_type=f32
                )
                queries.append(
                    jnp.dot(turned_tiles[head], dscores, preferred_element_type=f32).T
                )
            dproj_ref[here, pair_width : pair_width + LANES] = jnp.where(
                lane < HD, queries[0], pltpu.roll(queries[1], HD, axis=1)
            ).astype(bf16)
            dproj_ref[here, pair_width + LANES :] = jnp.where(lane < HD, queries[2], 0.0).astype(
                bf16
            )
            return inner

        lax.fori_loop(0, per_half, block, 0)

        @pl.when(step == 0)
        def _():
            mixed_copy.start()

        return carry

    lax.fori_loop(0, 2, half, 0)

    def halo_copy(side, part):
        return remote(
            halo_out.at[side, part],
            halo_in.at[side, part],
            halo_send.at[side, part],
            halo_recv.at[side, part],
            f - 1 if side == 0 else f + 1,
            t,
        )

    halves = group // QB
    for part in range(halves):
        sends, _ = margin_plan(f, fsdp_count, part)
        for side in range(2):

            @pl.when(sends[side])
            def _(side=side, part=part):
                base = (0 if side == 0 else margin + group) + part * QB
                for head in range(heads):
                    halo_out[side, part, head] = totals[head, pl.ds(base, QB), :].astype(bf16)
                halo_copy(side, part).start()

    for part in range(halves):
        _, receives = margin_plan(f, fsdp_count, part)
        here = pl.ds(margin + part * QB, QB)
        for side in range(2):

            @pl.when(receives[side])
            def _(side=side, part=part, here=here):
                halo_copy(side, part).wait_recv()
                for head in range(heads):
                    totals[head, here, :] += halo_in[side, part, head].astype(f32)

        for head in range(heads):
            dproj_ref[part * QB : (part + 1) * QB, head * LANES : (head + 1) * LANES] = (
                totals[head, here, :] * (1.0 / scale)
            ).astype(bf16)

    def add_rows(i, carry):
        return carry + column_sum(dproj_ref[pl.ds(i * rows, rows), :].astype(f32))

    sums_ref[...] = lax.fori_loop(
        0, tp_count, add_rows, jnp.zeros((1, dproj_ref.shape[1]), f32)
    )
    finish_grads((mlp_total, heads_total))
    mixed_copy.wait()

    def settle(j, carry):
        context_copy(j).wait_send()
        return carry

    lax.fori_loop(1, tp_count, settle, 0)
    for part in range(halves):
        sends, _ = margin_plan(f, fsdp_count, part)
        for side in range(2):

            @pl.when(sends[side])
            def _(side=side, part=part):
                halo_copy(side, part).wait_send()


def attend_back(
    fsdp_count, tp_count, lengths, dspread, wide, pairs, context, mlp_grad, heads_grad, mixed
):
    bf16 = jnp.bfloat16
    f32 = jnp.float32
    heads, group, _ = wide.shape
    _, rows, width = dspread.shape
    count = fsdp_count // 2
    depth, features = mlp_grad.shape[3:]
    dma = pltpu.SemaphoreType.DMA
    mlp_kinds = mlp_grad.shape[0]
    return pl.pallas_call(
        functools.partial(attend_back_kernel, fsdp_count, tp_count),
        out_shape=(
            jax.ShapeDtypeStruct((group, heads * LANES + 2 * LANES), bf16),
            jax.ShapeDtypeStruct((mlp_kinds, depth, features), f32),
            jax.ShapeDtypeStruct((tp_count, depth, width), f32),
            jax.ShapeDtypeStruct(mixed.shape, bf16),
            jax.ShapeDtypeStruct((1, heads * LANES + 2 * LANES), f32),
        ),
        in_specs=[pl.BlockSpec(memory_space=pltpu.SMEM)] + whole_specs(7),
        out_specs=tuple(whole_specs(5)),
        scratch_shapes=[
            pltpu.VMEM((tp_count, rows, width), bf16),
            pltpu.VMEM((heads, CLIP, LANES), bf16),
            pltpu.VMEM((heads, CLIP, LANES), bf16),
            pltpu.VMEM((heads, LANES, CLIP), bf16),
            pltpu.VMEM((heads, pairs.shape[0], LANES), f32),
            pltpu.VMEM((2, group // QB, heads, QB, LANES), bf16),
            pltpu.VMEM((2, group // QB, heads, QB, LANES), bf16),
            pltpu.VMEM((mlp_kinds, count, depth, features), bf16),
            pltpu.VMEM((count, mlp_kinds, depth, features), bf16),
            pltpu.VMEM((tp_count, count, depth, width), bf16),
            pltpu.VMEM((count, tp_count, depth, width), bf16),
            dma((tp_count,)),
            dma((tp_count,)),
            dma,
            dma,
            dma((2, group // QB)),
            dma((2, group // QB)),
            dma((2,)),
            dma((2,)),
            dma((count,)),
            dma((count,)),
            dma((count,)),
            dma((count,)),
        ],
        compiler_params=pltpu.CompilerParams(
            collective_id=5, has_side_effects=True, vmem_limit_bytes=VMEM_LIMIT
        ),
        name="attend_back",
    )(lengths, dspread, wide, pairs, context, mlp_grad, heads_grad, mixed)


def reduce_copies(f, t, fsdp_count, tp_count, vector, by_fsdp, by_tp, sends, recvs):
    def fsdp_copy(i):
        return remote(
            vector, by_fsdp.at[f], sends.at[i], recvs.at[f], lax.rem(f + i, fsdp_count), t
        )

    def tp_copy(j):
        return remote(
            by_tp.at[t],
            by_tp.at[t],
            sends.at[fsdp_count + j],
            recvs.at[fsdp_count + t],
            f,
            lax.rem(t + j, tp_count),
        )

    def start():
        def body(i, carry):
            fsdp_copy(i).start()
            return carry

        by_fsdp[f] = vector[...]
        lax.fori_loop(1, fsdp_count, body, 0)

    def middle():
        def wait(i, carry):
            source = lax.rem(f + i, fsdp_count)
            remote(
                vector, by_fsdp.at[source], sends.at[i], recvs.at[source], source, t
            ).wait_recv()
            return carry

        def add(i, total):
            return total + by_fsdp[i]

        def body(j, carry):
            tp_copy(j).start()
            return carry

        lax.fori_loop(1, fsdp_count, wait, 0)
        by_tp[t] = lax.fori_loop(0, fsdp_count, add, jnp.zeros(vector.shape, jnp.float32))
        lax.fori_loop(1, tp_count, body, 0)

    def finish():
        def wait(j, carry):
            source = lax.rem(t + j, tp_count)
            remote(
                vector,
                by_tp.at[source],
                sends.at[fsdp_count + j],
                recvs.at[fsdp_count + source],
                f,
                source,
            ).wait_recv()
            tp_copy(j).wait_send()
            return carry

        def drain(i, carry):
            fsdp_copy(i).wait_send()
            return carry

        lax.fori_loop(1, tp_count, wait, 0)
        lax.fori_loop(1, fsdp_count, drain, 0)

    return (start, middle, finish)


def finish_kernel(
    fsdp_count,
    tp_count,
    x_ref,
    gain_ref,
    shift_ref,
    dproj_ref,
    full_ref,
    normed_ref,
    gradient_ref,
    partial_ref,
    mixed_ref,
    mlp_ref,
    heads_ref,
    sums_ref,
    bias_ref,
    proj_ref,
    inputs_grad,
    outputs_ref,
    weight_total,
    mlp_total,
    heads_total,
    late_total,
    early_total,
    proj_total,
    bias_total,
    weight_grad,
    weight_first,
    weight_second,
    weight_sum,
    part_ref,
    row_out,
    row_in,
    mlp_out,
    mlp_in,
    heads_out,
    heads_in,
    early,
    early_fsdp,
    early_tp,
    late,
    late_fsdp,
    late_tp,
    row_send,
    row_recv,
    side_send,
    side_recv,
    one_send,
    one_recv,
    weight_send,
    weight_recv,
    early_send,
    early_recv,
    late_send,
    late_recv,
):
    f = lax.axis_index("fsdp")
    t = lax.axis_index("tp")
    bf16 = jnp.bfloat16
    f32 = jnp.float32
    rows, features = x_ref.shape
    proj_width = dproj_ref.shape[1]
    last = tp_count - 1
    units = bias_ref.shape[3]
    early[0:4, :] = sums_ref[...]
    early[4:5, :] = jnp.zeros((1, features), f32)
    early[4:5, 0:proj_width] = proj_ref[...]
    for level in range(2):
        for c in range(bias_ref.shape[1]):
            early[5 + level : 6 + level, c * units : (c + 1) * units] = bias_ref[level, c]
    mlp_out[...] = mlp_ref[2:4].astype(bf16)
    heads_out[...] = heads_ref[...].astype(bf16)
    greet(fsdp_count, tp_count, f, t)
    start_early, middle_early, finish_early = reduce_copies(
        f, t, fsdp_count, tp_count, early, early_fsdp, early_tp, early_send, early_recv
    )
    start_late, middle_late, finish_late = reduce_copies(
        f, t, fsdp_count, tp_count, late, late_fsdp, late_tp, late_send, late_recv
    )
    start_weights, add_weights, finish_weights = scatter_copies(
        f,
        t,
        fsdp_count,
        (weight_grad,),
        (weight_first,),
        (weight_second,),
        one_send,
        one_recv,
        (weight_send,),
        (weight_recv,),
    )

    def row_copy(block, side):
        return remote(
            row_out.at[block],
            row_in.at[side, block],
            row_send.at[block],
            row_recv.at[side, block],
            f,
            t + 1 if side == 0 else t - 1,
        )

    def partial_rows(k, carry):
        block = jnp.where(t < tp_count // 2, last - k, k)
        product = contract_cols(
            dproj_ref[pl.ds(pl.multiple_of(block * rows, rows), rows), :], full_ref[0]
        )
        part_ref[block] = product

        @pl.when((t == 0) & (block > t))
        def _():
            row_out[block] = product.astype(bf16)
            row_copy(block, 0).start()

        @pl.when((t == last) & (block < t))
        def _():
            row_out[block] = product.astype(bf16)
            row_copy(block, 1).start()

        return carry

    lax.fori_loop(0, tp_count, partial_rows, 0)
    start_early()
    depth = weight_grad.shape[3]

    mlp_copy = remote(
        mlp_out, mlp_in, side_send.at[0], side_recv.at[0], f, lax.rem(t + tp_count // 2, tp_count)
    )
    mlp_copy.start()

    def heads_copy(j):
        toward = lax.rem(t + j, tp_count)
        return remote(
            heads_out.at[toward],
            heads_in.at[t],
            side_send.at[j],
            side_recv.at[tp_count + t],
            f,
            toward,
        )

    def heads_start(j, carry):
        heads_copy(j).start()
        return carry

    lax.fori_loop(1, tp_count, heads_start, 0)
    tall = 256

    def weight_part(c, carry):
        columns = pl.ds(pl.multiple_of(c * tall, tall), tall)
        total = jnp.zeros((tall, proj_width), f32)
        for block in range(tp_count):
            total = total + contract_rows(
                normed_ref[block, :, columns],
                dproj_ref[block * rows : (block + 1) * rows, :],
            )
        weight_sum[columns, :] = total.astype(bf16)
        return carry

    lax.fori_loop(0, features // tall, weight_part, 0)

    def arrange(i, carry):
        weight_grad[0, i // 2, lax.rem(i, 2)] = weight_sum[
            pl.ds(pl.multiple_of(i * depth, 8), depth), :
        ]
        return carry

    lax.fori_loop(0, fsdp_count, arrange, 0)
    start_weights()
    outputs_ref[...] = partial_ref[...] + mixed_ref[...].astype(f32)
    unit, spread, _ = normalize(x_ref[...], gain_ref[...], shift_ref[...])
    add_weights()
    middle_early()

    def relay(k, carry):
        for side, (block, valid) in enumerate(
            ((last - k, (last - k > t) & (t > 0)), (k, (k < t) & (t < last)))
        ):

            @pl.when(valid)
            def _(side=side, block=block):
                row_copy(block, side).wait_recv()
                row_out[block] = (part_ref[block] + row_in[side, block].astype(f32)).astype(bf16)
                row_copy(block, side).start()

        return carry

    lax.fori_loop(0, last, relay, 0)
    finish_weights((weight_total,))
    heads_total[...] = heads_ref[t]

    def heads_done(j, carry):
        source = lax.rem(t + j, tp_count)
        remote(
            heads_out.at[source],
            heads_in.at[source],
            side_send.at[j],
            side_recv.at[tp_count + source],
            f,
            source,
        ).wait_recv()
        heads_total[...] += heads_in[source].astype(f32)
        heads_copy(j).wait_send()
        return carry

    lax.fori_loop(1, tp_count, heads_done, 0)
    mlp_copy.wait()
    mlp_total[...] = mlp_ref[0:2] + mlp_in[...].astype(f32)
    finish_early()
    early_total[...] = jnp.sum(early_tp[:, 0:4, :], axis=0)
    for j in range(tp_count):
        proj_total[j : j + 1, :] = early_tp[j, 4:5, 0:proj_width]
        bias_total[j : j + 1, :] = (
            early_tp[j, 5:6, :] + early_tp[(j + tp_count // 2) % tp_count, 6:7, :]
        )

    @pl.when(t > 0)
    def _():
        row_copy(t, 0).wait_recv()
        part_ref[t] += row_in[0, t].astype(f32)

    @pl.when(t < last)
    def _():
        row_copy(t, 1).wait_recv()
        part_ref[t] += row_in[1, t].astype(f32)

    dnorm = part_ref[t]
    late[0:1, :] = column_sum(dnorm * unit)
    late[1:2, :] = column_sum(dnorm)
    start_late()
    inputs_grad[...] = gradient_ref[...] + norm_back(dnorm, unit, spread, gain_ref[...])
    middle_late()

    def settle(block, carry):
        @pl.when(block > t)
        def _():
            row_copy(block, 0).wait_send()

        @pl.when(block < t)
        def _():
            row_copy(block, 1).wait_send()

        return carry

    lax.fori_loop(0, tp_count, settle, 0)
    finish_late()
    late_total[...] = jnp.sum(late_tp[...], axis=0)


def finish(
    fsdp_count,
    tp_count,
    x,
    gain,
    shift,
    dproj,
    full,
    normed,
    gradient,
    partial,
    mixed,
    mlp,
    heads,
    sums,
    bias,
    proj,
):
    bf16 = jnp.bfloat16
    f32 = jnp.float32
    rows, features = x.shape
    _, depth, width = heads.shape
    proj_width = dproj.shape[1]
    count = fsdp_count // 2
    dma = pltpu.SemaphoreType.DMA
    peers = fsdp_count + tp_count
    return pl.pallas_call(
        functools.partial(finish_kernel, fsdp_count, tp_count),
        out_shape=(
            jax.ShapeDtypeStruct((rows, features), f32),
            jax.ShapeDtypeStruct((rows, features), f32),
            jax.ShapeDtypeStruct((1, depth, proj_width), f32),
            jax.ShapeDtypeStruct((2, depth, features), f32),
            jax.ShapeDtypeStruct((depth, width), f32),
            jax.ShapeDtypeStruct((2, features), f32),
            jax.ShapeDtypeStruct((4, features), f32),
            jax.ShapeDtypeStruct((tp_count, proj_width), f32),
            jax.ShapeDtypeStruct((tp_count, features), f32),
        ),
        in_specs=whole_specs(14),
        out_specs=tuple(whole_specs(9)),
        scratch_shapes=[
            pltpu.VMEM((1, count, 2, depth, proj_width), bf16),
            pltpu.VMEM((1, count, depth, proj_width), bf16),
            pltpu.VMEM((count, 1, depth, proj_width), bf16),
            pltpu.VMEM((features, proj_width), bf16),
            pltpu.VMEM((tp_count, rows, features), f32),
            pltpu.VMEM((tp_count, rows, features), bf16),
            pltpu.VMEM((2, tp_count, rows, features), bf16),
            pltpu.VMEM((2, depth, features), bf16),
            pltpu.VMEM((2, depth, features), bf16),
            pltpu.VMEM((tp_count, depth, width), bf16),
            pltpu.VMEM((tp_count, depth, width), bf16),
            pltpu.VMEM((7, features), f32),
            pltpu.VMEM((fsdp_count, 7, features), f32),
            pltpu.VMEM((tp_count, 7, features), f32),
            pltpu.VMEM((2, features), f32),
            pltpu.VMEM((fsdp_count, 2, features), f32),
            pltpu.VMEM((tp_count, 2, features), f32),
            dma((tp_count,)),
            dma((2, tp_count)),
            dma((tp_count,)),
            dma((2 * tp_count,)),
            dma((1,)),
            dma((1,)),
            dma((count,)),
            dma((count,)),
            dma((peers,)),
            dma((peers,)),
            dma((peers,)),
            dma((peers,)),
        ],
        compiler_params=pltpu.CompilerParams(
            collective_id=6, has_side_effects=True, vmem_limit_bytes=VMEM_LIMIT
        ),
        name="finish",
    )(
        x,
        gain,
        shift,
        dproj,
        full,
        normed,
        gradient,
        partial,
        mixed,
        mlp,
        heads,
        sums,
        bias,
        proj,
    )


def pack_columns(key, value, query):
    lead = key.shape[:-1]
    heads = key.shape[-1] // HD
    pairs = jnp.stack([key.reshape(*lead, heads, HD), value.reshape(*lead, heads, HD)], axis=-2)
    spare = jnp.zeros((*lead, -key.shape[-1] % LANES), key.dtype)
    return jnp.concatenate([pairs.reshape(*lead, -1), query, spare], axis=-1)


def on_device(
    inputs,
    out_cotangent,
    clip_lengths,
    norm1_gain,
    norm1_shift,
    query_weight,
    query_bias,
    key_weight,
    value_weight,
    value_bias,
    out_weight,
    out_bias,
    norm2_gain,
    norm2_shift,
    fc1_weight,
    fc1_bias,
    fc2_weight,
    fc2_bias,
):
    f32 = jnp.float32
    tp_count = lax.axis_size("tp")
    fsdp_count = lax.axis_size("fsdp")
    margin = CLIP - QB
    local_width = query_weight.shape[1]
    heads_here = local_width // HD
    unit_count = fc1_weight.shape[0]
    by_tp = lambda bias: bias.reshape(tp_count, 1, local_width)
    pair_width = 2 * local_width
    mlp_own = jnp.stack([fc1_weight, fc2_weight])
    query, pairs, normed, attention_w, mlp_w, out_parts = project(
        fsdp_count,
        tp_count,
        inputs,
        norm1_gain.reshape(1, -1),
        norm1_shift.reshape(1, -1),
        pack_columns(key_weight, value_weight, query_weight)[None],
        pack_columns(jnp.zeros((tp_count, 1, local_width), f32), by_tp(value_bias), by_tp(query_bias)),
        mlp_own,
        out_weight,
        pair_width,
        margin,
    )
    spread, context, wide, mlp_other, out_full = attend(
        fsdp_count, tp_count, clip_lengths, query, pairs, mlp_own, out_parts, heads_here
    )
    unit_bias = jnp.swapaxes(fc1_bias.reshape(fsdp_count, tp_count, unit_count), 0, 1)
    dhidden, outputs, mixed, dspread, mlp_grad, heads_grad, bias_part, sums = by_rows(
        fsdp_count,
        tp_count,
        inputs,
        spread,
        out_full,
        jnp.stack([out_bias, norm2_gain, norm2_shift, fc2_bias]),
        unit_bias.reshape(tp_count, -1, 1, 256),
        mlp_w,
        mlp_other,
        out_cotangent,
    )
    count = fsdp_count // 2
    dproj, mlp_total, heads_total, mixed, proj_sums = attend_back(
        fsdp_count,
        tp_count,
        clip_lengths,
        dspread,
        wide,
        pairs,
        context,
        mlp_grad.reshape(4, count, 2, unit_count, -1),
        heads_grad.reshape(tp_count, count, 2, unit_count, -1),
        mixed,
    )
    inputs_grad, outputs, weight_total, mlp_total, grad_out, late, early, proj_total, bias_total = (
        finish(
            fsdp_count,
            tp_count,
            inputs,
            norm1_gain.reshape(1, -1),
            norm1_shift.reshape(1, -1),
            dproj,
            attention_w,
            normed,
            dhidden,
            outputs,
            mixed,
            mlp_total,
            heads_total,
            sums,
            bias_part,
            proj_sums,
        )
    )
    grad_gain1, grad_shift1 = late
    grad_gain2, grad_shift2, grad_obias, grad_b2 = early
    grad_fc1, grad_fc2 = mlp_total
    grad_b1 = jnp.swapaxes(bias_total.reshape(tp_count, fsdp_count, unit_count), 0, 1).reshape(-1)

    def unpack_columns(values):
        lead = values.shape[0]
        pair = values[:, :pair_width].reshape(lead, heads_here, 2, HD)
        return (
            pair[:, :, 0].reshape(lead, local_width),
            pair[:, :, 1].reshape(lead, local_width),
            values[:, pair_width : pair_width + local_width],
        )

    grad_key, grad_value, grad_query = unpack_columns(weight_total[0])
    _, grad_vbias, grad_qbias = (part.reshape(-1) for part in unpack_columns(proj_total))
    return (
        outputs,
        inputs_grad,
        grad_gain1,
        grad_shift1,
        grad_query,
        grad_qbias,
        grad_key,
        grad_value,
        grad_vbias,
        grad_out,
        grad_obias,
        grad_gain2,
        grad_shift2,
        grad_fc1,
        grad_b1,
        grad_fc2,
        grad_b2,
    )


def solution(mesh):
    in_specs = (
        P(("fsdp", "tp"), None),
        P("fsdp", None),
        P(),
        P(),
        P(),
        P("fsdp", "tp"),
        P(),
        P("fsdp", "tp"),
        P("fsdp", "tp"),
        P(),
        P("fsdp", "tp"),
        P(),
        P(),
        P(),
        P(("fsdp", "tp"), None),
        P(),
        P(("fsdp", "tp"), None),
        P(),
    )
    out_specs = (
        P(("fsdp", "tp"), None),
        P(("fsdp", "tp"), None),
        P(),
        P(),
        P("fsdp", "tp"),
        P(),
        P("fsdp", "tp"),
        P("fsdp", "tp"),
        P(),
        P("fsdp", "tp"),
        P(),
        P(),
        P(),
        P(("fsdp", "tp"), None),
        P(),
        P(("fsdp", "tp"), None),
        P(),
    )
    return jax.shard_map(
        on_device, mesh=mesh, in_specs=in_specs, out_specs=out_specs, check_vma=False
    )
```

```python
import functools
import math

import jax
import jax.numpy as jnp
from jax import lax
from jax.experimental import pallas as pl
from jax.experimental.pallas import tpu as pltpu
from jax.sharding import PartitionSpec as P

HD = 64
CLIP = 1536
QB = 512


eps_norm = 1e-05
root_half = 0.7071067811865476
inv_root_tau = 0.3989422804014327
far_negative = -1e30


def normalize(rows, gain, shift):
    centre = jnp.mean(rows, axis=-1, keepdims=True)
    centred = rows - centre
    inv_spread = lax.rsqrt(jnp.mean(centred * centred, axis=-1, keepdims=True) + eps_norm)
    unit_rows = centred * inv_spread
    return (unit_rows, inv_spread, unit_rows * gain + shift)


def norm_back(upstream, unit_rows, inv_spread, gain):
    scaled = upstream * gain
    return inv_spread * (
        scaled
        - jnp.mean(scaled, axis=-1, keepdims=True)
        - unit_rows * jnp.mean(scaled * unit_rows, axis=-1, keepdims=True)
    )


def contract_rows(left_rows, right_rows):
    return lax.dot_general(
        left_rows, right_rows, (((0,), (0,)), ((), ())), preferred_element_type=jnp.float32
    )


def contract_cols(left_rows, right_rows):
    return lax.dot_general(
        left_rows, right_rows, (((1,), (1,)), ((), ())), preferred_element_type=jnp.float32
    )


MESH = pl.DeviceIdType.MESH
VMEM_LIMIT = 32 * 1024 * 1024
LANES = 128


def row_of(ref):
    return ref[...].reshape(1, -1)


def remote(source, target, send_sem, recv_sem, fsdp_to, tp_to):
    return pltpu.make_async_remote_copy(
        src_ref=source,
        dst_ref=target,
        send_sem=send_sem,
        recv_sem=recv_sem,
        device_id=(fsdp_to, tp_to),
        device_id_type=MESH,
    )


def greet(fsdp_count, tp_count, f, t):
    barrier = pltpu.get_barrier_semaphore()

    def greet_fsdp(i, carry):
        pl.semaphore_signal(
            barrier, inc=1, device_id=(lax.rem(f + i, fsdp_count), t), device_id_type=MESH
        )
        return carry

    def greet_tp(j, carry):
        pl.semaphore_signal(
            barrier, inc=1, device_id=(f, lax.rem(t + j, tp_count)), device_id_type=MESH
        )
        return carry

    lax.fori_loop(1, fsdp_count, greet_fsdp, 0)
    lax.fori_loop(1, tp_count, greet_tp, 0)
    pl.semaphore_wait(barrier, fsdp_count + tp_count - 2)


def gather_copies(f, t, fsdp_count, sources, targets, depth, sends, recvs):
    partner = f + 1 - 2 * lax.rem(f, 2)

    def piece(target, owner):
        return target.at[:, pl.ds(owner * depth, depth)]

    def copies(owner, toward, lane, first):
        return [
            remote(
                source if first else piece(target, owner),
                piece(target, owner),
                send.at[lane],
                recv.at[owner],
                toward,
                t,
            )
            for source, target, send, recv in zip(sources, targets, sends, recvs)
        ]

    def start():
        def body(i, carry):
            for handle in copies(f, lax.rem(f + 2 * i, fsdp_count), i, True):
                handle.start()
            return carry

        lax.fori_loop(1, fsdp_count // 2, body, 0)
        for handle in copies(f, partner, 0, True):
            handle.start()
        for source, target in zip(sources, targets):
            target[:, pl.ds(f * depth, depth), :] = source[...]

    def relay():
        def body(i, carry):
            owner = lax.rem(f + fsdp_count - 2 * i, fsdp_count)
            for handle in copies(owner, partner, fsdp_count // 2 + i, False):
                handle.wait_recv()
                handle.start()
            return carry

        lax.fori_loop(1, fsdp_count // 2, body, 0)

    def finish():
        def body(i, carry):
            owner = lax.rem(partner + 2 * i, fsdp_count)
            for handle in copies(owner, partner, 0, False):
                handle.wait_recv()
            return carry

        lax.fori_loop(0, fsdp_count // 2, body, 0)

    def drain():
        def body(i, carry):
            for handle in copies(f, lax.rem(f + 2 * i, fsdp_count), i, True):
                handle.wait_send()
            for handle in copies(
                lax.rem(f + fsdp_count - 2 * i, fsdp_count),
                partner,
                fsdp_count // 2 + i,
                False,
            ):
                handle.wait_send()
            return carry

        lax.fori_loop(1, fsdp_count // 2, body, 0)
        for handle in copies(f, partner, 0, True):
            handle.wait_send()

    return (start, relay, finish, drain)


def project_kernel(
    fsdp_count,
    tp_count,
    x_ref,
    gain_ref,
    shift_ref,
    weight_ref,
    bias_ref,
    mlp_ref,
    out_ref,
    query_ref,
    pair_ref,
    normed_ref,
    full_ref,
    mlp_full,
    heads_ref,
    side_send,
    side_recv,
    weight_send,
    weight_recv,
    mlp_send,
    mlp_recv,
    row_send,
    row_recv,
    halo_send,
    halo_recv,
):
    f = lax.axis_index("fsdp")
    t = lax.axis_index("tp")
    rows = x_ref.shape[0]
    depth = weight_ref.shape[1]
    group = rows * tp_count
    pair_width = pair_ref.shape[1]
    margin = (pair_ref.shape[0] - group) // 2
    per_half = tp_count // 2
    phase = lax.rem(f, 3)
    above = f + 1 < fsdp_count
    below = f > 0
    blank = jnp.zeros((256, pair_width), jnp.bfloat16)

    def clear(i, carry):
        pair_ref[pl.ds(i * 256, 256), :] = blank
        pair_ref[pl.ds(margin + group + i * 256, 256), :] = blank
        return carry

    lax.fori_loop(0, margin // 256, clear, 0)
    greet(fsdp_count, tp_count, f, t)
    start_weights, relay_weights, finish_weights, drain_weights = gather_copies(
        f, t, fsdp_count, (weight_ref,), (full_ref,), depth, (weight_send,), (weight_recv,)
    )
    start_mlp, relay_mlp, finish_mlp, drain_mlp = gather_copies(
        f, t, fsdp_count, (mlp_ref,), (mlp_full,), depth, (mlp_send,), (mlp_recv,)
    )
    start_weights()
    _, _, normed = normalize(x_ref[...], row_of(gain_ref), row_of(shift_ref))
    normed_ref[t] = normed.astype(jnp.bfloat16)

    def row_copy(source, lane, toward):
        return remote(
            normed_ref.at[source],
            normed_ref.at[source],
            row_send.at[lane],
            row_recv.at[source],
            f,
            toward,
        )

    @pl.when(t > 0)
    def _():
        row_copy(t, tp_count, t - 1).start()

    @pl.when(t < tp_count - 1)
    def _():
        row_copy(t, tp_count + 1, t + 1).start()

    def heads_copy(j):
        return remote(
            out_ref,
            heads_ref.at[t],
            side_send.at[j],
            side_recv.at[j],
            f,
            lax.rem(t + j, tp_count),
        )

    def heads_start(j, carry):
        heads_copy(j).start()
        return carry

    def heads_done(j, carry):
        heads_copy(j).wait_send()
        source = lax.rem(t + tp_count - j, tp_count)
        remote(
            out_ref, heads_ref.at[source], side_send.at[j], side_recv.at[j], f, source
        ).wait_recv()
        return carry

    heads_ref[t] = out_ref[...]
    lax.fori_loop(1, tp_count, heads_start, 0)
    relay_weights()
    start_mlp()
    finish_weights()

    def halo_copy(source, side):
        return remote(
            pair_ref.at[pl.ds(margin + source * rows, rows)],
            pair_ref.at[pl.ds((0 if side == 0 else margin + group) + source * rows, rows)],
            halo_send.at[side, source],
            halo_recv.at[side, source],
            f + 1 if side == 0 else f - 1,
            t,
        )

    def halo_sends(source):
        late = source >= per_half
        return (
            above & ((phase == 0) | ((phase == 1) & late)),
            below & ((phase == 2) | ((phase == 1) & jnp.logical_not(late))),
        )

    def halo_receives(source):
        late = source >= per_half
        return (
            below & ((phase == 1) | ((phase == 2) & late)),
            above & ((phase == 1) | ((phase == 0) & jnp.logical_not(late))),
        )

    def compute(source):
        out = jnp.dot(normed_ref[source], full_ref[0], preferred_element_type=jnp.float32)
        out = (out + bias_ref[t]).astype(jnp.bfloat16)
        pair_ref[pl.ds(margin + source * rows, rows), :] = out[:, :pair_width]
        for side, needed in enumerate(halo_sends(source)):

            @pl.when(needed)
            def _(side=side):
                halo_copy(source, side).start()

        query_ref[pl.ds(source * rows, rows), :] = out[:, pair_width:]

    compute(t)

    def arrival(k):
        step = k // 2 + 1
        side = 2 * lax.rem(k, 2) - 1
        source = t + side * step
        onward = t - side
        valid = (source >= 0) & (source < tp_count)
        return (source, onward, valid, valid & (onward >= 0) & (onward < tp_count))

    def receive(k, carry):
        source, onward, valid, forward = arrival(k)

        @pl.when(valid)
        def _():
            row_copy(source, 0, t).wait_recv()

            @pl.when(forward)
            def _():
                row_copy(source, source, onward).start()

            compute(source)

        return carry

    lax.fori_loop(0, 2 * (tp_count - 1), receive, 0)
    relay_mlp()
    lax.fori_loop(1, tp_count, heads_done, 0)

    def sent(k, carry):
        source, onward, valid, forward = arrival(k)

        @pl.when(forward)
        def _():
            row_copy(source, source, onward).wait_send()

        return carry

    lax.fori_loop(0, 2 * (tp_count - 1), sent, 0)

    @pl.when(t > 0)
    def _():
        row_copy(t, tp_count, t - 1).wait_send()

    @pl.when(t < tp_count - 1)
    def _():
        row_copy(t, tp_count + 1, t + 1).wait_send()

    def halo_done(source, carry):
        for side, (sends, receives) in enumerate(zip(halo_sends(source), halo_receives(source))):

            @pl.when(sends)
            def _(side=side):
                halo_copy(source, side).wait_send()

            @pl.when(receives)
            def _(side=side):
                halo_copy(source, side).wait_recv()

        return carry

    lax.fori_loop(0, tp_count, halo_done, 0)
    drain_weights()
    finish_mlp()
    drain_mlp()


def whole_specs(count):
    return [pl.BlockSpec(memory_space=pltpu.VMEM)] * count


def project(fsdp_count, tp_count, x, gain, shift, weights, bias, mlp, out_weight, pair_width, margin):
    bf16 = jnp.bfloat16
    rows, features = x.shape
    group = rows * tp_count
    depth = weights.shape[1]
    dma = pltpu.SemaphoreType.DMA
    return pl.pallas_call(
        functools.partial(project_kernel, fsdp_count, tp_count),
        out_shape=(
            jax.ShapeDtypeStruct((group, weights.shape[2] - pair_width), bf16),
            jax.ShapeDtypeStruct((group + 2 * margin, pair_width), bf16),
            jax.ShapeDtypeStruct((tp_count, rows, features), bf16),
            jax.ShapeDtypeStruct((1, depth * fsdp_count, weights.shape[2]), bf16),
            jax.ShapeDtypeStruct((2, depth * fsdp_count, features), bf16),
            jax.ShapeDtypeStruct((tp_count, *out_weight.shape), bf16),
        ),
        in_specs=whole_specs(7),
        out_specs=tuple(whole_specs(6)),
        scratch_shapes=[
            dma((tp_count,)),
            dma((tp_count,)),
            dma((fsdp_count,)),
            dma((fsdp_count,)),
            dma((fsdp_count,)),
            dma((fsdp_count,)),
            dma((tp_count + 2,)),
            dma((tp_count,)),
            dma((2, tp_count)),
            dma((2, tp_count)),
        ],
        compiler_params=pltpu.CompilerParams(
            collective_id=1, has_side_effects=True, vmem_limit_bytes=VMEM_LIMIT
        ),
        name="project",
    )(x, gain, shift, weights, bias, mlp, out_weight)


def block_clip(f, part, margin):
    phase = lax.rem(f, 3)
    start = jnp.where(
        phase == 0,
        margin,
        jnp.where(phase == 2, margin - QB, jnp.where(part == 0, 0, margin + QB)),
    )
    return (pl.multiple_of(start, QB), (2 * f + part) // 3)


def head_tiles(pair, length):
    lane = lax.broadcasted_iota(jnp.int32, pair.shape, 1)
    row = lax.broadcasted_iota(jnp.int32, pair.shape, 0)
    extra = jnp.where(
        lane == HD,
        jnp.where(row < length, 0.0, far_negative),
        jnp.where(lane <= HD + 3, 1.0, 0.0),
    )
    return jnp.where(lane < HD, pair, extra)


def spread_heads(rows, head):
    tile = rows[:, (head // 2) * LANES : (head // 2 + 1) * LANES]
    return pltpu.roll(tile, HD, axis=1) if head % 2 else tile


def three_parts(column):
    high = column.astype(jnp.bfloat16).astype(jnp.float32)
    rest = column - high
    middle = rest.astype(jnp.bfloat16).astype(jnp.float32)
    return (high, middle, rest - middle)


def attend_kernel(
    fsdp_count,
    tp_count,
    lengths_ref,
    query_ref,
    pair_ref,
    mlp_ref,
    out_ref,
    spread_ref,
    context_ref,
    wide_ref,
    mlp_full,
    out_full,
    mate_ref,
    key_tiles,
    value_tiles,
    mate_send,
    mate_recv,
    context_send,
    context_recv,
    mlp_send,
    mlp_recv,
    out_send,
    out_recv,
):
    f = lax.axis_index("fsdp")
    t = lax.axis_index("tp")
    bf16 = jnp.bfloat16
    f32 = jnp.float32
    rows = spread_ref.shape[1]
    heads = wide_ref.shape[0]
    group = rows * tp_count
    margin = (pair_ref.shape[0] - group) // 2
    greet(fsdp_count, tp_count, f, t)
    depth = mlp_ref.shape[1]
    start_out, relay_out, finish_out, drain_out = gather_copies(
        f, t, fsdp_count, (out_ref,), (out_full,), depth, (out_send,), (out_recv,)
    )
    start_mlp, relay_mlp, finish_mlp, drain_mlp = gather_copies(
        f, t, fsdp_count, (mate_ref,), (mlp_full,), depth, (mlp_send,), (mlp_recv,)
    )
    mate_copy = remote(
        mlp_ref, mate_ref, mate_send, mate_recv, f, lax.rem(t + tp_count // 2, tp_count)
    )
    mate_copy.start()
    start_out()
    per_half = tp_count // 2

    def context_copy(toward):
        return remote(
            context_ref.at[pl.ds(toward * rows, rows)],
            spread_ref.at[t],
            context_send.at[toward],
            context_recv.at[t],
            f,
            toward,
        )

    lane = lax.broadcasted_iota(jnp.int32, (rows, LANES), 1)
    row = lax.broadcasted_iota(jnp.int32, (LANES, rows), 0)
    tall = lax.broadcasted_iota(jnp.int32, (LANES, CLIP), 0)

    def half(step, carry):
        part = lax.rem(t // per_half + 1 + step, 2)
        first, clip = block_clip(f, part, margin)
        length = lengths_ref[clip]
        for head in range(heads):
            pair = pair_ref[pl.ds(first, CLIP), head * LANES : (head + 1) * LANES].astype(f32)
            key_tiles[head] = head_tiles(pair, length).astype(bf16)
            value_tiles[head] = jnp.where(tall < HD, 1.0, pair.T).astype(bf16)

        def block(i, inner):
            within = lax.rem(lax.rem(t, per_half) + 1 + i, per_half)
            index = part * per_half + within
            here = pl.ds(pl.multiple_of(index * rows, rows), rows)
            query = query_ref[here, :].astype(f32) * (1.0 / math.sqrt(HD))
            parts = []
            for head in range(heads):
                wide = jnp.where(
                    lane < HD, spread_heads(query, head), jnp.where(lane == HD, 1.0, 0.0)
                )
                scores = lax.dot_general(
                    key_tiles[head],
                    wide.astype(bf16),
                    (((1,), (1,)), ((), ())),
                    preferred_element_type=f32,
                )
                highest = jnp.max(scores, axis=0, keepdims=True)
                weights = jnp.exp(scores - highest).astype(bf16)
                summed = jnp.dot(value_tiles[head], weights, preferred_element_type=f32)
                total = summed[0:1, :]
                log_total = highest + jnp.log(total)
                turned = jnp.where(row == 0, log_total, summed * (1.0 / total)).T
                high, middle, low = three_parts(turned[:, 0:1])
                wide_ref[head, here, :] = jnp.where(
                    lane == HD + 1,
                    -high,
                    jnp.where(lane == HD + 2, -middle, jnp.where(lane == HD + 3, -low, wide)),
                ).astype(bf16)
                parts.append(turned)
            context_ref[here, 0:LANES] = jnp.where(
                lane < HD, pltpu.roll(parts[0], HD, axis=1), parts[1]
            ).astype(bf16)
            context_ref[here, LANES : LANES + HD] = pltpu.roll(parts[2], HD, axis=1)[
                :, :HD
            ].astype(bf16)

            @pl.when(index == t)
            def _():
                spread_ref[t] = context_ref[here, :]

            @pl.when(index != t)
            def _():
                context_copy(index).start()

            return inner

        lax.fori_loop(0, per_half, block, 0)

        @pl.when(step == 0)
        def _():
            mate_copy.wait()
            start_mlp()
            relay_out()

        return carry

    lax.fori_loop(0, 2, half, 0)
    relay_mlp()

    def settle(j, carry):
        toward = lax.rem(t + j, tp_count)
        context_copy(toward).wait_send()
        remote(
            context_ref.at[pl.ds(0, rows)],
            spread_ref.at[toward],
            context_send.at[toward],
            context_recv.at[toward],
            f,
            toward,
        ).wait_recv()
        return carry

    lax.fori_loop(1, tp_count, settle, 0)
    finish_out()
    finish_mlp()
    drain_out()
    drain_mlp()


def attend(fsdp_count, tp_count, lengths, query, pairs, mlp, out_weights, heads):
    bf16 = jnp.bfloat16
    group = query.shape[0]
    rows = group // tp_count
    width = heads * HD
    dma = pltpu.SemaphoreType.DMA
    depth = mlp.shape[1]
    return pl.pallas_call(
        functools.partial(attend_kernel, fsdp_count, tp_count),
        out_shape=(
            jax.ShapeDtypeStruct((tp_count, rows, width), bf16),
            jax.ShapeDtypeStruct((group, width), bf16),
            jax.ShapeDtypeStruct((heads, group, LANES), bf16),
            jax.ShapeDtypeStruct((mlp.shape[0], depth * fsdp_count, mlp.shape[2]), bf16),
            jax.ShapeDtypeStruct((tp_count, depth * fsdp_count, width), bf16),
        ),
        in_specs=[pl.BlockSpec(memory_space=pltpu.SMEM)] + whole_specs(4),
        out_specs=tuple(whole_specs(5)),
        scratch_shapes=[
            pltpu.VMEM(mlp.shape, bf16),
            pltpu.VMEM((heads, CLIP, LANES), bf16),
            pltpu.VMEM((heads, LANES, CLIP), bf16),
            dma,
            dma,
            dma((tp_count,)),
            dma((tp_count,)),
            dma((fsdp_count,)),
            dma((fsdp_count,)),
            dma((fsdp_count,)),
            dma((fsdp_count,)),
        ],
        compiler_params=pltpu.CompilerParams(
            collective_id=2, has_side_effects=True, vmem_limit_bytes=VMEM_LIMIT
        ),
        name="attend",
    )(lengths, query, pairs, mlp, out_weights)


def column_sum(rows):
    return jnp.sum(rows, axis=0, keepdims=True)


def rows_kernel(
    fsdp_count,
    tp_count,
    x_ref,
    spread_ref,
    heads_ref,
    out_bias_ref,
    gain_ref,
    shift_ref,
    last_bias_ref,
    bias_ref,
    own_ref,
    mate_ref,
    cotangent_ref,
    gradient_ref,
    outputs_ref,
    mixed_ref,
    context_ref,
    own_grad,
    mate_grad,
    heads_grad,
    bias_grad,
    sums_ref,
    upstream,
    rounded,
    hidden_ref,
    unit_ref,
    normed_ref,
    active_ref,
    slope_ref,
    mixed_sum,
    norm_sum,
    norm_out,
    norm_in,
    load_sem,
    row_send,
    row_recv,
    norm_send,
    norm_recv,
):
    f = lax.axis_index("fsdp")
    t = lax.axis_index("tp")
    bf16 = jnp.bfloat16
    f32 = jnp.float32
    rows = x_ref.shape[0]
    tile = 256
    side = lax.rem(t, 2)
    peer = t + 1 - 2 * side
    load = pltpu.make_async_copy(
        cotangent_ref.at[pl.ds((t - side) * rows, 2 * rows)], upstream, load_sem
    )
    load.start()
    barrier = pltpu.get_barrier_semaphore()
    pl.semaphore_signal(barrier, inc=1, device_id=(f, peer), device_id_type=MESH)
    pl.semaphore_wait(barrier, 1)

    hidden = x_ref[...] + row_of(out_bias_ref)
    for j in range(tp_count):
        hidden = hidden + lax.dot_general(
            spread_ref[j], heads_ref[j], (((1,), (1,)), ((), ())), preferred_element_type=f32
        )
    hidden_ref[...] = hidden
    unit, spread, normed = normalize(hidden, row_of(gain_ref), row_of(shift_ref))
    unit_ref[...] = unit
    normed_ref[side] = normed.astype(bf16)
    row_copy = remote(normed_ref.at[side], normed_ref.at[side], row_send, row_recv, f, peer)
    row_copy.start()
    load.wait()

    def rounding(i, carry):
        rounded[pl.ds(i * rows, rows), :] = upstream[pl.ds(i * rows, rows), :].astype(bf16)
        return carry

    lax.fori_loop(0, 2, rounding, 0)
    mixed_sum[...] = jnp.zeros(mixed_sum.shape, f32)
    norm_sum[...] = jnp.zeros(norm_sum.shape, f32)
    chunks = own_ref.shape[1] // tile
    mate = lax.rem(t + tp_count // 2, tp_count)

    def feed_forward(turn, carry):
        which = lax.rem(side + turn, 2)

        @pl.when(turn == 1)
        def _():
            row_copy.wait_recv()

        here = pl.ds(pl.multiple_of(which * rows, rows), rows)
        normed_rows = normed_ref[which]
        upstream_rows = rounded[here, :]

        for level, (weights, owner) in enumerate(((own_ref, t), (mate_ref, mate))):

            def chunk(c, inner, weights=weights, owner=owner, level=level):
                units = pl.ds(pl.multiple_of(c * tile, tile), tile)
                up = weights[0, units, :]
                down = weights[1, units, :]
                preact = (
                    lax.dot_general(
                        normed_rows, up, (((1,), (1,)), ((), ())), preferred_element_type=f32
                    )
                    + bias_ref[owner, c]
                )
                cdf = 0.5 * (1.0 + lax.erf(preact * root_half))
                active = (preact * cdf).astype(bf16)
                slope = cdf + preact * jnp.exp(-0.5 * preact * preact) * inv_root_tau
                dactive = lax.dot_general(
                    upstream_rows, down, (((1,), (1,)), ((), ())), preferred_element_type=f32
                )
                dpreact = (dactive * slope).astype(bf16)
                active_ref[level, c, here, :] = active
                slope_ref[level, c, here, :] = dpreact
                norm_sum[which] += jnp.dot(dpreact, up, preferred_element_type=f32)
                mixed_sum[which] += jnp.dot(active, down, preferred_element_type=f32)
                return inner

            lax.fori_loop(0, chunks, chunk, 0)
        return carry

    lax.fori_loop(0, 2, feed_forward, 0)
    norm_out[...] = norm_sum[1 - side].astype(bf16)
    norm_copy = remote(norm_out, norm_in, norm_send, norm_recv, f, peer)
    norm_copy.start()
    mixed_ref[...] = mixed_sum[1 - side].astype(bf16)
    outputs_ref[...] = hidden_ref[...] + mixed_sum[side] + row_of(last_bias_ref)

    for level, grad in enumerate((own_grad, mate_grad)):

        def weight_grads(c, carry, level=level, grad=grad):
            units = pl.ds(pl.multiple_of(c * tile, tile), tile)
            slopes = slope_ref[level, c]
            both = jnp.concatenate([normed_ref[0], normed_ref[1]], axis=0)
            grad[0, units, :] = contract_rows(slopes, both).astype(bf16)
            grad[1, units, :] = contract_rows(active_ref[level, c], rounded[...]).astype(bf16)
            bias_grad[level, c] = column_sum(slopes.astype(f32))
            return carry

        lax.fori_loop(0, chunks, weight_grads, 0)

    norm_copy.wait()
    dnorm = norm_sum[side] + norm_in[...].astype(f32)
    unit = unit_ref[...]
    cotangent = upstream[pl.ds(pl.multiple_of(side * rows, rows), rows), :]
    gradient = cotangent + norm_back(dnorm, unit, spread, row_of(gain_ref))
    gradient_ref[...] = gradient
    sums_ref[0:1, :] = column_sum(dnorm * unit)
    sums_ref[1:2, :] = column_sum(dnorm)
    sums_ref[2:3, :] = column_sum(gradient)
    sums_ref[3:4, :] = column_sum(cotangent)
    gradient = gradient.astype(bf16)
    for j in range(tp_count):
        context_ref[j] = jnp.dot(gradient, heads_ref[j], preferred_element_type=f32).astype(bf16)
        heads_grad[j] = contract_rows(gradient, spread_ref[j]).astype(bf16)
    row_copy.wait_send()


def by_rows(fsdp_count, tp_count, x, spread, heads, vectors, bias, own, mate, cotangent):
    bf16 = jnp.bfloat16
    f32 = jnp.float32
    rows, features = x.shape
    units = own.shape[1]
    chunks = units // 256
    dma = pltpu.SemaphoreType.DMA
    return pl.pallas_call(
        functools.partial(rows_kernel, fsdp_count, tp_count),
        out_shape=(
            jax.ShapeDtypeStruct((rows, features), f32),
            jax.ShapeDtypeStruct((rows, features), f32),
            jax.ShapeDtypeStruct((rows, features), bf16),
            jax.ShapeDtypeStruct(spread.shape, bf16),
            jax.ShapeDtypeStruct(own.shape, bf16),
            jax.ShapeDtypeStruct(own.shape, bf16),
            jax.ShapeDtypeStruct(heads.shape, bf16),
            jax.ShapeDtypeStruct((2, chunks, 1, 256), f32),
            jax.ShapeDtypeStruct((4, features), f32),
        ),
        in_specs=whole_specs(10) + [pl.BlockSpec(memory_space=pl.ANY)],
        out_specs=tuple(whole_specs(9)),
        scratch_shapes=[
            pltpu.VMEM((2 * rows, features), f32),
            pltpu.VMEM((2 * rows, features), bf16),
            pltpu.VMEM((rows, features), f32),
            pltpu.VMEM((rows, features), f32),
            pltpu.VMEM((2, rows, features), bf16),
            pltpu.VMEM((2, chunks, 2 * rows, 256), bf16),
            pltpu.VMEM((2, chunks, 2 * rows, 256), bf16),
            pltpu.VMEM((2, rows, features), f32),
            pltpu.VMEM((2, rows, features), f32),
            pltpu.VMEM((rows, features), bf16),
            pltpu.VMEM((rows, features), bf16),
            dma,
            dma,
            dma,
            dma,
            dma,
        ],
        compiler_params=pltpu.CompilerParams(
            collective_id=4, has_side_effects=True, vmem_limit_bytes=VMEM_LIMIT
        ),
        name="by_rows",
    )(x, spread, heads, *vectors, bias, own, mate, cotangent)


def margin_plan(f, fsdp_count, part):
    phase = lax.rem(f, 3)
    above = f + 1 < fsdp_count
    below = f > 0
    sends = (
        below & ((phase == 1) | ((phase == 2) & (part == 1))),
        above & ((phase == 1) | ((phase == 0) & (part == 0))),
    )
    receives = (
        above & ((phase == 0) | ((phase == 1) & (part == 1))),
        below & ((phase == 2) | ((phase == 1) & (part == 0))),
    )
    return (sends, receives)


def scatter_copies(f, t, fsdp_count, grads, firsts, seconds, one_send, one_recv, sends, recvs):
    parity = lax.rem(f, 2)
    partner = f + 1 - 2 * parity
    place = f // 2
    count = fsdp_count // 2

    def first_copies():
        return [
            remote(
                grad.at[:, :, 1 - parity], first, one_send.at[i], one_recv.at[i], partner, t
            )
            for i, (grad, first) in enumerate(zip(grads, firsts))
        ]

    def second_copies(i):
        toward = lax.rem(f + 2 * i, fsdp_count)
        return [
            remote(
                first.at[:, toward // 2],
                second.at[place],
                send.at[toward // 2],
                recv.at[place],
                toward,
                t,
            )
            for first, second, send, recv in zip(firsts, seconds, sends, recvs)
        ]

    def start():
        for handle in first_copies():
            handle.start()

    def add_first():
        for handle in first_copies():
            handle.wait_recv()
        for grad, first in zip(grads, firsts):

            def body(k, carry, grad=grad, first=first):
                i, j = (k // count, lax.rem(k, count))
                mine = grad[i, j, parity].astype(jnp.float32)
                first[i, j] = (mine + first[i, j].astype(jnp.float32)).astype(jnp.bfloat16)
                return carry

            lax.fori_loop(0, grad.shape[0] * count, body, 0)

        def send(i, carry):
            for handle in second_copies(i):
                handle.start()
            return carry

        lax.fori_loop(1, count, send, 0)

    def finish(totals):
        for first, total in zip(firsts, totals):
            total[...] = first[:, place].astype(jnp.float32)

        def body(i, carry):
            source = lax.rem(f + fsdp_count - 2 * i, fsdp_count)
            for first, second, send, recv, total in zip(firsts, seconds, sends, recvs, totals):
                remote(
                    first.at[:, place],
                    second.at[source // 2],
                    send.at[0],
                    recv.at[source // 2],
                    source,
                    t,
                ).wait_recv()
                total[...] += second[source // 2].astype(jnp.float32)
            return carry

        lax.fori_loop(1, count, body, 0)

        def drain(i, carry):
            for handle in second_copies(i):
                handle.wait_send()
            return carry

        lax.fori_loop(1, count, drain, 0)
        for handle in first_copies():
            handle.wait_send()

    return (start, add_first, finish)


def attend_back_kernel(
    fsdp_count,
    tp_count,
    lengths_ref,
    dspread_ref,
    wide_ref,
    pair_ref,
    context_ref,
    mate_grad,
    mixed_ref,
    dproj_ref,
    mate_in,
    mixed_in,
    sums_ref,
    dcontext,
    key_tiles,
    value_tiles,
    turned_tiles,
    totals,
    halo_out,
    halo_in,
    mate_first,
    mate_second,
    mate_total,
    mate_out,
    context_send,
    context_recv,
    mixed_send,
    mixed_recv,
    mate_send,
    mate_recv,
    halo_send,
    halo_recv,
    one_send,
    one_recv,
    two_send,
    two_recv,
):
    f = lax.axis_index("fsdp")
    t = lax.axis_index("tp")
    bf16 = jnp.bfloat16
    f32 = jnp.float32
    rows = dspread_ref.shape[1]
    heads = wide_ref.shape[0]
    group = rows * tp_count
    margin = (pair_ref.shape[0] - group) // 2
    per_half = tp_count // 2
    pair_width = heads * LANES
    scale = 1.0 / math.sqrt(HD)
    greet(fsdp_count, tp_count, f, t)

    def context_copy(j):
        toward = lax.rem(t + j, tp_count)
        return remote(
            dspread_ref.at[toward],
            dcontext.at[t],
            context_send.at[j],
            context_recv.at[t],
            f,
            toward,
        )

    def context_start(j, carry):
        context_copy(j).start()
        return carry

    lax.fori_loop(1, tp_count, context_start, 0)
    start_grads, add_grads, finish_grads = scatter_copies(
        f,
        t,
        fsdp_count,
        (mate_grad,),
        (mate_first,),
        (mate_second,),
        one_send,
        one_recv,
        (two_send,),
        (two_recv,),
    )
    start_grads()
    dcontext[t] = dspread_ref[t]
    mixed_copy = remote(
        mixed_ref, mixed_in, mixed_send, mixed_recv, f, t + 1 - 2 * lax.rem(t, 2)
    )

    def clear(i, carry):
        for head in range(heads):
            totals[head, pl.ds(i * QB, QB), :] = jnp.zeros((QB, LANES), f32)
        return carry

    lax.fori_loop(0, pair_ref.shape[0] // QB, clear, 0)
    add_grads()
    lane = lax.broadcasted_iota(jnp.int32, (rows, LANES), 1)
    tall = lax.broadcasted_iota(jnp.int32, (CLIP, LANES), 1)

    def half(step, carry):
        part = lax.rem(t // per_half + step, 2)
        first, clip = block_clip(f, part, margin)
        length = lengths_ref[clip]
        for head in range(heads):
            pair = pair_ref[pl.ds(first, CLIP), head * LANES : (head + 1) * LANES].astype(f32)
            key_tiles[head] = head_tiles(pair, length).astype(bf16)
            value_tiles[head] = jnp.where(
                tall < HD, jnp.where(tall < 3, 1.0, 0.0), pair
            ).astype(bf16)
            turned_tiles[head] = pair.T.astype(bf16)

        def block(i, inner):
            within = lax.rem(lax.rem(t, per_half) + i, per_half)
            index = part * per_half + within

            @pl.when(index != t)
            def _():
                remote(
                    dspread_ref.at[0],
                    dcontext.at[index],
                    context_send.at[0],
                    context_recv.at[index],
                    f,
                    index,
                ).wait_recv()

            here = pl.ds(pl.multiple_of(index * rows, rows), rows)
            empty = jnp.zeros((rows, HD), f32)

            def two_tiles(ref, at):
                return (
                    ref[at + (slice(0, LANES),)].astype(f32),
                    jnp.concatenate(
                        [ref[at + (slice(LANES, LANES + HD),)].astype(f32), empty], axis=1
                    ),
                )

            upstream = two_tiles(dcontext, (index, slice(None)))
            forward = two_tiles(context_ref, (here,))
            queries = []
            for head in range(heads):
                tile = upstream[head // 2]
                odd = head % 2
                kept = jnp.where((lane >= HD) if odd else (lane < HD), tile * forward[head // 2], 0.0)
                delta = jnp.sum(kept, axis=1, keepdims=True) * scale
                high, middle, low = three_parts(delta)
                grad = (tile if odd else pltpu.roll(tile, HD, axis=1)) * scale
                grad = jnp.where(
                    lane >= HD,
                    grad,
                    jnp.where(
                        lane == 0,
                        -high,
                        jnp.where(lane == 1, -middle, jnp.where(lane == 2, -low, 0.0)),
                    ),
                ).astype(bf16)
                wide = wide_ref[head, here, :]
                probs = jnp.exp(contract_cols(key_tiles[head], wide))
                dscores = (probs * contract_cols(value_tiles[head], grad)).astype(bf16)
                both = jnp.concatenate([dscores, probs.astype(bf16)], axis=1)
                fold = jnp.concatenate(
                    [
                        jnp.where(lane < HD, wide.astype(f32), 0.0),
                        jnp.where(lane < HD, 0.0, grad.astype(f32)),
                    ],
                    axis=0,
                ).astype(bf16)
                totals[head, pl.ds(first, CLIP), :] += jnp.dot(
                    both, fold, preferred_element_type=f32
                )
                queries.append(
                    jnp.dot(turned_tiles[head], dscores, preferred_element_type=f32).T
                )
            dproj_ref[here, pair_width : pair_width + LANES] = jnp.where(
                lane < HD, queries[0], pltpu.roll(queries[1], HD, axis=1)
            ).astype(bf16)
            dproj_ref[here, pair_width + LANES :] = jnp.where(lane < HD, queries[2], 0.0).astype(
                bf16
            )
            return inner

        lax.fori_loop(0, per_half, block, 0)

        @pl.when(step == 0)
        def _():
            mixed_copy.start()

        return carry

    lax.fori_loop(0, 2, half, 0)
    mate_copy = remote(
        mate_out, mate_in, mate_send, mate_recv, f, lax.rem(t + tp_count // 2, tp_count)
    )

    def halo_copy(side, part):
        return remote(
            halo_out.at[side, part],
            halo_in.at[side, part],
            halo_send.at[side, part],
            halo_recv.at[side, part],
            f - 1 if side == 0 else f + 1,
            t,
        )

    halves = group // QB
    for part in range(halves):
        sends, _ = margin_plan(f, fsdp_count, part)
        for side in range(2):

            @pl.when(sends[side])
            def _(side=side, part=part):
                base = (0 if side == 0 else margin + group) + part * QB
                for head in range(heads):
                    halo_out[side, part, head] = totals[head, pl.ds(base, QB), :].astype(bf16)
                halo_copy(side, part).start()

    finish_grads((mate_total,))
    mate_out[...] = mate_total[...].astype(bf16)
    mate_copy.start()

    for part in range(halves):
        _, receives = margin_plan(f, fsdp_count, part)
        here = pl.ds(margin + part * QB, QB)
        for side in range(2):

            @pl.when(receives[side])
            def _(side=side, part=part, here=here):
                halo_copy(side, part).wait_recv()
                for head in range(heads):
                    totals[head, here, :] += halo_in[side, part, head].astype(f32)

        for head in range(heads):
            dproj_ref[part * QB : (part + 1) * QB, head * LANES : (head + 1) * LANES] = (
                totals[head, here, :] * (1.0 / scale)
            ).astype(bf16)

    def add_rows(i, carry):
        return carry + column_sum(dproj_ref[pl.ds(i * rows, rows), :].astype(f32))

    sums_ref[...] = lax.fori_loop(
        0, tp_count, add_rows, jnp.zeros((1, dproj_ref.shape[1]), f32)
    )
    mixed_copy.wait()

    def settle(j, carry):
        context_copy(j).wait_send()
        return carry

    lax.fori_loop(1, tp_count, settle, 0)
    for part in range(halves):
        sends, _ = margin_plan(f, fsdp_count, part)
        for side in range(2):

            @pl.when(sends[side])
            def _(side=side, part=part):
                halo_copy(side, part).wait_send()

    mate_copy.wait()


def attend_back(fsdp_count, tp_count, lengths, dspread, wide, pairs, context, mate_grad, mixed):
    bf16 = jnp.bfloat16
    f32 = jnp.float32
    heads, group, _ = wide.shape
    _, rows, width = dspread.shape
    count = fsdp_count // 2
    kinds, _, _, depth, features = mate_grad.shape
    dma = pltpu.SemaphoreType.DMA
    return pl.pallas_call(
        functools.partial(attend_back_kernel, fsdp_count, tp_count),
        out_shape=(
            jax.ShapeDtypeStruct((group, heads * LANES + 2 * LANES), bf16),
            jax.ShapeDtypeStruct((kinds, depth, features), bf16),
            jax.ShapeDtypeStruct(mixed.shape, bf16),
            jax.ShapeDtypeStruct((1, heads * LANES + 2 * LANES), f32),
        ),
        in_specs=[pl.BlockSpec(memory_space=pltpu.SMEM)] + whole_specs(6),
        out_specs=tuple(whole_specs(4)),
        scratch_shapes=[
            pltpu.VMEM((tp_count, rows, width), bf16),
            pltpu.VMEM((heads, CLIP, LANES), bf16),
            pltpu.VMEM((heads, CLIP, LANES), bf16),
            pltpu.VMEM((heads, LANES, CLIP), bf16),
            pltpu.VMEM((heads, pairs.shape[0], LANES), f32),
            pltpu.VMEM((2, group // QB, heads, QB, LANES), bf16),
            pltpu.VMEM((2, group // QB, heads, QB, LANES), bf16),
            pltpu.VMEM((kinds, count, depth, features), bf16),
            pltpu.VMEM((count, kinds, depth, features), bf16),
            pltpu.VMEM((kinds, depth, features), f32),
            pltpu.VMEM((kinds, depth, features), bf16),
            dma((tp_count,)),
            dma((tp_count,)),
            dma,
            dma,
            dma,
            dma,
            dma((2, group // QB)),
            dma((2, group // QB)),
            dma((1,)),
            dma((1,)),
            dma((count,)),
            dma((count,)),
        ],
        compiler_params=pltpu.CompilerParams(
            collective_id=5, has_side_effects=True, vmem_limit_bytes=VMEM_LIMIT
        ),
        name="attend_back",
    )(lengths, dspread, wide, pairs, context, mate_grad, mixed)


def reduce_copies(f, t, fsdp_count, tp_count, vector, by_fsdp, by_tp, sends, recvs):
    def fsdp_copy(i):
        return remote(
            vector, by_fsdp.at[f], sends.at[i], recvs.at[f], lax.rem(f + i, fsdp_count), t
        )

    def tp_copy(j):
        return remote(
            by_tp.at[t],
            by_tp.at[t],
            sends.at[fsdp_count + j],
            recvs.at[fsdp_count + t],
            f,
            lax.rem(t + j, tp_count),
        )

    def start():
        def body(i, carry):
            fsdp_copy(i).start()
            return carry

        by_fsdp[f] = vector[...]
        lax.fori_loop(1, fsdp_count, body, 0)

    def middle():
        def wait(i, carry):
            source = lax.rem(f + i, fsdp_count)
            remote(
                vector, by_fsdp.at[source], sends.at[i], recvs.at[source], source, t
            ).wait_recv()
            return carry

        def add(i, total):
            return total + by_fsdp[i]

        def body(j, carry):
            tp_copy(j).start()
            return carry

        lax.fori_loop(1, fsdp_count, wait, 0)
        by_tp[t] = lax.fori_loop(0, fsdp_count, add, jnp.zeros(vector.shape, jnp.float32))
        lax.fori_loop(1, tp_count, body, 0)

    def finish():
        def wait(j, carry):
            source = lax.rem(t + j, tp_count)
            remote(
                vector,
                by_tp.at[source],
                sends.at[fsdp_count + j],
                recvs.at[fsdp_count + source],
                f,
                source,
            ).wait_recv()
            tp_copy(j).wait_send()
            return carry

        def drain(i, carry):
            fsdp_copy(i).wait_send()
            return carry

        lax.fori_loop(1, tp_count, wait, 0)
        lax.fori_loop(1, fsdp_count, drain, 0)

    return (start, middle, finish)


def finish_kernel(
    fsdp_count,
    tp_count,
    x_ref,
    gain_ref,
    shift_ref,
    dproj_ref,
    full_ref,
    normed_ref,
    gradient_ref,
    partial_ref,
    mixed_ref,
    own_grad,
    heads_grad,
    mate_ref,
    sums_ref,
    bias_ref,
    proj_ref,
    inputs_grad,
    outputs_ref,
    key_total,
    value_total,
    query_total,
    up_total,
    down_total,
    heads_total,
    gain1_total,
    shift1_total,
    gain2_total,
    shift2_total,
    out_bias_total,
    last_bias_total,
    query_bias_total,
    value_bias_total,
    bias_total,
    weight_grad,
    weight_first,
    weight_second,
    weight_sum,
    weight_total,
    own_first,
    own_second,
    own_total,
    heads_first,
    heads_second,
    heads_sum,
    part_ref,
    row_out,
    row_in,
    heads_out,
    heads_in,
    early,
    early_fsdp,
    early_tp,
    late,
    late_fsdp,
    late_tp,
    row_send,
    row_recv,
    side_send,
    side_recv,
    one_send,
    one_recv,
    weight_send,
    weight_recv,
    two_send,
    two_recv,
    own_send,
    own_recv,
    three_send,
    three_recv,
    early_send,
    early_recv,
    late_send,
    late_recv,
):
    f = lax.axis_index("fsdp")
    t = lax.axis_index("tp")
    bf16 = jnp.bfloat16
    f32 = jnp.float32
    rows, features = x_ref.shape
    proj_width = dproj_ref.shape[1]
    last = tp_count - 1
    sub = rows // 2
    units = bias_ref.shape[3]
    early[0:4, :] = sums_ref[...]
    early[4:5, :] = jnp.zeros((1, features), f32)
    early[4:5, 0:proj_width] = proj_ref[...]
    for level in range(2):
        for c in range(bias_ref.shape[1]):
            early[5 + level : 6 + level, c * units : (c + 1) * units] = bias_ref[level, c]
    greet(fsdp_count, tp_count, f, t)
    start_own, add_own, finish_own = scatter_copies(
        f,
        t,
        fsdp_count,
        (own_grad, heads_grad),
        (own_first, heads_first),
        (own_second, heads_second),
        two_send,
        two_recv,
        (own_send, three_send),
        (own_recv, three_recv),
    )
    start_own()
    start_early, middle_early, finish_early = reduce_copies(
        f, t, fsdp_count, tp_count, early, early_fsdp, early_tp, early_send, early_recv
    )
    start_late, middle_late, finish_late = reduce_copies(
        f, t, fsdp_count, tp_count, late, late_fsdp, late_tp, late_send, late_recv
    )
    start_weights, add_weights, finish_weights = scatter_copies(
        f,
        t,
        fsdp_count,
        (weight_grad,),
        (weight_first,),
        (weight_second,),
        one_send,
        one_recv,
        (weight_send,),
        (weight_recv,),
    )

    def row_copy(piece, side):
        return remote(
            row_out.at[piece],
            row_in.at[side, piece],
            row_send.at[piece],
            row_recv.at[side, piece],
            f,
            t + 1 if side == 0 else t - 1,
        )

    def relay(unit, carry):
        k, low = (unit // 2, lax.rem(unit, 2))
        for side, (block, valid, inner) in enumerate(
            ((last - k, last - k > t, t > 0), (k, k < t, t < last))
        ):
            piece = 2 * block + low
            here = pl.ds(pl.multiple_of(low * sub, sub), sub)

            @pl.when(valid & (inner | (unit >= 2)))
            def _(side=side, block=block, inner=inner, piece=piece, here=here):
                @pl.when(inner)
                def _():
                    row_copy(piece, side).wait_recv()
                    row_out[piece] = (
                        part_ref[block, here, :] + row_in[side, piece].astype(f32)
                    ).astype(bf16)

                @pl.when(jnp.logical_not(inner))
                def _():
                    row_out[piece] = part_ref[block, here, :].astype(bf16)

                @pl.when(unit >= 2)
                def _():
                    row_copy(piece + 2 - 4 * side, side).wait_send()

                row_copy(piece, side).start()

        return carry

    def partial_rows(k, carry):
        block = jnp.where(t < tp_count // 2, last - k, k)
        part_ref[block] = contract_cols(
            dproj_ref[pl.ds(pl.multiple_of(block * rows, rows), rows), :], full_ref[0]
        )
        for side, (first, end) in enumerate(((last, 0), (0, last))):

            @pl.when((k == 0) & (t == end))
            def _(side=side, first=first):
                for low in range(2):
                    row_out[2 * first + low] = part_ref[
                        first, low * sub : (low + 1) * sub, :
                    ].astype(bf16)
                    row_copy(2 * first + low, side).start()

        return carry

    lax.fori_loop(0, tp_count, partial_rows, 0)
    start_early()
    depth = weight_grad.shape[3]
    add_own()
    tall = 256

    def weight_part(c, carry):
        columns = pl.ds(pl.multiple_of(c * tall, tall), tall)
        total = jnp.zeros((tall, proj_width), f32)
        for block in range(tp_count):
            total = total + contract_rows(
                normed_ref[block, :, columns],
                dproj_ref[block * rows : (block + 1) * rows, :],
            )
        weight_sum[columns, :] = total.astype(bf16)
        return carry

    lax.fori_loop(0, features // tall, weight_part, 0)

    def arrange(i, carry):
        weight_grad[0, i // 2, lax.rem(i, 2)] = weight_sum[
            pl.ds(pl.multiple_of(i * depth, 8), depth), :
        ]
        return carry

    lax.fori_loop(0, fsdp_count, arrange, 0)
    start_weights()
    outputs_ref[...] = partial_ref[...] + mixed_ref[...].astype(f32)
    unit, spread, _ = normalize(x_ref[...], row_of(gain_ref), row_of(shift_ref))
    add_weights()
    middle_early()

    lax.fori_loop(0, 2 * last, relay, 0)
    finish_own((own_total, heads_sum))
    heads_out[...] = heads_sum[...].astype(bf16)

    def heads_copy(j):
        toward = lax.rem(t + j, tp_count)
        return remote(
            heads_out.at[toward],
            heads_in.at[t],
            side_send.at[j],
            side_recv.at[t],
            f,
            toward,
        )

    def heads_start(j, carry):
        heads_copy(j).start()
        return carry

    lax.fori_loop(1, tp_count, heads_start, 0)
    finish_weights((weight_total,))
    lane = lax.broadcasted_iota(jnp.int32, (depth, LANES), 1)
    tiles = [weight_total[0, :, j * LANES : (j + 1) * LANES] for j in range(5)]
    turned = [pltpu.roll(tile, HD, axis=1) for tile in tiles[:3]]
    key_total[:, 0:LANES] = jnp.where(lane < HD, tiles[0], turned[1])
    key_total[:, LANES:] = tiles[2][:, :HD]
    value_total[:, 0:LANES] = jnp.where(lane < HD, turned[0], tiles[1])
    value_total[:, LANES:] = turned[2][:, :HD]
    query_total[:, 0:LANES] = tiles[3]
    query_total[:, LANES:] = tiles[4][:, :HD]
    up_total[...] = own_total[0] + mate_ref[0].astype(f32)
    down_total[...] = own_total[1] + mate_ref[1].astype(f32)
    finish_early()
    for row, total in enumerate((gain2_total, shift2_total, out_bias_total, last_bias_total)):
        total[...] = jnp.sum(early_tp[:, row, :], axis=0)
    for j in range(tp_count):
        tiles = [early_tp[j, 4:5, i * LANES : (i + 1) * LANES] for i in range(5)]
        turned = [pltpu.roll(tile, HD, axis=1) for tile in tiles[:3]]
        value_bias_total[j : j + 1, 0:LANES] = jnp.where(lane[0:1] < HD, turned[0], tiles[1])
        value_bias_total[j : j + 1, LANES:] = turned[2][:, :HD]
        query_bias_total[j : j + 1, 0:LANES] = tiles[3]
        query_bias_total[j : j + 1, LANES:] = tiles[4][:, :HD]
        bias_total[j : j + 1, :] = (
            early_tp[j, 5:6, :] + early_tp[(j + tp_count // 2) % tp_count, 6:7, :]
        )

    for side, inner in enumerate((t > 0, t < last)):

        @pl.when(inner)
        def _(side=side):
            for low in range(2):
                row_copy(2 * t + low, side).wait_recv()
                part_ref[t, low * sub : (low + 1) * sub, :] += row_in[side, 2 * t + low].astype(
                    f32
                )

    dnorm = part_ref[t]
    late[0:1, :] = column_sum(dnorm * unit)
    late[1:2, :] = column_sum(dnorm)
    start_late()
    inputs_grad[...] = gradient_ref[...] + norm_back(dnorm, unit, spread, row_of(gain_ref))
    middle_late()

    for side, outer in enumerate((t < last, t > 0)):

        @pl.when(outer)
        def _(side=side):
            for low in range(2):
                row_copy(2 * (t + 1 - 2 * side) + low, side).wait_send()

    heads_total[...] = heads_sum[t]

    def heads_done(j, carry):
        source = lax.rem(t + j, tp_count)
        remote(
            heads_out.at[source],
            heads_in.at[source],
            side_send.at[j],
            side_recv.at[source],
            f,
            source,
        ).wait_recv()
        heads_total[...] += heads_in[source].astype(f32)
        heads_copy(j).wait_send()
        return carry

    lax.fori_loop(1, tp_count, heads_done, 0)
    finish_late()
    gain1_total[...] = jnp.sum(late_tp[:, 0, :], axis=0)
    shift1_total[...] = jnp.sum(late_tp[:, 1, :], axis=0)


def finish(
    fsdp_count,
    tp_count,
    x,
    gain,
    shift,
    dproj,
    full,
    normed,
    gradient,
    partial,
    mixed,
    own_grad,
    heads_grad,
    mate,
    sums,
    bias,
    proj,
):
    bf16 = jnp.bfloat16
    f32 = jnp.float32
    rows, features = x.shape
    kinds = own_grad.shape[0]
    _, _, _, depth, width = heads_grad.shape
    proj_width = dproj.shape[1]
    count = fsdp_count // 2
    dma = pltpu.SemaphoreType.DMA
    peers = fsdp_count + tp_count
    return pl.pallas_call(
        functools.partial(finish_kernel, fsdp_count, tp_count),
        out_shape=(
            jax.ShapeDtypeStruct((rows, features), f32),
            jax.ShapeDtypeStruct((rows, features), f32),
            jax.ShapeDtypeStruct((depth, width), f32),
            jax.ShapeDtypeStruct((depth, width), f32),
            jax.ShapeDtypeStruct((depth, width), f32),
            jax.ShapeDtypeStruct((depth, features), f32),
            jax.ShapeDtypeStruct((depth, features), f32),
            jax.ShapeDtypeStruct((depth, width), f32),
            *[jax.ShapeDtypeStruct((features,), f32)] * 6,
            jax.ShapeDtypeStruct((tp_count, width), f32),
            jax.ShapeDtypeStruct((tp_count, width), f32),
            jax.ShapeDtypeStruct((tp_count, features), f32),
        ),
        in_specs=whole_specs(15),
        out_specs=tuple(whole_specs(17)),
        scratch_shapes=[
            pltpu.VMEM((1, count, 2, depth, proj_width), bf16),
            pltpu.VMEM((1, count, depth, proj_width), bf16),
            pltpu.VMEM((count, 1, depth, proj_width), bf16),
            pltpu.VMEM((features, proj_width), bf16),
            pltpu.VMEM((1, depth, proj_width), f32),
            pltpu.VMEM((kinds, count, depth, features), bf16),
            pltpu.VMEM((count, kinds, depth, features), bf16),
            pltpu.VMEM((kinds, depth, features), f32),
            pltpu.VMEM((tp_count, count, depth, width), bf16),
            pltpu.VMEM((count, tp_count, depth, width), bf16),
            pltpu.VMEM((tp_count, depth, width), f32),
            pltpu.VMEM((tp_count, rows, features), f32),
            pltpu.VMEM((2 * tp_count, rows // 2, features), bf16),
            pltpu.VMEM((2, 2 * tp_count, rows // 2, features), bf16),
            pltpu.VMEM((tp_count, depth, width), bf16),
            pltpu.VMEM((tp_count, depth, width), bf16),
            pltpu.VMEM((7, features), f32),
            pltpu.VMEM((fsdp_count, 7, features), f32),
            pltpu.VMEM((tp_count, 7, features), f32),
            pltpu.VMEM((2, features), f32),
            pltpu.VMEM((fsdp_count, 2, features), f32),
            pltpu.VMEM((tp_count, 2, features), f32),
            dma((2 * tp_count,)),
            dma((2, 2 * tp_count)),
            dma((tp_count,)),
            dma((tp_count,)),
            dma((1,)),
            dma((1,)),
            dma((count,)),
            dma((count,)),
            dma((2,)),
            dma((2,)),
            dma((count,)),
            dma((count,)),
            dma((count,)),
            dma((count,)),
            dma((peers,)),
            dma((peers,)),
            dma((peers,)),
            dma((peers,)),
        ],
        compiler_params=pltpu.CompilerParams(
            collective_id=6, has_side_effects=True, vmem_limit_bytes=VMEM_LIMIT
        ),
        name="finish",
    )(
        x,
        gain,
        shift,
        dproj,
        full,
        normed,
        gradient,
        partial,
        mixed,
        own_grad,
        heads_grad,
        mate,
        sums,
        bias,
        proj,
    )


def pack_columns(key, value, query):
    lead = key.shape[:-1]
    heads = key.shape[-1] // HD
    pairs = jnp.stack([key.reshape(*lead, heads, HD), value.reshape(*lead, heads, HD)], axis=-2)
    spare = jnp.zeros((*lead, -key.shape[-1] % LANES), key.dtype)
    return jnp.concatenate([pairs.reshape(*lead, -1), query, spare], axis=-1)


def on_device(
    inputs,
    out_cotangent,
    clip_lengths,
    norm1_gain,
    norm1_shift,
    query_weight,
    query_bias,
    key_weight,
    value_weight,
    value_bias,
    out_weight,
    out_bias,
    norm2_gain,
    norm2_shift,
    fc1_weight,
    fc1_bias,
    fc2_weight,
    fc2_bias,
):
    f32 = jnp.float32
    tp_count = lax.axis_size("tp")
    fsdp_count = lax.axis_size("fsdp")
    margin = CLIP - QB
    local_width = query_weight.shape[1]
    heads_here = local_width // HD
    unit_count = fc1_weight.shape[0]
    by_tp = lambda bias: bias.reshape(tp_count, 1, local_width)
    pair_width = 2 * local_width
    mlp_own = jnp.stack([fc1_weight, fc2_weight])
    query, pairs, normed, attention_w, mlp_w, out_parts = project(
        fsdp_count,
        tp_count,
        inputs,
        norm1_gain,
        norm1_shift,
        pack_columns(key_weight, value_weight, query_weight)[None],
        pack_columns(jnp.zeros((tp_count, 1, local_width), f32), by_tp(value_bias), by_tp(query_bias)),
        mlp_own,
        out_weight,
        pair_width,
        margin,
    )
    spread, context, wide, mlp_other, out_full = attend(
        fsdp_count, tp_count, clip_lengths, query, pairs, mlp_own, out_parts, heads_here
    )
    unit_bias = jnp.swapaxes(fc1_bias.reshape(fsdp_count, tp_count, unit_count), 0, 1)
    (
        dhidden,
        outputs,
        mixed,
        dspread,
        own_grad,
        mate_grad,
        heads_grad,
        bias_part,
        sums,
    ) = by_rows(
        fsdp_count,
        tp_count,
        inputs,
        spread,
        out_full,
        (out_bias, norm2_gain, norm2_shift, fc2_bias),
        unit_bias.reshape(tp_count, -1, 1, 256),
        mlp_w,
        mlp_other,
        out_cotangent,
    )
    count = fsdp_count // 2
    by_owner = lambda grad: grad.reshape(grad.shape[0], count, 2, unit_count, -1)
    dproj, mate_total, mixed, proj_sums = attend_back(
        fsdp_count,
        tp_count,
        clip_lengths,
        dspread,
        wide,
        pairs,
        context,
        by_owner(mate_grad),
        mixed,
    )
    (
        inputs_grad,
        outputs,
        grad_key,
        grad_value,
        grad_query,
        grad_fc1,
        grad_fc2,
        grad_out,
        grad_gain1,
        grad_shift1,
        grad_gain2,
        grad_shift2,
        grad_obias,
        grad_b2,
        grad_qbias,
        grad_vbias,
        bias_total,
    ) = finish(
        fsdp_count,
        tp_count,
        inputs,
        norm1_gain,
        norm1_shift,
        dproj,
        attention_w,
        normed,
        dhidden,
        outputs,
        mixed,
        by_owner(own_grad),
        by_owner(heads_grad),
        mate_total,
        sums,
        bias_part,
        proj_sums,
    )
    grad_qbias = grad_qbias.reshape(-1)
    grad_vbias = grad_vbias.reshape(-1)
    grad_b1 = jnp.swapaxes(bias_total.reshape(tp_count, fsdp_count, unit_count), 0, 1).reshape(-1)
    return (
        outputs,
        inputs_grad,
        grad_gain1,
        grad_shift1,
        grad_query,
        grad_qbias,
        grad_key,
        grad_value,
        grad_vbias,
        grad_out,
        grad_obias,
        grad_gain2,
        grad_shift2,
        grad_fc1,
        grad_b1,
        grad_fc2,
        grad_b2,
    )


def solution(mesh):
    in_specs = (
        P(("fsdp", "tp"), None),
        P("fsdp", None),
        P(),
        P(),
        P(),
        P("fsdp", "tp"),
        P(),
        P("fsdp", "tp"),
        P("fsdp", "tp"),
        P(),
        P("fsdp", "tp"),
        P(),
        P(),
        P(),
        P(("fsdp", "tp"), None),
        P(),
        P(("fsdp", "tp"), None),
        P(),
    )
    out_specs = (
        P(("fsdp", "tp"), None),
        P(("fsdp", "tp"), None),
        P(),
        P(),
        P("fsdp", "tp"),
        P(),
        P("fsdp", "tp"),
        P("fsdp", "tp"),
        P(),
        P("fsdp", "tp"),
        P(),
        P(),
        P(),
        P(("fsdp", "tp"), None),
        P(),
        P(("fsdp", "tp"), None),
        P(),
    )
    return jax.shard_map(
        on_device, mesh=mesh, in_specs=in_specs, out_specs=out_specs, check_vma=False
    )
```

```python
import functools
import math

import jax
import jax.numpy as jnp
from jax import lax
from jax.experimental import pallas as pl
from jax.experimental.pallas import tpu as pltpu
from jax.sharding import PartitionSpec as P

HD = 64
CLIP = 1536
QB = 512


eps_norm = 1e-05
root_half = 0.7071067811865476
inv_root_tau = 0.3989422804014327
far_negative = -1e30


def normalize(rows, gain, shift):
    centre = jnp.mean(rows, axis=-1, keepdims=True)
    centred = rows - centre
    inv_spread = lax.rsqrt(jnp.mean(centred * centred, axis=-1, keepdims=True) + eps_norm)
    unit_rows = centred * inv_spread
    return (unit_rows, inv_spread, unit_rows * gain + shift)


def norm_back(upstream, unit_rows, inv_spread, gain):
    scaled = upstream * gain
    return inv_spread * (
        scaled
        - jnp.mean(scaled, axis=-1, keepdims=True)
        - unit_rows * jnp.mean(scaled * unit_rows, axis=-1, keepdims=True)
    )


def contract_rows(left_rows, right_rows):
    return lax.dot_general(
        left_rows, right_rows, (((0,), (0,)), ((), ())), preferred_element_type=jnp.float32
    )


def contract_cols(left_rows, right_rows):
    return lax.dot_general(
        left_rows, right_rows, (((1,), (1,)), ((), ())), preferred_element_type=jnp.float32
    )


MESH = pl.DeviceIdType.MESH
VMEM_LIMIT = 32 * 1024 * 1024
LANES = 128


def row_of(ref):
    return ref[...].reshape(1, -1)


def remote(source, target, send_sem, recv_sem, fsdp_to, tp_to):
    return pltpu.make_async_remote_copy(
        src_ref=source,
        dst_ref=target,
        send_sem=send_sem,
        recv_sem=recv_sem,
        device_id=(fsdp_to, tp_to),
        device_id_type=MESH,
    )


def greet(fsdp_count, tp_count, f, t):
    barrier = pltpu.get_barrier_semaphore()

    def greet_fsdp(i, carry):
        pl.semaphore_signal(
            barrier, inc=1, device_id=(lax.rem(f + i, fsdp_count), t), device_id_type=MESH
        )
        return carry

    def greet_tp(j, carry):
        pl.semaphore_signal(
            barrier, inc=1, device_id=(f, lax.rem(t + j, tp_count)), device_id_type=MESH
        )
        return carry

    lax.fori_loop(1, fsdp_count, greet_fsdp, 0)
    lax.fori_loop(1, tp_count, greet_tp, 0)
    pl.semaphore_wait(barrier, fsdp_count + tp_count - 2)


def gather_copies(f, t, fsdp_count, sources, targets, depth, sends, recvs):
    partner = f + 1 - 2 * lax.rem(f, 2)

    def piece(target, owner):
        return target.at[:, pl.ds(owner * depth, depth)]

    def copies(owner, toward, lane, first):
        return [
            remote(
                source if first else piece(target, owner),
                piece(target, owner),
                send.at[lane],
                recv.at[owner],
                toward,
                t,
            )
            for source, target, send, recv in zip(sources, targets, sends, recvs)
        ]

    def start():
        def body(i, carry):
            for handle in copies(f, lax.rem(f + 2 * i, fsdp_count), i, True):
                handle.start()
            return carry

        lax.fori_loop(1, fsdp_count // 2, body, 0)
        for handle in copies(f, partner, 0, True):
            handle.start()
        for source, target in zip(sources, targets):
            target[:, pl.ds(f * depth, depth), :] = source[...]

    def relay():
        def body(i, carry):
            owner = lax.rem(f + fsdp_count - 2 * i, fsdp_count)
            for handle in copies(owner, partner, fsdp_count // 2 + i, False):
                handle.wait_recv()
                handle.start()
            return carry

        lax.fori_loop(1, fsdp_count // 2, body, 0)

    def finish():
        def body(i, carry):
            owner = lax.rem(partner + 2 * i, fsdp_count)
            for handle in copies(owner, partner, 0, False):
                handle.wait_recv()
            return carry

        lax.fori_loop(0, fsdp_count // 2, body, 0)

    def drain():
        def body(i, carry):
            for handle in copies(f, lax.rem(f + 2 * i, fsdp_count), i, True):
                handle.wait_send()
            for handle in copies(
                lax.rem(f + fsdp_count - 2 * i, fsdp_count),
                partner,
                fsdp_count // 2 + i,
                False,
            ):
                handle.wait_send()
            return carry

        lax.fori_loop(1, fsdp_count // 2, body, 0)
        for handle in copies(f, partner, 0, True):
            handle.wait_send()

    return (start, relay, finish, drain)


def swapped(tile):
    return pltpu.roll(tile, HD, axis=1)


def joined(low, high):
    lane = lax.broadcasted_iota(jnp.int32, low.shape, 1)
    return jnp.where(lane < HD, low, high)


def pack_weights(key_ref, value_ref, query_ref, packed_ref):
    def tiles(ref):
        spare = jnp.zeros((ref.shape[0], HD), jnp.float32)
        return (
            ref[:, :LANES].astype(jnp.float32),
            jnp.concatenate([ref[:, LANES:].astype(jnp.float32), spare], axis=1),
        )

    key, value, query = tiles(key_ref), tiles(value_ref), tiles(query_ref)
    packed = (
        joined(key[0], swapped(value[0])),
        joined(swapped(key[0]), value[0]),
        joined(key[1], swapped(value[1])),
        *query,
    )
    for j, tile in enumerate(packed):
        packed_ref[0, :, j * LANES : (j + 1) * LANES] = tile.astype(jnp.bfloat16)


def pack_bias(t, tp_count, value, query):
    def half(row, head, high):
        tile = row[:, (head // 2) * LANES : (head // 2 + 1) * LANES]
        return tile if head % 2 == high else swapped(tile)

    heads = value.shape[1] // HD // tp_count
    none = jnp.zeros((1, LANES), jnp.float32)
    total = jnp.zeros((1, (heads + 2) * LANES), jnp.float32)
    for j in range(tp_count):
        first = j * heads
        tiles = [joined(none, half(value, first + h, 1)) for h in range(heads)]
        tiles.append(joined(half(query, first, 0), half(query, first + 1, 1)))
        tiles.append(joined(half(query, first + 2, 0), none))
        total = total + jnp.where(t == j, jnp.concatenate(tiles, axis=1), 0.0)
    return total


def project_kernel(
    fsdp_count,
    tp_count,
    x_hbm,
    gain_hbm,
    shift_hbm,
    key_hbm,
    value_hbm,
    query_hbm,
    value_bias_hbm,
    query_bias_hbm,
    up_hbm,
    down_hbm,
    out_hbm,
    query_ref,
    pair_ref,
    normed_ref,
    full_ref,
    mlp_full,
    heads_ref,
    mlp_ref,
    x_ref,
    gain_ref,
    shift_ref,
    key_weight,
    value_weight,
    query_weight,
    value_bias,
    query_bias,
    out_ref,
    weight_ref,
    bias_ref,
    load_sem,
    side_send,
    side_recv,
    weight_send,
    weight_recv,
    mlp_send,
    mlp_recv,
    row_send,
    row_recv,
    halo_send,
    halo_recv,
):
    f = lax.axis_index("fsdp")
    t = lax.axis_index("tp")
    rows = x_ref.shape[0]
    depth = weight_ref.shape[1]
    group = rows * tp_count
    pair_width = pair_ref.shape[1]
    margin = (pair_ref.shape[0] - group) // 2
    per_half = tp_count // 2
    phase = lax.rem(f, 3)
    above = f + 1 < fsdp_count
    below = f > 0
    blank = jnp.zeros((256, pair_width), jnp.bfloat16)
    loads = [
        pltpu.make_async_copy(source, target, load_sem.at[i])
        for i, (source, target) in enumerate(
            (
                (key_hbm, key_weight),
                (value_hbm, value_weight),
                (query_hbm, query_weight),
                (x_hbm, x_ref),
                (gain_hbm, gain_ref),
                (shift_hbm, shift_ref),
                (value_bias_hbm, value_bias),
                (query_bias_hbm, query_bias),
                (out_hbm, out_ref),
                (up_hbm, mlp_ref.at[0]),
                (down_hbm, mlp_ref.at[1]),
            )
        )
    ]
    for load in loads:
        load.start()

    def clear(i, carry):
        pair_ref[pl.ds(i * 256, 256), :] = blank
        pair_ref[pl.ds(margin + group + i * 256, 256), :] = blank
        return carry

    lax.fori_loop(0, margin // 256, clear, 0)
    for load in loads:
        load.wait()
    pack_weights(key_weight, value_weight, query_weight, weight_ref)
    greet(fsdp_count, tp_count, f, t)
    bias_ref[...] = pack_bias(t, tp_count, row_of(value_bias), row_of(query_bias))
    start_weights, relay_weights, finish_weights, drain_weights = gather_copies(
        f, t, fsdp_count, (weight_ref,), (full_ref,), depth, (weight_send,), (weight_recv,)
    )
    start_mlp, relay_mlp, finish_mlp, drain_mlp = gather_copies(
        f, t, fsdp_count, (mlp_ref,), (mlp_full,), depth, (mlp_send,), (mlp_recv,)
    )
    start_weights()
    _, _, normed = normalize(x_ref[...], row_of(gain_ref), row_of(shift_ref))
    normed_ref[t] = normed.astype(jnp.bfloat16)

    def row_copy(source, lane, toward):
        return remote(
            normed_ref.at[source],
            normed_ref.at[source],
            row_send.at[lane],
            row_recv.at[source],
            f,
            toward,
        )

    @pl.when(t > 0)
    def _():
        row_copy(t, tp_count, t - 1).start()

    @pl.when(t < tp_count - 1)
    def _():
        row_copy(t, tp_count + 1, t + 1).start()

    def heads_copy(j):
        return remote(
            out_ref,
            heads_ref.at[t],
            side_send.at[j],
            side_recv.at[j],
            f,
            lax.rem(t + j, tp_count),
        )

    def heads_start(j, carry):
        heads_copy(j).start()
        return carry

    def heads_done(j, carry):
        heads_copy(j).wait_send()
        source = lax.rem(t + tp_count - j, tp_count)
        remote(
            out_ref, heads_ref.at[source], side_send.at[j], side_recv.at[j], f, source
        ).wait_recv()
        return carry

    heads_ref[t] = out_ref[...]
    lax.fori_loop(1, tp_count, heads_start, 0)
    relay_weights()
    start_mlp()
    finish_weights()

    def halo_copy(source, side):
        return remote(
            pair_ref.at[pl.ds(margin + source * rows, rows)],
            pair_ref.at[pl.ds((0 if side == 0 else margin + group) + source * rows, rows)],
            halo_send.at[side, source],
            halo_recv.at[side, source],
            f + 1 if side == 0 else f - 1,
            t,
        )

    def halo_sends(source):
        late = source >= per_half
        return (
            above & ((phase == 0) | ((phase == 1) & late)),
            below & ((phase == 2) | ((phase == 1) & jnp.logical_not(late))),
        )

    def halo_receives(source):
        late = source >= per_half
        return (
            below & ((phase == 1) | ((phase == 2) & late)),
            above & ((phase == 1) | ((phase == 0) & jnp.logical_not(late))),
        )

    def compute(source):
        out = jnp.dot(normed_ref[source], full_ref[0], preferred_element_type=jnp.float32)
        out = (out + bias_ref[...]).astype(jnp.bfloat16)
        pair_ref[pl.ds(margin + source * rows, rows), :] = out[:, :pair_width]
        for side, needed in enumerate(halo_sends(source)):

            @pl.when(needed)
            def _(side=side):
                halo_copy(source, side).start()

        query_ref[pl.ds(source * rows, rows), :] = out[:, pair_width:]

    compute(t)

    def arrival(k):
        step = k // 2 + 1
        side = 2 * lax.rem(k, 2) - 1
        source = t + side * step
        onward = t - side
        valid = (source >= 0) & (source < tp_count)
        return (source, onward, valid, valid & (onward >= 0) & (onward < tp_count))

    def receive(step, carry):
        for side in range(2):
            source, onward, valid, forward = arrival(2 * step + side)

            @pl.when(valid)
            def _(source=source, onward=onward, forward=forward):
                row_copy(source, 0, t).wait_recv()

                @pl.when(forward)
                def _():
                    row_copy(source, source, onward).start()

        def work(side, inner):
            source, _, valid, _ = arrival(2 * step + side)

            @pl.when(valid)
            def _():
                compute(source)

            return inner

        return lax.fori_loop(0, 2, work, carry)

    lax.fori_loop(0, tp_count - 1, receive, 0)
    relay_mlp()
    lax.fori_loop(1, tp_count, heads_done, 0)

    def sent(k, carry):
        source, onward, valid, forward = arrival(k)

        @pl.when(forward)
        def _():
            row_copy(source, source, onward).wait_send()

        return carry

    lax.fori_loop(0, 2 * (tp_count - 1), sent, 0)

    @pl.when(t > 0)
    def _():
        row_copy(t, tp_count, t - 1).wait_send()

    @pl.when(t < tp_count - 1)
    def _():
        row_copy(t, tp_count + 1, t + 1).wait_send()

    def halo_done(source, carry):
        for side, (sends, receives) in enumerate(zip(halo_sends(source), halo_receives(source))):

            @pl.when(sends)
            def _(side=side):
                halo_copy(source, side).wait_send()

            @pl.when(receives)
            def _(side=side):
                halo_copy(source, side).wait_recv()

        return carry

    lax.fori_loop(0, tp_count, halo_done, 0)
    drain_weights()
    finish_mlp()
    drain_mlp()


def whole_specs(count):
    return [pl.BlockSpec(memory_space=pltpu.VMEM)] * count


def project(fsdp_count, tp_count, x, gain, shift, weights, biases, mlp, out_weight, margin):
    bf16 = jnp.bfloat16
    rows, features = x.shape
    group = rows * tp_count
    depth, width = out_weight.shape
    pair_width = width // HD * LANES
    packed_width = pair_width + 2 * LANES
    dma = pltpu.SemaphoreType.DMA
    return pl.pallas_call(
        functools.partial(project_kernel, fsdp_count, tp_count),
        out_shape=(
            jax.ShapeDtypeStruct((group, 2 * LANES), bf16),
            jax.ShapeDtypeStruct((group + 2 * margin, pair_width), bf16),
            jax.ShapeDtypeStruct((tp_count, rows, features), bf16),
            jax.ShapeDtypeStruct((1, depth * fsdp_count, packed_width), bf16),
            jax.ShapeDtypeStruct((2, depth * fsdp_count, features), bf16),
            jax.ShapeDtypeStruct((tp_count, *out_weight.shape), bf16),
            jax.ShapeDtypeStruct((2, depth, features), bf16),
        ),
        in_specs=[pl.BlockSpec(memory_space=pltpu.MemorySpace.HBM)] * 11,
        out_specs=tuple(whole_specs(7)),
        scratch_shapes=[
            *[
                pltpu.VMEM(v.shape, v.dtype)
                for v in (x, gain, shift, *weights, *biases, out_weight)
            ],
            pltpu.VMEM((1, depth, packed_width), bf16),
            pltpu.VMEM((1, packed_width), jnp.float32),
            dma((11,)),
            dma((tp_count,)),
            dma((tp_count,)),
            dma((fsdp_count,)),
            dma((fsdp_count,)),
            dma((fsdp_count,)),
            dma((fsdp_count,)),
            dma((tp_count + 2,)),
            dma((tp_count,)),
            dma((2, tp_count)),
            dma((2, tp_count)),
        ],
        compiler_params=pltpu.CompilerParams(
            collective_id=1, has_side_effects=True, vmem_limit_bytes=VMEM_LIMIT
        ),
        name="project",
    )(x, gain, shift, *weights, *biases, *mlp, out_weight)


def block_clip(f, part, margin):
    phase = lax.rem(f, 3)
    start = jnp.where(
        phase == 0,
        margin,
        jnp.where(phase == 2, margin - QB, jnp.where(part == 0, 0, margin + QB)),
    )
    return (pl.multiple_of(start, QB), (2 * f + part) // 3)


def head_tiles(pair, length):
    lane = lax.broadcasted_iota(jnp.int32, pair.shape, 1)
    row = lax.broadcasted_iota(jnp.int32, pair.shape, 0)
    extra = jnp.where(
        lane == HD,
        jnp.where(row < length, 0.0, far_negative),
        jnp.where(lane <= HD + 3, 1.0, 0.0),
    )
    return jnp.where(lane < HD, pair, extra)


def spread_heads(rows, head):
    tile = rows[:, (head // 2) * LANES : (head // 2 + 1) * LANES]
    return pltpu.roll(tile, HD, axis=1) if head % 2 else tile


def three_parts(column):
    high = column.astype(jnp.bfloat16).astype(jnp.float32)
    rest = column - high
    middle = rest.astype(jnp.bfloat16).astype(jnp.float32)
    return (high, middle, rest - middle)


def attend_kernel(
    fsdp_count,
    tp_count,
    lengths_ref,
    query_ref,
    pair_ref,
    mlp_ref,
    out_ref,
    spread_ref,
    context_ref,
    wide_ref,
    mlp_full,
    out_full,
    mate_ref,
    key_tiles,
    value_tiles,
    mate_send,
    mate_recv,
    context_send,
    context_recv,
    mlp_send,
    mlp_recv,
    out_send,
    out_recv,
):
    f = lax.axis_index("fsdp")
    t = lax.axis_index("tp")
    bf16 = jnp.bfloat16
    f32 = jnp.float32
    rows = spread_ref.shape[1]
    heads = wide_ref.shape[0]
    group = rows * tp_count
    margin = (pair_ref.shape[0] - group) // 2
    greet(fsdp_count, tp_count, f, t)
    depth = mlp_ref.shape[1]
    start_out, relay_out, finish_out, drain_out = gather_copies(
        f, t, fsdp_count, (out_ref,), (out_full,), depth, (out_send,), (out_recv,)
    )
    mates = [
        remote(
            mlp_ref.at[i],
            mate_ref.at[i],
            mate_send.at[i],
            mate_recv.at[i],
            f,
            lax.rem(t + tp_count // 2, tp_count),
        )
        for i in range(2)
    ]
    gathers = [
        gather_copies(
            f,
            t,
            fsdp_count,
            (mate_ref.at[pl.ds(i, 1)],),
            (mlp_full.at[pl.ds(i, 1)],),
            depth,
            (mlp_send.at[i],),
            (mlp_recv.at[i],),
        )
        for i in range(2)
    ]
    start_out()
    mates[0].start()
    mates[1].start()
    per_half = tp_count // 2

    def context_copy(toward):
        return remote(
            context_ref.at[pl.ds(toward * rows, rows)],
            spread_ref.at[t],
            context_send.at[toward],
            context_recv.at[t],
            f,
            toward,
        )

    lane = lax.broadcasted_iota(jnp.int32, (rows, LANES), 1)
    row = lax.broadcasted_iota(jnp.int32, (LANES, rows), 0)
    tall = lax.broadcasted_iota(jnp.int32, (LANES, CLIP), 0)

    def half(step, carry):
        part = lax.rem(t // per_half + 1 + step, 2)
        first, clip = block_clip(f, part, margin)
        length = lengths_ref[clip]
        for head in range(heads):
            pair = pair_ref[pl.ds(first, CLIP), head * LANES : (head + 1) * LANES].astype(f32)
            key_tiles[head] = head_tiles(pair, length).astype(bf16)
            value_tiles[head] = jnp.where(tall < HD, 1.0, pair.T).astype(bf16)

        def block(i, inner):
            within = lax.rem(lax.rem(t, per_half) + 1 + i, per_half)
            index = part * per_half + within
            here = pl.ds(pl.multiple_of(index * rows, rows), rows)
            query = query_ref[here, :].astype(f32) * (1.0 / math.sqrt(HD))
            parts = []
            for head in range(heads):
                wide = jnp.where(
                    lane < HD, spread_heads(query, head), jnp.where(lane == HD, 1.0, 0.0)
                )
                scores = lax.dot_general(
                    key_tiles[head],
                    wide.astype(bf16),
                    (((1,), (1,)), ((), ())),
                    preferred_element_type=f32,
                )
                highest = jnp.max(scores, axis=0, keepdims=True)
                weights = jnp.exp(scores - highest).astype(bf16)
                summed = jnp.dot(value_tiles[head], weights, preferred_element_type=f32)
                total = summed[0:1, :]
                log_total = highest + jnp.log(total)
                turned = jnp.where(row == 0, log_total, summed * (1.0 / total)).T
                high, middle, low = three_parts(turned[:, 0:1])
                wide_ref[head, here, :] = jnp.where(
                    lane == HD + 1,
                    -high,
                    jnp.where(lane == HD + 2, -middle, jnp.where(lane == HD + 3, -low, wide)),
                ).astype(bf16)
                parts.append(turned)
            context_ref[here, 0:LANES] = jnp.where(
                lane < HD, pltpu.roll(parts[0], HD, axis=1), parts[1]
            ).astype(bf16)
            context_ref[here, LANES : LANES + HD] = pltpu.roll(parts[2], HD, axis=1)[
                :, :HD
            ].astype(bf16)

            @pl.when(index == t)
            def _():
                spread_ref[t] = context_ref[here, :]

            @pl.when(index != t)
            def _():
                context_copy(index).start()

            for turn in range(2):

                @pl.when((step == 0) & (i == turn))
                def _(turn=turn):
                    mates[turn].wait()
                    gathers[turn][0]()

                @pl.when((step == 1) & (i == turn))
                def _(turn=turn):
                    gathers[turn][1]()

            return inner

        lax.fori_loop(0, per_half, block, 0)

        @pl.when(step == 0)
        def _():
            relay_out()

        return carry

    lax.fori_loop(0, 2, half, 0)

    def settle(j, carry):
        toward = lax.rem(t + j, tp_count)
        context_copy(toward).wait_send()
        remote(
            context_ref.at[pl.ds(0, rows)],
            spread_ref.at[toward],
            context_send.at[toward],
            context_recv.at[toward],
            f,
            toward,
        ).wait_recv()
        return carry

    lax.fori_loop(1, tp_count, settle, 0)
    finish_out()
    drain_out()
    for _, _, finish_mlp, drain_mlp in gathers:
        finish_mlp()
        drain_mlp()


def attend(fsdp_count, tp_count, lengths, query, pairs, mlp, out_weights, heads):
    bf16 = jnp.bfloat16
    group = query.shape[0]
    rows = group // tp_count
    width = heads * HD
    dma = pltpu.SemaphoreType.DMA
    depth = mlp.shape[1]
    return pl.pallas_call(
        functools.partial(attend_kernel, fsdp_count, tp_count),
        out_shape=(
            jax.ShapeDtypeStruct((tp_count, rows, width), bf16),
            jax.ShapeDtypeStruct((group, width), bf16),
            jax.ShapeDtypeStruct((heads, group, LANES), bf16),
            jax.ShapeDtypeStruct((mlp.shape[0], depth * fsdp_count, mlp.shape[2]), bf16),
            jax.ShapeDtypeStruct((tp_count, depth * fsdp_count, width), bf16),
        ),
        in_specs=[pl.BlockSpec(memory_space=pltpu.SMEM)] + whole_specs(4),
        out_specs=tuple(whole_specs(5)),
        scratch_shapes=[
            pltpu.VMEM(mlp.shape, bf16),
            pltpu.VMEM((heads, CLIP, LANES), bf16),
            pltpu.VMEM((heads, LANES, CLIP), bf16),
            dma((2,)),
            dma((2,)),
            dma((tp_count,)),
            dma((tp_count,)),
            dma((2, fsdp_count)),
            dma((2, fsdp_count)),
            dma((fsdp_count,)),
            dma((fsdp_count,)),
        ],
        compiler_params=pltpu.CompilerParams(
            collective_id=2, has_side_effects=True, vmem_limit_bytes=VMEM_LIMIT
        ),
        name="attend",
    )(lengths, query, pairs, mlp, out_weights)


def column_sum(rows):
    return jnp.sum(rows, axis=0, keepdims=True)


def rows_kernel(
    fsdp_count,
    tp_count,
    x_ref,
    spread_ref,
    heads_ref,
    out_bias_ref,
    gain_ref,
    shift_ref,
    last_bias_ref,
    bias_ref,
    own_ref,
    mate_ref,
    cotangent_ref,
    gradient_ref,
    outputs_ref,
    mixed_ref,
    context_ref,
    own_grad,
    mate_grad,
    heads_grad,
    bias_grad,
    sums_ref,
    upstream,
    rounded,
    hidden_ref,
    unit_ref,
    normed_ref,
    active_ref,
    slope_ref,
    mixed_sum,
    norm_sum,
    norm_out,
    norm_in,
    load_sem,
    row_send,
    row_recv,
    norm_send,
    norm_recv,
):
    f = lax.axis_index("fsdp")
    t = lax.axis_index("tp")
    bf16 = jnp.bfloat16
    f32 = jnp.float32
    rows = x_ref.shape[0]
    tile = 256
    side = lax.rem(t, 2)
    peer = t + 1 - 2 * side
    load = pltpu.make_async_copy(
        cotangent_ref.at[pl.ds((t - side) * rows, 2 * rows)], upstream, load_sem
    )
    load.start()
    barrier = pltpu.get_barrier_semaphore()
    pl.semaphore_signal(barrier, inc=1, device_id=(f, peer), device_id_type=MESH)
    pl.semaphore_wait(barrier, 1)

    hidden = x_ref[...] + row_of(out_bias_ref)
    for j in range(tp_count):
        hidden = hidden + lax.dot_general(
            spread_ref[j], heads_ref[j], (((1,), (1,)), ((), ())), preferred_element_type=f32
        )
    hidden_ref[...] = hidden
    unit, spread, normed = normalize(hidden, row_of(gain_ref), row_of(shift_ref))
    unit_ref[...] = unit
    normed_ref[side] = normed.astype(bf16)
    row_copy = remote(normed_ref.at[side], normed_ref.at[side], row_send, row_recv, f, peer)
    row_copy.start()
    load.wait()

    def rounding(i, carry):
        rounded[pl.ds(i * rows, rows), :] = upstream[pl.ds(i * rows, rows), :].astype(bf16)
        return carry

    lax.fori_loop(0, 2, rounding, 0)
    mixed_sum[...] = jnp.zeros(mixed_sum.shape, f32)
    norm_sum[...] = jnp.zeros(norm_sum.shape, f32)
    chunks = own_ref.shape[1] // tile
    mate = lax.rem(t + tp_count // 2, tp_count)

    def feed_forward(turn, carry):
        which = lax.rem(side + turn, 2)

        @pl.when(turn == 1)
        def _():
            row_copy.wait_recv()

        here = pl.ds(pl.multiple_of(which * rows, rows), rows)
        normed_rows = normed_ref[which]
        upstream_rows = rounded[here, :]

        for level, (weights, owner) in enumerate(((own_ref, t), (mate_ref, mate))):

            def chunk(c, inner, weights=weights, owner=owner, level=level):
                units = pl.ds(pl.multiple_of(c * tile, tile), tile)
                up = weights[0, units, :]
                down = weights[1, units, :]
                preact = (
                    lax.dot_general(
                        normed_rows, up, (((1,), (1,)), ((), ())), preferred_element_type=f32
                    )
                    + bias_ref[owner, c]
                )
                cdf = 0.5 * (1.0 + lax.erf(preact * root_half))
                active = (preact * cdf).astype(bf16)
                slope = cdf + preact * jnp.exp(-0.5 * preact * preact) * inv_root_tau
                dactive = lax.dot_general(
                    upstream_rows, down, (((1,), (1,)), ((), ())), preferred_element_type=f32
                )
                dpreact = (dactive * slope).astype(bf16)
                active_ref[level, c, here, :] = active
                slope_ref[level, c, here, :] = dpreact
                norm_sum[which] += jnp.dot(dpreact, up, preferred_element_type=f32)
                mixed_sum[which] += jnp.dot(active, down, preferred_element_type=f32)
                return inner

            lax.fori_loop(0, chunks, chunk, 0)
        return carry

    lax.fori_loop(0, 2, feed_forward, 0)
    norm_out[...] = norm_sum[1 - side].astype(bf16)
    norm_copy = remote(norm_out, norm_in, norm_send, norm_recv, f, peer)
    norm_copy.start()
    mixed_ref[...] = mixed_sum[1 - side].astype(bf16)
    outputs_ref[...] = hidden_ref[...] + mixed_sum[side] + row_of(last_bias_ref)

    for level, grad in enumerate((own_grad, mate_grad)):

        def weight_grads(c, carry, level=level, grad=grad):
            units = pl.ds(pl.multiple_of(c * tile, tile), tile)
            slopes = slope_ref[level, c]
            both = jnp.concatenate([normed_ref[0], normed_ref[1]], axis=0)
            grad[0, units, :] = contract_rows(slopes, both).astype(bf16)
            grad[1, units, :] = contract_rows(active_ref[level, c], rounded[...]).astype(bf16)
            bias_grad[level, c] = column_sum(slopes.astype(f32))
            return carry

        lax.fori_loop(0, chunks, weight_grads, 0)

    norm_copy.wait()
    dnorm = norm_sum[side] + norm_in[...].astype(f32)
    unit = unit_ref[...]
    cotangent = upstream[pl.ds(pl.multiple_of(side * rows, rows), rows), :]
    gradient = cotangent + norm_back(dnorm, unit, spread, row_of(gain_ref))
    gradient_ref[...] = gradient
    sums_ref[0:1, :] = column_sum(dnorm * unit)
    sums_ref[1:2, :] = column_sum(dnorm)
    sums_ref[2:3, :] = column_sum(gradient)
    sums_ref[3:4, :] = column_sum(cotangent)
    gradient = gradient.astype(bf16)
    for j in range(tp_count):
        context_ref[j] = jnp.dot(gradient, heads_ref[j], preferred_element_type=f32).astype(bf16)
        heads_grad[j] = contract_rows(gradient, spread_ref[j]).astype(bf16)
    row_copy.wait_send()


def by_rows(fsdp_count, tp_count, x, spread, heads, vectors, bias, own, mate, cotangent):
    bf16 = jnp.bfloat16
    f32 = jnp.float32
    rows, features = x.shape
    units = own.shape[1]
    chunks = units // 256
    dma = pltpu.SemaphoreType.DMA
    return pl.pallas_call(
        functools.partial(rows_kernel, fsdp_count, tp_count),
        out_shape=(
            jax.ShapeDtypeStruct((rows, features), f32),
            jax.ShapeDtypeStruct((rows, features), f32),
            jax.ShapeDtypeStruct((rows, features), bf16),
            jax.ShapeDtypeStruct(spread.shape, bf16),
            jax.ShapeDtypeStruct(own.shape, bf16),
            jax.ShapeDtypeStruct(own.shape, bf16),
            jax.ShapeDtypeStruct(heads.shape, bf16),
            jax.ShapeDtypeStruct((2, chunks, 1, 256), f32),
            jax.ShapeDtypeStruct((4, features), f32),
        ),
        in_specs=whole_specs(10) + [pl.BlockSpec(memory_space=pl.ANY)],
        out_specs=tuple(whole_specs(9)),
        scratch_shapes=[
            pltpu.VMEM((2 * rows, features), f32),
            pltpu.VMEM((2 * rows, features), bf16),
            pltpu.VMEM((rows, features), f32),
            pltpu.VMEM((rows, features), f32),
            pltpu.VMEM((2, rows, features), bf16),
            pltpu.VMEM((2, chunks, 2 * rows, 256), bf16),
            pltpu.VMEM((2, chunks, 2 * rows, 256), bf16),
            pltpu.VMEM((2, rows, features), f32),
            pltpu.VMEM((2, rows, features), f32),
            pltpu.VMEM((rows, features), bf16),
            pltpu.VMEM((rows, features), bf16),
            dma,
            dma,
            dma,
            dma,
            dma,
        ],
        compiler_params=pltpu.CompilerParams(
            collective_id=4, has_side_effects=True, vmem_limit_bytes=VMEM_LIMIT
        ),
        name="by_rows",
    )(x, spread, heads, *vectors, bias, own, mate, cotangent)


def margin_plan(f, fsdp_count, part):
    phase = lax.rem(f, 3)
    above = f + 1 < fsdp_count
    below = f > 0
    sends = (
        below & ((phase == 1) | ((phase == 2) & (part == 1))),
        above & ((phase == 1) | ((phase == 0) & (part == 0))),
    )
    receives = (
        above & ((phase == 0) | ((phase == 1) & (part == 1))),
        below & ((phase == 2) | ((phase == 1) & (part == 0))),
    )
    return (sends, receives)


def scatter_copies(f, t, fsdp_count, grads, firsts, seconds, one_send, one_recv, sends, recvs):
    parity = lax.rem(f, 2)
    partner = f + 1 - 2 * parity
    place = f // 2
    count = fsdp_count // 2

    def first_copies():
        return [
            remote(
                grad.at[:, :, 1 - parity], first, one_send.at[i], one_recv.at[i], partner, t
            )
            for i, (grad, first) in enumerate(zip(grads, firsts))
        ]

    def second_copies(i):
        toward = lax.rem(f + 2 * i, fsdp_count)
        return [
            remote(
                first.at[:, toward // 2],
                second.at[place],
                send.at[toward // 2],
                recv.at[place],
                toward,
                t,
            )
            for first, second, send, recv in zip(firsts, seconds, sends, recvs)
        ]

    def start():
        for handle in first_copies():
            handle.start()

    def add_first():
        for handle in first_copies():
            handle.wait_recv()
        for grad, first in zip(grads, firsts):

            def body(k, carry, grad=grad, first=first):
                i, j = (k // count, lax.rem(k, count))
                mine = grad[i, j, parity].astype(jnp.float32)
                first[i, j] = (mine + first[i, j].astype(jnp.float32)).astype(jnp.bfloat16)
                return carry

            lax.fori_loop(0, grad.shape[0] * count, body, 0)

        def send(i, carry):
            for handle in second_copies(i):
                handle.start()
            return carry

        lax.fori_loop(1, count, send, 0)

    def finish(totals):
        for first, total in zip(firsts, totals):
            total[...] = first[:, place].astype(jnp.float32)

        def body(i, carry):
            source = lax.rem(f + fsdp_count - 2 * i, fsdp_count)
            for first, second, send, recv, total in zip(firsts, seconds, sends, recvs, totals):
                remote(
                    first.at[:, place],
                    second.at[source // 2],
                    send.at[0],
                    recv.at[source // 2],
                    source,
                    t,
                ).wait_recv()
                total[...] += second[source // 2].astype(jnp.float32)
            return carry

        lax.fori_loop(1, count, body, 0)

        def drain(i, carry):
            for handle in second_copies(i):
                handle.wait_send()
            return carry

        lax.fori_loop(1, count, drain, 0)
        for handle in first_copies():
            handle.wait_send()

    return (start, add_first, finish)


def attend_back_kernel(
    fsdp_count,
    tp_count,
    lengths_ref,
    dspread_ref,
    wide_ref,
    pair_ref,
    context_ref,
    mate_grad,
    mixed_ref,
    dproj_ref,
    mate_in,
    mixed_in,
    sums_ref,
    dcontext,
    key_tiles,
    value_tiles,
    turned_tiles,
    totals,
    halo_out,
    halo_in,
    mate_first,
    mate_second,
    mate_total,
    mate_out,
    context_send,
    context_recv,
    mixed_send,
    mixed_recv,
    mate_send,
    mate_recv,
    halo_send,
    halo_recv,
    one_send,
    one_recv,
    two_send,
    two_recv,
):
    f = lax.axis_index("fsdp")
    t = lax.axis_index("tp")
    bf16 = jnp.bfloat16
    f32 = jnp.float32
    rows = dspread_ref.shape[1]
    heads = wide_ref.shape[0]
    group = rows * tp_count
    margin = (pair_ref.shape[0] - group) // 2
    per_half = tp_count // 2
    pair_width = heads * LANES
    scale = 1.0 / math.sqrt(HD)
    greet(fsdp_count, tp_count, f, t)

    def context_copy(j):
        toward = lax.rem(t + j, tp_count)
        return remote(
            dspread_ref.at[toward],
            dcontext.at[t],
            context_send.at[j],
            context_recv.at[t],
            f,
            toward,
        )

    def context_start(j, carry):
        context_copy(j).start()
        return carry

    lax.fori_loop(1, tp_count, context_start, 0)
    start_grads, add_grads, finish_grads = scatter_copies(
        f,
        t,
        fsdp_count,
        (mate_grad,),
        (mate_first,),
        (mate_second,),
        one_send,
        one_recv,
        (two_send,),
        (two_recv,),
    )
    start_grads()
    dcontext[t] = dspread_ref[t]
    mixed_copy = remote(
        mixed_ref, mixed_in, mixed_send, mixed_recv, f, t + 1 - 2 * lax.rem(t, 2)
    )

    def clear(i, carry):
        for head in range(heads):
            totals[head, pl.ds(i * QB, QB), :] = jnp.zeros((QB, LANES), f32)
        return carry

    lax.fori_loop(0, pair_ref.shape[0] // QB, clear, 0)
    add_grads()
    lane = lax.broadcasted_iota(jnp.int32, (rows, LANES), 1)
    tall = lax.broadcasted_iota(jnp.int32, (CLIP, LANES), 1)

    def half(step, carry):
        part = lax.rem(t // per_half + step, 2)
        first, clip = block_clip(f, part, margin)
        length = lengths_ref[clip]
        for head in range(heads):
            pair = pair_ref[pl.ds(first, CLIP), head * LANES : (head + 1) * LANES].astype(f32)
            key_tiles[head] = head_tiles(pair, length).astype(bf16)
            value_tiles[head] = jnp.where(
                tall < HD, jnp.where(tall < 3, 1.0, 0.0), pair
            ).astype(bf16)
            turned_tiles[head] = pair.T.astype(bf16)

        def block(i, inner):
            within = lax.rem(lax.rem(t, per_half) + i, per_half)
            index = part * per_half + within

            @pl.when(index != t)
            def _():
                remote(
                    dspread_ref.at[0],
                    dcontext.at[index],
                    context_send.at[0],
                    context_recv.at[index],
                    f,
                    index,
                ).wait_recv()

            here = pl.ds(pl.multiple_of(index * rows, rows), rows)
            empty = jnp.zeros((rows, HD), f32)

            def two_tiles(ref, at):
                return (
                    ref[at + (slice(0, LANES),)].astype(f32),
                    jnp.concatenate(
                        [ref[at + (slice(LANES, LANES + HD),)].astype(f32), empty], axis=1
                    ),
                )

            upstream = two_tiles(dcontext, (index, slice(None)))
            forward = two_tiles(context_ref, (here,))
            queries = []
            for head in range(heads):
                tile = upstream[head // 2]
                odd = head % 2
                kept = jnp.where((lane >= HD) if odd else (lane < HD), tile * forward[head // 2], 0.0)
                delta = jnp.sum(kept, axis=1, keepdims=True) * scale
                high, middle, low = three_parts(delta)
                grad = (tile if odd else pltpu.roll(tile, HD, axis=1)) * scale
                grad = jnp.where(
                    lane >= HD,
                    grad,
                    jnp.where(
                        lane == 0,
                        -high,
                        jnp.where(lane == 1, -middle, jnp.where(lane == 2, -low, 0.0)),
                    ),
                ).astype(bf16)
                wide = wide_ref[head, here, :]
                probs = jnp.exp(contract_cols(key_tiles[head], wide))
                dscores = (probs * contract_cols(value_tiles[head], grad)).astype(bf16)
                both = jnp.concatenate([dscores, probs.astype(bf16)], axis=1)
                fold = jnp.concatenate(
                    [
                        jnp.where(lane < HD, wide.astype(f32), 0.0),
                        jnp.where(lane < HD, 0.0, grad.astype(f32)),
                    ],
                    axis=0,
                ).astype(bf16)
                totals[head, pl.ds(first, CLIP), :] += jnp.dot(
                    both, fold, preferred_element_type=f32
                )
                queries.append(
                    jnp.dot(turned_tiles[head], dscores, preferred_element_type=f32).T
                )
            dproj_ref[here, pair_width : pair_width + LANES] = jnp.where(
                lane < HD, queries[0], pltpu.roll(queries[1], HD, axis=1)
            ).astype(bf16)
            dproj_ref[here, pair_width + LANES :] = jnp.where(lane < HD, queries[2], 0.0).astype(
                bf16
            )
            return inner

        lax.fori_loop(0, per_half, block, 0)

        @pl.when(step == 0)
        def _():
            mixed_copy.start()

        return carry

    lax.fori_loop(0, 2, half, 0)
    mate_copy = remote(
        mate_out, mate_in, mate_send, mate_recv, f, lax.rem(t + tp_count // 2, tp_count)
    )

    def halo_copy(side, part):
        return remote(
            halo_out.at[side, part],
            halo_in.at[side, part],
            halo_send.at[side, part],
            halo_recv.at[side, part],
            f - 1 if side == 0 else f + 1,
            t,
        )

    halves = group // QB
    for part in range(halves):
        sends, _ = margin_plan(f, fsdp_count, part)
        for side in range(2):

            @pl.when(sends[side])
            def _(side=side, part=part):
                base = (0 if side == 0 else margin + group) + part * QB
                for head in range(heads):
                    halo_out[side, part, head] = totals[head, pl.ds(base, QB), :].astype(bf16)
                halo_copy(side, part).start()

    finish_grads((mate_total,))
    mate_out[...] = mate_total[...].astype(bf16)
    mate_copy.start()

    for part in range(halves):
        _, receives = margin_plan(f, fsdp_count, part)
        here = pl.ds(margin + part * QB, QB)
        for side in range(2):

            @pl.when(receives[side])
            def _(side=side, part=part, here=here):
                halo_copy(side, part).wait_recv()
                for head in range(heads):
                    totals[head, here, :] += halo_in[side, part, head].astype(f32)

        for head in range(heads):
            dproj_ref[part * QB : (part + 1) * QB, head * LANES : (head + 1) * LANES] = (
                totals[head, here, :] * (1.0 / scale)
            ).astype(bf16)

    def add_rows(i, carry):
        return carry + column_sum(dproj_ref[pl.ds(i * rows, rows), :].astype(f32))

    sums_ref[...] = lax.fori_loop(
        0, tp_count, add_rows, jnp.zeros((1, dproj_ref.shape[1]), f32)
    )
    mixed_copy.wait()

    def settle(j, carry):
        context_copy(j).wait_send()
        return carry

    lax.fori_loop(1, tp_count, settle, 0)
    for part in range(halves):
        sends, _ = margin_plan(f, fsdp_count, part)
        for side in range(2):

            @pl.when(sends[side])
            def _(side=side, part=part):
                halo_copy(side, part).wait_send()

    mate_copy.wait()


def attend_back(fsdp_count, tp_count, lengths, dspread, wide, pairs, context, mate_grad, mixed):
    bf16 = jnp.bfloat16
    f32 = jnp.float32
    heads, group, _ = wide.shape
    _, rows, width = dspread.shape
    count = fsdp_count // 2
    kinds, _, _, depth, features = mate_grad.shape
    dma = pltpu.SemaphoreType.DMA
    return pl.pallas_call(
        functools.partial(attend_back_kernel, fsdp_count, tp_count),
        out_shape=(
            jax.ShapeDtypeStruct((group, heads * LANES + 2 * LANES), bf16),
            jax.ShapeDtypeStruct((kinds, depth, features), bf16),
            jax.ShapeDtypeStruct(mixed.shape, bf16),
            jax.ShapeDtypeStruct((1, heads * LANES + 2 * LANES), f32),
        ),
        in_specs=[pl.BlockSpec(memory_space=pltpu.SMEM)] + whole_specs(6),
        out_specs=tuple(whole_specs(4)),
        scratch_shapes=[
            pltpu.VMEM((tp_count, rows, width), bf16),
            pltpu.VMEM((heads, CLIP, LANES), bf16),
            pltpu.VMEM((heads, CLIP, LANES), bf16),
            pltpu.VMEM((heads, LANES, CLIP), bf16),
            pltpu.VMEM((heads, pairs.shape[0], LANES), f32),
            pltpu.VMEM((2, group // QB, heads, QB, LANES), bf16),
            pltpu.VMEM((2, group // QB, heads, QB, LANES), bf16),
            pltpu.VMEM((kinds, count, depth, features), bf16),
            pltpu.VMEM((count, kinds, depth, features), bf16),
            pltpu.VMEM((kinds, depth, features), f32),
            pltpu.VMEM((kinds, depth, features), bf16),
            dma((tp_count,)),
            dma((tp_count,)),
            dma,
            dma,
            dma,
            dma,
            dma((2, group // QB)),
            dma((2, group // QB)),
            dma((1,)),
            dma((1,)),
            dma((count,)),
            dma((count,)),
        ],
        compiler_params=pltpu.CompilerParams(
            collective_id=5, has_side_effects=True, vmem_limit_bytes=VMEM_LIMIT
        ),
        name="attend_back",
    )(lengths, dspread, wide, pairs, context, mate_grad, mixed)


def reduce_copies(f, t, fsdp_count, tp_count, vector, by_fsdp, by_tp, sends, recvs):
    def fsdp_copy(i):
        return remote(
            vector, by_fsdp.at[f], sends.at[i], recvs.at[f], lax.rem(f + i, fsdp_count), t
        )

    def tp_copy(j):
        return remote(
            by_tp.at[t],
            by_tp.at[t],
            sends.at[fsdp_count + j],
            recvs.at[fsdp_count + t],
            f,
            lax.rem(t + j, tp_count),
        )

    def start():
        def body(i, carry):
            fsdp_copy(i).start()
            return carry

        by_fsdp[f] = vector[...]
        lax.fori_loop(1, fsdp_count, body, 0)

    def middle():
        def wait(i, carry):
            source = lax.rem(f + i, fsdp_count)
            remote(
                vector, by_fsdp.at[source], sends.at[i], recvs.at[source], source, t
            ).wait_recv()
            return carry

        def add(i, total):
            return total + by_fsdp[i]

        def body(j, carry):
            tp_copy(j).start()
            return carry

        lax.fori_loop(1, fsdp_count, wait, 0)
        by_tp[t] = lax.fori_loop(0, fsdp_count, add, jnp.zeros(vector.shape, jnp.float32))
        lax.fori_loop(1, tp_count, body, 0)

    def finish():
        def wait(j, carry):
            source = lax.rem(t + j, tp_count)
            remote(
                vector,
                by_tp.at[source],
                sends.at[fsdp_count + j],
                recvs.at[fsdp_count + source],
                f,
                source,
            ).wait_recv()
            tp_copy(j).wait_send()
            return carry

        def drain(i, carry):
            fsdp_copy(i).wait_send()
            return carry

        lax.fori_loop(1, tp_count, wait, 0)
        lax.fori_loop(1, fsdp_count, drain, 0)

    return (start, middle, finish)


def finish_kernel(
    fsdp_count,
    tp_count,
    x_ref,
    gain_ref,
    shift_ref,
    dproj_ref,
    full_ref,
    normed_ref,
    gradient_ref,
    partial_ref,
    mixed_ref,
    own_grad,
    heads_grad,
    mate_ref,
    sums_ref,
    bias_ref,
    proj_ref,
    inputs_grad,
    outputs_ref,
    key_total,
    value_total,
    query_total,
    up_total,
    down_total,
    heads_total,
    gain1_total,
    shift1_total,
    gain2_total,
    shift2_total,
    out_bias_total,
    last_bias_total,
    query_bias_total,
    value_bias_total,
    bias_total,
    weight_grad,
    weight_first,
    weight_second,
    weight_sum,
    weight_total,
    own_first,
    own_second,
    own_total,
    heads_first,
    heads_second,
    heads_sum,
    part_ref,
    row_out,
    row_in,
    heads_out,
    heads_in,
    early,
    early_fsdp,
    early_tp,
    row_send,
    row_recv,
    side_send,
    side_recv,
    one_send,
    one_recv,
    weight_send,
    weight_recv,
    two_send,
    two_recv,
    own_send,
    own_recv,
    three_send,
    three_recv,
    early_send,
    early_recv,
):
    f = lax.axis_index("fsdp")
    t = lax.axis_index("tp")
    bf16 = jnp.bfloat16
    f32 = jnp.float32
    rows, features = x_ref.shape
    proj_width = dproj_ref.shape[1]
    last = tp_count - 1
    sub = rows // 2
    units = bias_ref.shape[3]
    early[0:4, :] = sums_ref[...]
    early[4:5, :] = jnp.zeros((1, features), f32)
    early[4:5, 0:proj_width] = proj_ref[...]
    parts = jnp.concatenate([*three_parts(proj_ref[...]), jnp.zeros((5, proj_width), f32)], axis=0)
    early[7:8, :] = column_sum(contract_cols(parts.astype(bf16), full_ref[0]))
    for level in range(2):
        for c in range(bias_ref.shape[1]):
            early[5 + level : 6 + level, c * units : (c + 1) * units] = bias_ref[level, c]
    greet(fsdp_count, tp_count, f, t)
    start_own, add_own, finish_own = scatter_copies(
        f,
        t,
        fsdp_count,
        (own_grad, heads_grad),
        (own_first, heads_first),
        (own_second, heads_second),
        two_send,
        two_recv,
        (own_send, three_send),
        (own_recv, three_recv),
    )
    start_own()
    start_early, middle_early, finish_early = reduce_copies(
        f, t, fsdp_count, tp_count, early, early_fsdp, early_tp, early_send, early_recv
    )
    start_weights, add_weights, finish_weights = scatter_copies(
        f,
        t,
        fsdp_count,
        (weight_grad,),
        (weight_first,),
        (weight_second,),
        one_send,
        one_recv,
        (weight_send,),
        (weight_recv,),
    )

    def row_copy(piece, side):
        return remote(
            row_out.at[piece],
            row_in.at[side, piece],
            row_send.at[piece],
            row_recv.at[side, piece],
            f,
            t + 1 if side == 0 else t - 1,
        )

    def relay(unit, carry):
        k, low = (unit // 2, lax.rem(unit, 2))
        for side, (block, valid, inner) in enumerate(
            ((last - k, last - k > t, t > 0), (k, k < t, t < last))
        ):
            piece = 2 * block + low
            here = pl.ds(pl.multiple_of(low * sub, sub), sub)

            @pl.when(valid & (inner | (unit >= 2)))
            def _(side=side, block=block, inner=inner, piece=piece, here=here):
                @pl.when(inner)
                def _():
                    row_copy(piece, side).wait_recv()
                    row_out[piece] = (
                        part_ref[block, here, :] + row_in[side, piece].astype(f32)
                    ).astype(bf16)

                @pl.when(jnp.logical_not(inner))
                def _():
                    row_out[piece] = part_ref[block, here, :].astype(bf16)

                @pl.when(unit >= 2)
                def _():
                    row_copy(piece + 2 - 4 * side, side).wait_send()

                row_copy(piece, side).start()

        return carry

    def partial_rows(k, carry):
        block = jnp.where(t < tp_count // 2, last - k, k)
        part_ref[block] = contract_cols(
            dproj_ref[pl.ds(pl.multiple_of(block * rows, rows), rows), :], full_ref[0]
        )
        for side, (first, end) in enumerate(((last, 0), (0, last))):

            @pl.when((k == 0) & (t == end))
            def _(side=side, first=first):
                for low in range(2):
                    row_out[2 * first + low] = part_ref[
                        first, low * sub : (low + 1) * sub, :
                    ].astype(bf16)
                    row_copy(2 * first + low, side).start()

        return carry

    lax.fori_loop(0, tp_count, partial_rows, 0)
    depth = weight_grad.shape[3]
    add_own()
    tall = 256

    for c in range(features // tall):
        columns = slice(c * tall, (c + 1) * tall)
        total = jnp.zeros((tall, proj_width), f32)
        for block in range(tp_count):
            total = total + contract_rows(
                normed_ref[block, :, columns],
                dproj_ref[block * rows : (block + 1) * rows, :],
            )
        weight_sum[columns, :] = total.astype(bf16)
        along = jnp.sum(total * full_ref[0, columns, :].astype(f32), axis=1, keepdims=True)
        early[8:9, columns] = jnp.broadcast_to(along, (tall, LANES)).T[0:1, :]

    start_early()

    def arrange(i, carry):
        weight_grad[0, i // 2, lax.rem(i, 2)] = weight_sum[
            pl.ds(pl.multiple_of(i * depth, 8), depth), :
        ]
        return carry

    lax.fori_loop(0, fsdp_count, arrange, 0)
    start_weights()
    outputs_ref[...] = partial_ref[...] + mixed_ref[...].astype(f32)
    unit, spread, _ = normalize(x_ref[...], row_of(gain_ref), row_of(shift_ref))
    add_weights()

    lax.fori_loop(0, 2 * last, relay, 0)
    middle_early()
    finish_own((own_total, heads_sum))
    heads_out[...] = heads_sum[...].astype(bf16)

    def heads_copy(j):
        toward = lax.rem(t + j, tp_count)
        return remote(
            heads_out.at[toward],
            heads_in.at[t],
            side_send.at[j],
            side_recv.at[t],
            f,
            toward,
        )

    def heads_start(j, carry):
        heads_copy(j).start()
        return carry

    lax.fori_loop(1, tp_count, heads_start, 0)
    finish_weights((weight_total,))
    lane = lax.broadcasted_iota(jnp.int32, (depth, LANES), 1)
    tiles = [weight_total[0, :, j * LANES : (j + 1) * LANES] for j in range(5)]
    turned = [pltpu.roll(tile, HD, axis=1) for tile in tiles[:3]]
    key_total[:, 0:LANES] = jnp.where(lane < HD, tiles[0], turned[1])
    key_total[:, LANES:] = tiles[2][:, :HD]
    value_total[:, 0:LANES] = jnp.where(lane < HD, turned[0], tiles[1])
    value_total[:, LANES:] = turned[2][:, :HD]
    query_total[:, 0:LANES] = tiles[3]
    query_total[:, LANES:] = tiles[4][:, :HD]
    up_total[...] = own_total[0] + mate_ref[0].astype(f32)
    down_total[...] = own_total[1] + mate_ref[1].astype(f32)
    finish_early()
    for row, total in enumerate((gain2_total, shift2_total, out_bias_total, last_bias_total)):
        total[...] = jnp.sum(early_tp[:, row, :], axis=0)
    shift_sum = jnp.sum(early_tp[:, 7, :], axis=0, keepdims=True)
    product = jnp.sum(early_tp[:, 8, :], axis=0, keepdims=True)
    shift1_total[...] = shift_sum.reshape(-1)
    gain1_total[...] = ((product - row_of(shift_ref) * shift_sum) / row_of(gain_ref)).reshape(-1)
    heads = heads_grad.shape[4] // HD

    def piece(head, at, high):
        owner, index = (head // heads, head % heads)
        tile, odd = (index, 1) if at == 0 else (heads + index // 2, index % 2)
        row = early_tp[owner, 4:5, tile * LANES : (tile + 1) * LANES]
        return row if odd == high else swapped(row)

    for at, total in enumerate((value_bias_total, query_bias_total)):
        row = jnp.concatenate(
            [
                joined(piece(2 * i, at, 0), piece(2 * i + 1, at, 1))
                for i in range(tp_count * heads // 2)
            ],
            axis=1,
        )
        total[...] = row.reshape(-1)
    for j in range(tp_count):
        bias_total[j : j + 1, :] = (
            early_tp[j, 5:6, :] + early_tp[(j + tp_count // 2) % tp_count, 6:7, :]
        )

    for side, inner in enumerate((t > 0, t < last)):

        @pl.when(inner)
        def _(side=side):
            for low in range(2):
                row_copy(2 * t + low, side).wait_recv()
                part_ref[t, low * sub : (low + 1) * sub, :] += row_in[side, 2 * t + low].astype(
                    f32
                )

    dnorm = part_ref[t]
    inputs_grad[...] = gradient_ref[...] + norm_back(dnorm, unit, spread, row_of(gain_ref))

    for side, outer in enumerate((t < last, t > 0)):

        @pl.when(outer)
        def _(side=side):
            for low in range(2):
                row_copy(2 * (t + 1 - 2 * side) + low, side).wait_send()

    heads_total[...] = heads_sum[t]

    def heads_done(j, carry):
        source = lax.rem(t + j, tp_count)
        remote(
            heads_out.at[source],
            heads_in.at[source],
            side_send.at[j],
            side_recv.at[source],
            f,
            source,
        ).wait_recv()
        heads_total[...] += heads_in[source].astype(f32)
        heads_copy(j).wait_send()
        return carry

    lax.fori_loop(1, tp_count, heads_done, 0)


def finish(
    fsdp_count,
    tp_count,
    x,
    gain,
    shift,
    dproj,
    full,
    normed,
    gradient,
    partial,
    mixed,
    own_grad,
    heads_grad,
    mate,
    sums,
    bias,
    proj,
):
    bf16 = jnp.bfloat16
    f32 = jnp.float32
    rows, features = x.shape
    kinds = own_grad.shape[0]
    _, _, _, depth, width = heads_grad.shape
    proj_width = dproj.shape[1]
    count = fsdp_count // 2
    dma = pltpu.SemaphoreType.DMA
    peers = fsdp_count + tp_count
    return pl.pallas_call(
        functools.partial(finish_kernel, fsdp_count, tp_count),
        out_shape=(
            jax.ShapeDtypeStruct((rows, features), f32),
            jax.ShapeDtypeStruct((rows, features), f32),
            jax.ShapeDtypeStruct((depth, width), f32),
            jax.ShapeDtypeStruct((depth, width), f32),
            jax.ShapeDtypeStruct((depth, width), f32),
            jax.ShapeDtypeStruct((depth, features), f32),
            jax.ShapeDtypeStruct((depth, features), f32),
            jax.ShapeDtypeStruct((depth, width), f32),
            *[jax.ShapeDtypeStruct((features,), f32)] * 6,
            *[jax.ShapeDtypeStruct((tp_count * width,), f32)] * 2,
            jax.ShapeDtypeStruct((tp_count, features), f32),
        ),
        in_specs=whole_specs(15),
        out_specs=tuple(whole_specs(17)),
        scratch_shapes=[
            pltpu.VMEM((1, count, 2, depth, proj_width), bf16),
            pltpu.VMEM((1, count, depth, proj_width), bf16),
            pltpu.VMEM((count, 1, depth, proj_width), bf16),
            pltpu.VMEM((features, proj_width), bf16),
            pltpu.VMEM((1, depth, proj_width), f32),
            pltpu.VMEM((kinds, count, depth, features), bf16),
            pltpu.VMEM((count, kinds, depth, features), bf16),
            pltpu.VMEM((kinds, depth, features), f32),
            pltpu.VMEM((tp_count, count, depth, width), bf16),
            pltpu.VMEM((count, tp_count, depth, width), bf16),
            pltpu.VMEM((tp_count, depth, width), f32),
            pltpu.VMEM((tp_count, rows, features), f32),
            pltpu.VMEM((2 * tp_count, rows // 2, features), bf16),
            pltpu.VMEM((2, 2 * tp_count, rows // 2, features), bf16),
            pltpu.VMEM((tp_count, depth, width), bf16),
            pltpu.VMEM((tp_count, depth, width), bf16),
            pltpu.VMEM((9, features), f32),
            pltpu.VMEM((fsdp_count, 9, features), f32),
            pltpu.VMEM((tp_count, 9, features), f32),
            dma((2 * tp_count,)),
            dma((2, 2 * tp_count)),
            dma((tp_count,)),
            dma((tp_count,)),
            dma((1,)),
            dma((1,)),
            dma((count,)),
            dma((count,)),
            dma((2,)),
            dma((2,)),
            dma((count,)),
            dma((count,)),
            dma((count,)),
            dma((count,)),
            dma((peers,)),
            dma((peers,)),
        ],
        compiler_params=pltpu.CompilerParams(
            collective_id=6, has_side_effects=True, vmem_limit_bytes=VMEM_LIMIT
        ),
        name="finish",
    )(
        x,
        gain,
        shift,
        dproj,
        full,
        normed,
        gradient,
        partial,
        mixed,
        own_grad,
        heads_grad,
        mate,
        sums,
        bias,
        proj,
    )


def write_kernel(*refs):
    count = len(refs) // 2
    for source, target in zip(refs[:count], refs[count:]):
        target[...] = source[...]


def write_out(*values):
    return pl.pallas_call(
        write_kernel,
        out_shape=tuple(jax.ShapeDtypeStruct(v.shape, v.dtype) for v in values),
        in_specs=whole_specs(len(values)),
        out_specs=tuple(whole_specs(len(values))),
        compiler_params=pltpu.CompilerParams(vmem_limit_bytes=VMEM_LIMIT // 2),
        name="write_out",
    )(*values)


def on_device(
    inputs,
    out_cotangent,
    clip_lengths,
    norm1_gain,
    norm1_shift,
    query_weight,
    query_bias,
    key_weight,
    value_weight,
    value_bias,
    out_weight,
    out_bias,
    norm2_gain,
    norm2_shift,
    fc1_weight,
    fc1_bias,
    fc2_weight,
    fc2_bias,
):
    f32 = jnp.float32
    tp_count = lax.axis_size("tp")
    fsdp_count = lax.axis_size("fsdp")
    margin = CLIP - QB
    heads_here = query_weight.shape[1] // HD
    unit_count = fc1_weight.shape[0]
    query, pairs, normed, attention_w, mlp_w, out_parts, mlp_own = project(
        fsdp_count,
        tp_count,
        inputs,
        norm1_gain,
        norm1_shift,
        (key_weight, value_weight, query_weight),
        (value_bias, query_bias),
        (fc1_weight, fc2_weight),
        out_weight,
        margin,
    )
    spread, context, wide, mlp_other, out_full = attend(
        fsdp_count, tp_count, clip_lengths, query, pairs, mlp_own, out_parts, heads_here
    )
    unit_bias = jnp.swapaxes(fc1_bias.reshape(fsdp_count, tp_count, unit_count), 0, 1)
    (
        dhidden,
        outputs,
        mixed,
        dspread,
        own_grad,
        mate_grad,
        heads_grad,
        bias_part,
        sums,
    ) = by_rows(
        fsdp_count,
        tp_count,
        inputs,
        spread,
        out_full,
        (out_bias, norm2_gain, norm2_shift, fc2_bias),
        unit_bias.reshape(tp_count, -1, 1, 256),
        mlp_w,
        mlp_other,
        out_cotangent,
    )
    count = fsdp_count // 2
    by_owner = lambda grad: grad.reshape(grad.shape[0], count, 2, unit_count, -1)
    dproj, mate_total, mixed, proj_sums = attend_back(
        fsdp_count,
        tp_count,
        clip_lengths,
        dspread,
        wide,
        pairs,
        context,
        by_owner(mate_grad),
        mixed,
    )
    (
        inputs_grad,
        outputs,
        grad_key,
        grad_value,
        grad_query,
        grad_fc1,
        grad_fc2,
        grad_out,
        grad_gain1,
        grad_shift1,
        grad_gain2,
        grad_shift2,
        grad_obias,
        grad_b2,
        grad_qbias,
        grad_vbias,
        bias_total,
    ) = finish(
        fsdp_count,
        tp_count,
        inputs,
        norm1_gain,
        norm1_shift,
        dproj,
        attention_w,
        normed,
        dhidden,
        outputs,
        mixed,
        by_owner(own_grad),
        by_owner(heads_grad),
        mate_total,
        sums,
        bias_part,
        proj_sums,
    )
    grad_b1 = jnp.swapaxes(bias_total.reshape(tp_count, fsdp_count, unit_count), 0, 1).reshape(-1)
    return write_out(
        outputs,
        inputs_grad,
        grad_gain1,
        grad_shift1,
        grad_query,
        grad_qbias,
        grad_key,
        grad_value,
        grad_vbias,
        grad_out,
        grad_obias,
        grad_gain2,
        grad_shift2,
        grad_fc1,
        grad_b1,
        grad_fc2,
        grad_b2,
    )


def solution(mesh):
    in_specs = (
        P(("fsdp", "tp"), None),
        P("fsdp", None),
        P(),
        P(),
        P(),
        P("fsdp", "tp"),
        P(),
        P("fsdp", "tp"),
        P("fsdp", "tp"),
        P(),
        P("fsdp", "tp"),
        P(),
        P(),
        P(),
        P(("fsdp", "tp"), None),
        P(),
        P(("fsdp", "tp"), None),
        P(),
    )
    out_specs = (
        P(("fsdp", "tp"), None),
        P(("fsdp", "tp"), None),
        P(),
        P(),
        P("fsdp", "tp"),
        P(),
        P("fsdp", "tp"),
        P("fsdp", "tp"),
        P(),
        P("fsdp", "tp"),
        P(),
        P(),
        P(),
        P(("fsdp", "tp"), None),
        P(),
        P(("fsdp", "tp"), None),
        P(),
    )
    return jax.shard_map(
        on_device, mesh=mesh, in_specs=in_specs, out_specs=out_specs, check_vma=False
    )
```

```python
import functools
import math

import jax
import jax.numpy as jnp
from jax import lax
from jax.experimental import pallas as pl
from jax.experimental.pallas import tpu as pltpu
from jax.sharding import PartitionSpec as P

HD = 64
CLIP = 1536
QB = 512


eps_norm = 1e-05
root_half = 0.7071067811865476
inv_root_tau = 0.3989422804014327
far_negative = -1e30


def normalize(rows, gain, shift):
    centre = jnp.mean(rows, axis=-1, keepdims=True)
    centred = rows - centre
    inv_spread = lax.rsqrt(jnp.mean(centred * centred, axis=-1, keepdims=True) + eps_norm)
    unit_rows = centred * inv_spread
    return (unit_rows, inv_spread, unit_rows * gain + shift)


def norm_back(upstream, unit_rows, inv_spread, gain):
    scaled = upstream * gain
    return inv_spread * (
        scaled
        - jnp.mean(scaled, axis=-1, keepdims=True)
        - unit_rows * jnp.mean(scaled * unit_rows, axis=-1, keepdims=True)
    )


def contract_rows(left_rows, right_rows):
    return lax.dot_general(
        left_rows, right_rows, (((0,), (0,)), ((), ())), preferred_element_type=jnp.float32
    )


def contract_cols(left_rows, right_rows):
    return lax.dot_general(
        left_rows, right_rows, (((1,), (1,)), ((), ())), preferred_element_type=jnp.float32
    )


MESH = pl.DeviceIdType.MESH
VMEM_LIMIT = 32 * 1024 * 1024
LANES = 128


def row_of(ref):
    return ref[...].reshape(1, -1)


def remote(source, target, send_sem, recv_sem, fsdp_to, tp_to):
    return pltpu.make_async_remote_copy(
        src_ref=source,
        dst_ref=target,
        send_sem=send_sem,
        recv_sem=recv_sem,
        device_id=(fsdp_to, tp_to),
        device_id_type=MESH,
    )


def greet(fsdp_count, tp_count, f, t):
    barrier = pltpu.get_barrier_semaphore()

    def greet_fsdp(i, carry):
        pl.semaphore_signal(
            barrier, inc=1, device_id=(lax.rem(f + i, fsdp_count), t), device_id_type=MESH
        )
        return carry

    def greet_tp(j, carry):
        pl.semaphore_signal(
            barrier, inc=1, device_id=(f, lax.rem(t + j, tp_count)), device_id_type=MESH
        )
        return carry

    lax.fori_loop(1, fsdp_count, greet_fsdp, 0)
    lax.fori_loop(1, tp_count, greet_tp, 0)
    pl.semaphore_wait(barrier, fsdp_count + tp_count - 2)


def gather_copies(f, t, fsdp_count, sources, targets, depth, sends, recvs):
    partner = f + 1 - 2 * lax.rem(f, 2)

    def piece(target, owner):
        return target.at[:, pl.ds(owner * depth, depth)]

    def copies(owner, toward, lane, first):
        return [
            remote(
                source if first else piece(target, owner),
                piece(target, owner),
                send.at[lane],
                recv.at[owner],
                toward,
                t,
            )
            for source, target, send, recv in zip(sources, targets, sends, recvs)
        ]

    def start():
        def body(i, carry):
            for handle in copies(f, lax.rem(f + 2 * i, fsdp_count), i, True):
                handle.start()
            return carry

        lax.fori_loop(1, fsdp_count // 2, body, 0)
        for handle in copies(f, partner, 0, True):
            handle.start()
        for source, target in zip(sources, targets):
            target[:, pl.ds(f * depth, depth), :] = source[...]

    def relay():
        def body(i, carry):
            owner = lax.rem(f + fsdp_count - 2 * i, fsdp_count)
            for handle in copies(owner, partner, fsdp_count // 2 + i, False):
                handle.wait_recv()
                handle.start()
            return carry

        lax.fori_loop(1, fsdp_count // 2, body, 0)

    def finish():
        def body(i, carry):
            owner = lax.rem(partner + 2 * i, fsdp_count)
            for handle in copies(owner, partner, 0, False):
                handle.wait_recv()
            return carry

        lax.fori_loop(0, fsdp_count // 2, body, 0)

    def drain():
        def body(i, carry):
            for handle in copies(f, lax.rem(f + 2 * i, fsdp_count), i, True):
                handle.wait_send()
            for handle in copies(
                lax.rem(f + fsdp_count - 2 * i, fsdp_count),
                partner,
                fsdp_count // 2 + i,
                False,
            ):
                handle.wait_send()
            return carry

        lax.fori_loop(1, fsdp_count // 2, body, 0)
        for handle in copies(f, partner, 0, True):
            handle.wait_send()

    return (start, relay, finish, drain)


def swapped(tile):
    return pltpu.roll(tile, HD, axis=1)


def joined(low, high):
    lane = lax.broadcasted_iota(jnp.int32, low.shape, 1)
    return jnp.where(lane < HD, low, high)


def pack_weights(key_ref, value_ref, query_ref, packed_ref):
    def tiles(ref):
        spare = jnp.zeros((ref.shape[0], HD), jnp.float32)
        return (
            ref[:, :LANES].astype(jnp.float32),
            jnp.concatenate([ref[:, LANES:].astype(jnp.float32), spare], axis=1),
        )

    key, value, query = tiles(key_ref), tiles(value_ref), tiles(query_ref)
    packed = (
        joined(key[0], swapped(value[0])),
        joined(swapped(key[0]), value[0]),
        joined(key[1], swapped(value[1])),
        *query,
    )
    for j, tile in enumerate(packed):
        packed_ref[0, :, j * LANES : (j + 1) * LANES] = tile.astype(jnp.bfloat16)


def pack_bias(t, tp_count, value, query):
    def half(row, head, high):
        tile = row[:, (head // 2) * LANES : (head // 2 + 1) * LANES]
        return tile if head % 2 == high else swapped(tile)

    heads = value.shape[1] // HD // tp_count
    none = jnp.zeros((1, LANES), jnp.float32)
    total = jnp.zeros((1, (heads + 2) * LANES), jnp.float32)
    for j in range(tp_count):
        first = j * heads
        tiles = [joined(none, half(value, first + h, 1)) for h in range(heads)]
        tiles.append(joined(half(query, first, 0), half(query, first + 1, 1)))
        tiles.append(joined(half(query, first + 2, 0), none))
        total = total + jnp.where(t == j, jnp.concatenate(tiles, axis=1), 0.0)
    return total


def project_kernel(
    fsdp_count,
    tp_count,
    x_ref,
    gain_ref,
    shift_ref,
    key_weight,
    value_weight,
    query_weight,
    value_bias,
    query_bias,
    up_ref,
    down_ref,
    out_ref,
    query_ref,
    pair_ref,
    normed_ref,
    full_ref,
    mlp_full,
    heads_ref,
    mlp_ref,
    weight_ref,
    bias_ref,
    side_send,
    side_recv,
    weight_send,
    weight_recv,
    mlp_send,
    mlp_recv,
    row_send,
    row_recv,
    halo_send,
    halo_recv,
):
    f = lax.axis_index("fsdp")
    t = lax.axis_index("tp")
    rows = x_ref.shape[0]
    depth = weight_ref.shape[1]
    group = rows * tp_count
    pair_width = pair_ref.shape[1]
    margin = (pair_ref.shape[0] - group) // 2
    per_half = tp_count // 2
    phase = lax.rem(f, 3)
    above = f + 1 < fsdp_count
    below = f > 0
    blank = jnp.zeros((256, pair_width), jnp.bfloat16)

    def clear(i, carry):
        pair_ref[pl.ds(i * 256, 256), :] = blank
        pair_ref[pl.ds(margin + group + i * 256, 256), :] = blank
        return carry

    lax.fori_loop(0, margin // 256, clear, 0)
    pack_weights(key_weight, value_weight, query_weight, weight_ref)
    mlp_ref[0] = up_ref[...]
    mlp_ref[1] = down_ref[...]
    greet(fsdp_count, tp_count, f, t)
    bias_ref[...] = pack_bias(t, tp_count, row_of(value_bias), row_of(query_bias))
    start_weights, relay_weights, finish_weights, drain_weights = gather_copies(
        f, t, fsdp_count, (weight_ref,), (full_ref,), depth, (weight_send,), (weight_recv,)
    )
    start_mlp, relay_mlp, finish_mlp, drain_mlp = gather_copies(
        f, t, fsdp_count, (mlp_ref,), (mlp_full,), depth, (mlp_send,), (mlp_recv,)
    )
    start_weights()
    _, _, normed = normalize(x_ref[...], row_of(gain_ref), row_of(shift_ref))
    normed_ref[t] = normed.astype(jnp.bfloat16)

    def row_copy(source, lane, toward):
        return remote(
            normed_ref.at[source],
            normed_ref.at[source],
            row_send.at[lane],
            row_recv.at[source],
            f,
            toward,
        )

    @pl.when(t > 0)
    def _():
        row_copy(t, tp_count, t - 1).start()

    @pl.when(t < tp_count - 1)
    def _():
        row_copy(t, tp_count + 1, t + 1).start()

    def heads_copy(j):
        return remote(
            out_ref,
            heads_ref.at[t],
            side_send.at[j],
            side_recv.at[j],
            f,
            lax.rem(t + j, tp_count),
        )

    def heads_start(j, carry):
        heads_copy(j).start()
        return carry

    def heads_done(j, carry):
        heads_copy(j).wait_send()
        source = lax.rem(t + tp_count - j, tp_count)
        remote(
            out_ref, heads_ref.at[source], side_send.at[j], side_recv.at[j], f, source
        ).wait_recv()
        return carry

    heads_ref[t] = out_ref[...]
    lax.fori_loop(1, tp_count, heads_start, 0)
    relay_weights()
    start_mlp()
    finish_weights()

    def halo_copy(source, side):
        return remote(
            pair_ref.at[pl.ds(margin + source * rows, rows)],
            pair_ref.at[pl.ds((0 if side == 0 else margin + group) + source * rows, rows)],
            halo_send.at[side, source],
            halo_recv.at[side, source],
            f + 1 if side == 0 else f - 1,
            t,
        )

    def halo_sends(source):
        late = source >= per_half
        return (
            above & ((phase == 0) | ((phase == 1) & late)),
            below & ((phase == 2) | ((phase == 1) & jnp.logical_not(late))),
        )

    def halo_receives(source):
        late = source >= per_half
        return (
            below & ((phase == 1) | ((phase == 2) & late)),
            above & ((phase == 1) | ((phase == 0) & jnp.logical_not(late))),
        )

    def compute(source):
        out = jnp.dot(normed_ref[source], full_ref[0], preferred_element_type=jnp.float32)
        out = (out + bias_ref[...]).astype(jnp.bfloat16)
        pair_ref[pl.ds(margin + source * rows, rows), :] = out[:, :pair_width]
        for side, needed in enumerate(halo_sends(source)):

            @pl.when(needed)
            def _(side=side):
                halo_copy(source, side).start()

        query_ref[pl.ds(source * rows, rows), :] = out[:, pair_width:]

    compute(t)

    def arrival(k):
        step = k // 2 + 1
        side = 2 * lax.rem(k, 2) - 1
        source = t + side * step
        onward = t - side
        valid = (source >= 0) & (source < tp_count)
        return (source, onward, valid, valid & (onward >= 0) & (onward < tp_count))

    def receive(step, carry):
        for side in range(2):
            source, onward, valid, forward = arrival(2 * step + side)

            @pl.when(valid)
            def _(source=source, onward=onward, forward=forward):
                row_copy(source, 0, t).wait_recv()

                @pl.when(forward)
                def _():
                    row_copy(source, source, onward).start()

        def work(side, inner):
            source, _, valid, _ = arrival(2 * step + side)

            @pl.when(valid)
            def _():
                compute(source)

            return inner

        return lax.fori_loop(0, 2, work, carry)

    lax.fori_loop(0, tp_count - 1, receive, 0)
    relay_mlp()
    lax.fori_loop(1, tp_count, heads_done, 0)

    def sent(k, carry):
        source, onward, valid, forward = arrival(k)

        @pl.when(forward)
        def _():
            row_copy(source, source, onward).wait_send()

        return carry

    lax.fori_loop(0, 2 * (tp_count - 1), sent, 0)

    @pl.when(t > 0)
    def _():
        row_copy(t, tp_count, t - 1).wait_send()

    @pl.when(t < tp_count - 1)
    def _():
        row_copy(t, tp_count + 1, t + 1).wait_send()

    def halo_done(source, carry):
        for side, (sends, receives) in enumerate(zip(halo_sends(source), halo_receives(source))):

            @pl.when(sends)
            def _(side=side):
                halo_copy(source, side).wait_send()

            @pl.when(receives)
            def _(side=side):
                halo_copy(source, side).wait_recv()

        return carry

    lax.fori_loop(0, tp_count, halo_done, 0)
    drain_weights()
    finish_mlp()
    drain_mlp()


def whole_specs(count):
    return [pl.BlockSpec(memory_space=pltpu.VMEM)] * count


def project(fsdp_count, tp_count, x, gain, shift, weights, biases, mlp, out_weight, margin):
    bf16 = jnp.bfloat16
    rows, features = x.shape
    group = rows * tp_count
    depth, width = out_weight.shape
    pair_width = width // HD * LANES
    packed_width = pair_width + 2 * LANES
    dma = pltpu.SemaphoreType.DMA
    return pl.pallas_call(
        functools.partial(project_kernel, fsdp_count, tp_count),
        out_shape=(
            jax.ShapeDtypeStruct((group, 2 * LANES), bf16),
            jax.ShapeDtypeStruct((group + 2 * margin, pair_width), bf16),
            jax.ShapeDtypeStruct((tp_count, rows, features), bf16),
            jax.ShapeDtypeStruct((1, depth * fsdp_count, packed_width), bf16),
            jax.ShapeDtypeStruct((2, depth * fsdp_count, features), bf16),
            jax.ShapeDtypeStruct((tp_count, *out_weight.shape), bf16),
            jax.ShapeDtypeStruct((2, depth, features), bf16),
        ),
        in_specs=whole_specs(11),
        out_specs=tuple(whole_specs(7)),
        scratch_shapes=[
            pltpu.VMEM((1, depth, packed_width), bf16),
            pltpu.VMEM((1, packed_width), jnp.float32),
            dma((tp_count,)),
            dma((tp_count,)),
            dma((fsdp_count,)),
            dma((fsdp_count,)),
            dma((fsdp_count,)),
            dma((fsdp_count,)),
            dma((tp_count + 2,)),
            dma((tp_count,)),
            dma((2, tp_count)),
            dma((2, tp_count)),
        ],
        compiler_params=pltpu.CompilerParams(
            collective_id=1, has_side_effects=True, vmem_limit_bytes=VMEM_LIMIT
        ),
        name="project",
    )(x, gain, shift, *weights, *biases, *mlp, out_weight)


def block_clip(f, part, margin):
    phase = lax.rem(f, 3)
    start = jnp.where(
        phase == 0,
        margin,
        jnp.where(phase == 2, margin - QB, jnp.where(part == 0, 0, margin + QB)),
    )
    return (pl.multiple_of(start, QB), (2 * f + part) // 3)


def head_tiles(pair, length):
    lane = lax.broadcasted_iota(jnp.int32, pair.shape, 1)
    row = lax.broadcasted_iota(jnp.int32, pair.shape, 0)
    extra = jnp.where(
        lane == HD,
        jnp.where(row < length, 0.0, far_negative),
        jnp.where(lane <= HD + 3, 1.0, 0.0),
    )
    return jnp.where(lane < HD, pair, extra)


def spread_heads(rows, head):
    tile = rows[:, (head // 2) * LANES : (head // 2 + 1) * LANES]
    return pltpu.roll(tile, HD, axis=1) if head % 2 else tile


def three_parts(column):
    high = column.astype(jnp.bfloat16).astype(jnp.float32)
    rest = column - high
    middle = rest.astype(jnp.bfloat16).astype(jnp.float32)
    return (high, middle, rest - middle)


def attend_kernel(
    fsdp_count,
    tp_count,
    lengths_ref,
    query_ref,
    pair_ref,
    mlp_ref,
    out_ref,
    spread_ref,
    context_ref,
    wide_ref,
    mlp_full,
    out_full,
    mate_ref,
    key_tiles,
    value_tiles,
    mate_send,
    mate_recv,
    context_send,
    context_recv,
    mlp_send,
    mlp_recv,
    out_send,
    out_recv,
):
    f = lax.axis_index("fsdp")
    t = lax.axis_index("tp")
    bf16 = jnp.bfloat16
    f32 = jnp.float32
    rows = spread_ref.shape[1]
    heads = wide_ref.shape[0]
    group = rows * tp_count
    margin = (pair_ref.shape[0] - group) // 2
    greet(fsdp_count, tp_count, f, t)
    depth = mlp_ref.shape[1]
    start_out, relay_out, finish_out, drain_out = gather_copies(
        f, t, fsdp_count, (out_ref,), (out_full,), depth, (out_send,), (out_recv,)
    )
    mates = [
        remote(
            mlp_ref.at[i],
            mate_ref.at[i],
            mate_send.at[i],
            mate_recv.at[i],
            f,
            lax.rem(t + tp_count // 2, tp_count),
        )
        for i in range(2)
    ]
    gathers = [
        gather_copies(
            f,
            t,
            fsdp_count,
            (mate_ref.at[pl.ds(i, 1)],),
            (mlp_full.at[pl.ds(i, 1)],),
            depth,
            (mlp_send.at[i],),
            (mlp_recv.at[i],),
        )
        for i in range(2)
    ]
    start_out()
    mates[0].start()
    mates[1].start()
    per_half = tp_count // 2

    def context_copy(toward):
        return remote(
            context_ref.at[pl.ds(toward * rows, rows)],
            spread_ref.at[t],
            context_send.at[toward],
            context_recv.at[t],
            f,
            toward,
        )

    lane = lax.broadcasted_iota(jnp.int32, (rows, LANES), 1)
    row = lax.broadcasted_iota(jnp.int32, (LANES, rows), 0)
    tall = lax.broadcasted_iota(jnp.int32, (LANES, CLIP), 0)

    def half(step, carry):
        part = lax.rem(t // per_half + 1 + step, 2)
        first, clip = block_clip(f, part, margin)
        length = lengths_ref[clip]
        for head in range(heads):
            pair = pair_ref[pl.ds(first, CLIP), head * LANES : (head + 1) * LANES].astype(f32)
            key_tiles[head] = head_tiles(pair, length).astype(bf16)
            value_tiles[head] = jnp.where(tall < HD, 1.0, pair.T).astype(bf16)

        def block(i, inner):
            within = lax.rem(lax.rem(t, per_half) + 1 + i, per_half)
            index = part * per_half + within
            here = pl.ds(pl.multiple_of(index * rows, rows), rows)
            query = query_ref[here, :].astype(f32) * (1.0 / math.sqrt(HD))
            parts = []
            for head in range(heads):
                wide = jnp.where(
                    lane < HD, spread_heads(query, head), jnp.where(lane == HD, 1.0, 0.0)
                )
                scores = lax.dot_general(
                    key_tiles[head],
                    wide.astype(bf16),
                    (((1,), (1,)), ((), ())),
                    preferred_element_type=f32,
                )
                highest = jnp.max(scores, axis=0, keepdims=True)
                weights = jnp.exp(scores - highest).astype(bf16)
                summed = jnp.dot(value_tiles[head], weights, preferred_element_type=f32)
                total = summed[0:1, :]
                log_total = highest + jnp.log(total)
                turned = jnp.where(row == 0, log_total, summed * (1.0 / total)).T
                high, middle, low = three_parts(turned[:, 0:1])
                wide_ref[head, here, :] = jnp.where(
                    lane == HD + 1,
                    -high,
                    jnp.where(lane == HD + 2, -middle, jnp.where(lane == HD + 3, -low, wide)),
                ).astype(bf16)
                parts.append(turned)
            context_ref[here, 0:LANES] = jnp.where(
                lane < HD, pltpu.roll(parts[0], HD, axis=1), parts[1]
            ).astype(bf16)
            context_ref[here, LANES : LANES + HD] = pltpu.roll(parts[2], HD, axis=1)[
                :, :HD
            ].astype(bf16)

            @pl.when(index == t)
            def _():
                spread_ref[t] = context_ref[here, :]

            @pl.when(index != t)
            def _():
                context_copy(index).start()

            for turn in range(2):

                @pl.when((step == 0) & (i == turn))
                def _(turn=turn):
                    mates[turn].wait()
                    gathers[turn][0]()

                @pl.when((step == 1) & (i == turn))
                def _(turn=turn):
                    gathers[turn][1]()

            return inner

        lax.fori_loop(0, per_half, block, 0)

        @pl.when(step == 0)
        def _():
            relay_out()

        return carry

    lax.fori_loop(0, 2, half, 0)

    def settle(j, carry):
        toward = lax.rem(t + j, tp_count)
        context_copy(toward).wait_send()
        remote(
            context_ref.at[pl.ds(0, rows)],
            spread_ref.at[toward],
            context_send.at[toward],
            context_recv.at[toward],
            f,
            toward,
        ).wait_recv()
        return carry

    lax.fori_loop(1, tp_count, settle, 0)
    finish_out()
    drain_out()
    for _, _, finish_mlp, drain_mlp in gathers:
        finish_mlp()
        drain_mlp()


def attend(fsdp_count, tp_count, lengths, query, pairs, mlp, out_weights, heads):
    bf16 = jnp.bfloat16
    group = query.shape[0]
    rows = group // tp_count
    width = heads * HD
    dma = pltpu.SemaphoreType.DMA
    depth = mlp.shape[1]
    return pl.pallas_call(
        functools.partial(attend_kernel, fsdp_count, tp_count),
        out_shape=(
            jax.ShapeDtypeStruct((tp_count, rows, width), bf16),
            jax.ShapeDtypeStruct((group, width), bf16),
            jax.ShapeDtypeStruct((heads, group, LANES), bf16),
            jax.ShapeDtypeStruct((mlp.shape[0], depth * fsdp_count, mlp.shape[2]), bf16),
            jax.ShapeDtypeStruct((tp_count, depth * fsdp_count, width), bf16),
        ),
        in_specs=[pl.BlockSpec(memory_space=pltpu.SMEM)] + whole_specs(4),
        out_specs=tuple(whole_specs(5)),
        scratch_shapes=[
            pltpu.VMEM(mlp.shape, bf16),
            pltpu.VMEM((heads, CLIP, LANES), bf16),
            pltpu.VMEM((heads, LANES, CLIP), bf16),
            dma((2,)),
            dma((2,)),
            dma((tp_count,)),
            dma((tp_count,)),
            dma((2, fsdp_count)),
            dma((2, fsdp_count)),
            dma((fsdp_count,)),
            dma((fsdp_count,)),
        ],
        compiler_params=pltpu.CompilerParams(
            collective_id=2, has_side_effects=True, vmem_limit_bytes=VMEM_LIMIT
        ),
        name="attend",
    )(lengths, query, pairs, mlp, out_weights)


def column_sum(rows):
    return jnp.sum(rows, axis=0, keepdims=True)


def rows_kernel(
    fsdp_count,
    tp_count,
    x_ref,
    spread_ref,
    heads_ref,
    out_bias_ref,
    gain_ref,
    shift_ref,
    last_bias_ref,
    bias_ref,
    own_ref,
    mate_ref,
    cotangent_ref,
    gradient_ref,
    outputs_ref,
    mixed_ref,
    context_ref,
    own_grad,
    mate_grad,
    heads_grad,
    bias_grad,
    sums_ref,
    upstream,
    rounded,
    hidden_ref,
    unit_ref,
    normed_ref,
    active_ref,
    slope_ref,
    mixed_sum,
    norm_sum,
    norm_out,
    norm_in,
    load_sem,
    row_send,
    row_recv,
    norm_send,
    norm_recv,
):
    f = lax.axis_index("fsdp")
    t = lax.axis_index("tp")
    bf16 = jnp.bfloat16
    f32 = jnp.float32
    rows = x_ref.shape[0]
    tile = 256
    side = lax.rem(t, 2)
    peer = t + 1 - 2 * side
    load = pltpu.make_async_copy(
        cotangent_ref.at[pl.ds((t - side) * rows, 2 * rows)], upstream, load_sem
    )
    load.start()
    barrier = pltpu.get_barrier_semaphore()
    pl.semaphore_signal(barrier, inc=1, device_id=(f, peer), device_id_type=MESH)
    pl.semaphore_wait(barrier, 1)

    hidden = x_ref[...] + row_of(out_bias_ref)
    for j in range(tp_count):
        hidden = hidden + lax.dot_general(
            spread_ref[j], heads_ref[j], (((1,), (1,)), ((), ())), preferred_element_type=f32
        )
    hidden_ref[...] = hidden
    unit, spread, normed = normalize(hidden, row_of(gain_ref), row_of(shift_ref))
    unit_ref[...] = unit
    normed_ref[side] = normed.astype(bf16)
    sub = rows // 2

    def row_copy(low):
        piece = normed_ref.at[side, pl.ds(pl.multiple_of(low * sub, sub), sub)]
        return remote(piece, piece, row_send.at[low], row_recv.at[low], f, peer)

    row_copy(0).start()
    row_copy(1).start()
    load.wait()

    def rounding(i, carry):
        rounded[pl.ds(i * rows, rows), :] = upstream[pl.ds(i * rows, rows), :].astype(bf16)
        return carry

    lax.fori_loop(0, 2, rounding, 0)
    mixed_sum[...] = jnp.zeros(mixed_sum.shape, f32)
    norm_sum[...] = jnp.zeros(norm_sum.shape, f32)
    chunks = own_ref.shape[1] // tile
    mate = lax.rem(t + tp_count // 2, tp_count)

    def norm_copy(low):
        return remote(
            norm_out.at[low], norm_in.at[low], norm_send.at[low], norm_recv.at[low], f, peer
        )

    def feed_forward(turn, carry):
        which = lax.rem(side + turn // 2, 2)
        low = lax.rem(turn, 2)

        @pl.when(turn >= 2)
        def _():
            row_copy(low).wait_recv()

        within = pl.ds(pl.multiple_of(low * sub, sub), sub)
        here = pl.ds(pl.multiple_of(which * rows + low * sub, sub), sub)
        normed_rows = normed_ref[which, within, :]
        upstream_rows = rounded[here, :]

        for level, (weights, owner) in enumerate(((own_ref, t), (mate_ref, mate))):

            def chunk(c, inner, weights=weights, owner=owner, level=level):
                units = pl.ds(pl.multiple_of(c * tile, tile), tile)
                up = weights[0, units, :]
                down = weights[1, units, :]
                preact = (
                    lax.dot_general(
                        normed_rows, up, (((1,), (1,)), ((), ())), preferred_element_type=f32
                    )
                    + bias_ref[owner, c]
                )
                cdf = 0.5 * (1.0 + lax.erf(preact * root_half))
                active = (preact * cdf).astype(bf16)
                slope = cdf + preact * jnp.exp(-0.5 * preact * preact) * inv_root_tau
                dactive = lax.dot_general(
                    upstream_rows, down, (((1,), (1,)), ((), ())), preferred_element_type=f32
                )
                dpreact = (dactive * slope).astype(bf16)
                active_ref[level, c, here, :] = active
                slope_ref[level, c, here, :] = dpreact
                norm_sum[which, within, :] += jnp.dot(dpreact, up, preferred_element_type=f32)
                mixed_sum[which, within, :] += jnp.dot(active, down, preferred_element_type=f32)
                return inner

            lax.fori_loop(0, chunks, chunk, 0)

        @pl.when(turn >= 2)
        def _():
            norm_out[low] = norm_sum[1 - side, within, :].astype(bf16)
            norm_copy(low).start()

        return carry

    lax.fori_loop(0, 4, feed_forward, 0)
    mixed_ref[...] = mixed_sum[1 - side].astype(bf16)
    outputs_ref[...] = hidden_ref[...] + mixed_sum[side] + row_of(last_bias_ref)

    for level, grad in enumerate((own_grad, mate_grad)):

        def weight_grads(c, carry, level=level, grad=grad):
            units = pl.ds(pl.multiple_of(c * tile, tile), tile)
            slopes = slope_ref[level, c]
            both = jnp.concatenate([normed_ref[0], normed_ref[1]], axis=0)
            grad[0, units, :] = contract_rows(slopes, both).astype(bf16)
            grad[1, units, :] = contract_rows(active_ref[level, c], rounded[...]).astype(bf16)
            bias_grad[level, c] = column_sum(slopes.astype(f32))
            return carry

        lax.fori_loop(0, chunks, weight_grads, 0)

    norm_copy(0).wait()
    norm_copy(1).wait()
    dnorm = norm_sum[side] + jnp.concatenate([norm_in[0], norm_in[1]], axis=0).astype(f32)
    unit = unit_ref[...]
    cotangent = upstream[pl.ds(pl.multiple_of(side * rows, rows), rows), :]
    gradient = cotangent + norm_back(dnorm, unit, spread, row_of(gain_ref))
    gradient_ref[...] = gradient
    sums_ref[0:1, :] = column_sum(dnorm * unit)
    sums_ref[1:2, :] = column_sum(dnorm)
    sums_ref[2:3, :] = column_sum(gradient)
    sums_ref[3:4, :] = column_sum(cotangent)
    gradient = gradient.astype(bf16)
    for j in range(tp_count):
        context_ref[j] = jnp.dot(gradient, heads_ref[j], preferred_element_type=f32).astype(bf16)
        heads_grad[j] = contract_rows(gradient, spread_ref[j]).astype(bf16)
    row_copy(0).wait_send()
    row_copy(1).wait_send()


def by_rows(fsdp_count, tp_count, x, spread, heads, vectors, bias, own, mate, cotangent):
    bf16 = jnp.bfloat16
    f32 = jnp.float32
    rows, features = x.shape
    units = own.shape[1]
    chunks = units // 256
    dma = pltpu.SemaphoreType.DMA
    return pl.pallas_call(
        functools.partial(rows_kernel, fsdp_count, tp_count),
        out_shape=(
            jax.ShapeDtypeStruct((rows, features), f32),
            jax.ShapeDtypeStruct((rows, features), f32),
            jax.ShapeDtypeStruct((rows, features), bf16),
            jax.ShapeDtypeStruct(spread.shape, bf16),
            jax.ShapeDtypeStruct(own.shape, bf16),
            jax.ShapeDtypeStruct(own.shape, bf16),
            jax.ShapeDtypeStruct(heads.shape, bf16),
            jax.ShapeDtypeStruct((2, chunks, 1, 256), f32),
            jax.ShapeDtypeStruct((4, features), f32),
        ),
        in_specs=whole_specs(10) + [pl.BlockSpec(memory_space=pl.ANY)],
        out_specs=tuple(whole_specs(9)),
        scratch_shapes=[
            pltpu.VMEM((2 * rows, features), f32),
            pltpu.VMEM((2 * rows, features), bf16),
            pltpu.VMEM((rows, features), f32),
            pltpu.VMEM((rows, features), f32),
            pltpu.VMEM((2, rows, features), bf16),
            pltpu.VMEM((2, chunks, 2 * rows, 256), bf16),
            pltpu.VMEM((2, chunks, 2 * rows, 256), bf16),
            pltpu.VMEM((2, rows, features), f32),
            pltpu.VMEM((2, rows, features), f32),
            pltpu.VMEM((2, rows // 2, features), bf16),
            pltpu.VMEM((2, rows // 2, features), bf16),
            dma,
            dma((2,)),
            dma((2,)),
            dma((2,)),
            dma((2,)),
        ],
        compiler_params=pltpu.CompilerParams(
            collective_id=4, has_side_effects=True, vmem_limit_bytes=VMEM_LIMIT
        ),
        name="by_rows",
    )(x, spread, heads, *vectors, bias, own, mate, cotangent)


def margin_plan(f, fsdp_count, part):
    phase = lax.rem(f, 3)
    above = f + 1 < fsdp_count
    below = f > 0
    sends = (
        below & ((phase == 1) | ((phase == 2) & (part == 1))),
        above & ((phase == 1) | ((phase == 0) & (part == 0))),
    )
    receives = (
        above & ((phase == 0) | ((phase == 1) & (part == 1))),
        below & ((phase == 2) | ((phase == 1) & (part == 0))),
    )
    return (sends, receives)


def scatter_copies(f, t, fsdp_count, grads, firsts, seconds, one_send, one_recv, sends, recvs):
    parity = lax.rem(f, 2)
    partner = f + 1 - 2 * parity
    place = f // 2
    count = fsdp_count // 2

    def first_copies():
        return [
            remote(
                grad.at[:, :, 1 - parity], first, one_send.at[i], one_recv.at[i], partner, t
            )
            for i, (grad, first) in enumerate(zip(grads, firsts))
        ]

    def second_copies(i):
        toward = lax.rem(f + 2 * i, fsdp_count)
        return [
            remote(
                first.at[:, toward // 2],
                second.at[place],
                send.at[toward // 2],
                recv.at[place],
                toward,
                t,
            )
            for first, second, send, recv in zip(firsts, seconds, sends, recvs)
        ]

    def start():
        for handle in first_copies():
            handle.start()

    def add_first():
        for handle in first_copies():
            handle.wait_recv()
        for grad, first in zip(grads, firsts):

            def body(k, carry, grad=grad, first=first):
                i, j = (k // count, lax.rem(k, count))
                mine = grad[i, j, parity].astype(jnp.float32)
                first[i, j] = (mine + first[i, j].astype(jnp.float32)).astype(jnp.bfloat16)
                return carry

            lax.fori_loop(0, grad.shape[0] * count, body, 0)

        def send(i, carry):
            for handle in second_copies(i):
                handle.start()
            return carry

        lax.fori_loop(1, count, send, 0)

    def finish(totals):
        for first, total in zip(firsts, totals):
            total[...] = first[:, place].astype(jnp.float32)

        def body(i, carry):
            source = lax.rem(f + fsdp_count - 2 * i, fsdp_count)
            for first, second, send, recv, total in zip(firsts, seconds, sends, recvs, totals):
                remote(
                    first.at[:, place],
                    second.at[source // 2],
                    send.at[0],
                    recv.at[source // 2],
                    source,
                    t,
                ).wait_recv()
                total[...] += second[source // 2].astype(jnp.float32)
            return carry

        lax.fori_loop(1, count, body, 0)

        def drain(i, carry):
            for handle in second_copies(i):
                handle.wait_send()
            return carry

        lax.fori_loop(1, count, drain, 0)
        for handle in first_copies():
            handle.wait_send()

    return (start, add_first, finish)


def attend_back_kernel(
    fsdp_count,
    tp_count,
    lengths_ref,
    dspread_ref,
    wide_ref,
    pair_ref,
    context_ref,
    mate_grad,
    mixed_ref,
    dproj_ref,
    mate_in,
    mixed_in,
    sums_ref,
    dcontext,
    key_tiles,
    value_tiles,
    turned_tiles,
    totals,
    halo_out,
    halo_in,
    mate_first,
    mate_second,
    mate_total,
    mate_out,
    context_send,
    context_recv,
    mixed_send,
    mixed_recv,
    mate_send,
    mate_recv,
    halo_send,
    halo_recv,
    one_send,
    one_recv,
    two_send,
    two_recv,
):
    f = lax.axis_index("fsdp")
    t = lax.axis_index("tp")
    bf16 = jnp.bfloat16
    f32 = jnp.float32
    rows = dspread_ref.shape[1]
    heads = wide_ref.shape[0]
    group = rows * tp_count
    margin = (pair_ref.shape[0] - group) // 2
    per_half = tp_count // 2
    pair_width = heads * LANES
    scale = 1.0 / math.sqrt(HD)
    greet(fsdp_count, tp_count, f, t)

    def context_copy(j):
        toward = lax.rem(t + j, tp_count)
        return remote(
            dspread_ref.at[toward],
            dcontext.at[t],
            context_send.at[j],
            context_recv.at[t],
            f,
            toward,
        )

    def context_start(j, carry):
        context_copy(j).start()
        return carry

    lax.fori_loop(1, tp_count, context_start, 0)
    start_grads, add_grads, finish_grads = scatter_copies(
        f,
        t,
        fsdp_count,
        (mate_grad,),
        (mate_first,),
        (mate_second,),
        one_send,
        one_recv,
        (two_send,),
        (two_recv,),
    )
    start_grads()
    dcontext[t] = dspread_ref[t]
    mixed_copy = remote(
        mixed_ref, mixed_in, mixed_send, mixed_recv, f, t + 1 - 2 * lax.rem(t, 2)
    )

    def clear(i, carry):
        for head in range(heads):
            totals[head, pl.ds(i * QB, QB), :] = jnp.zeros((QB, LANES), f32)
        return carry

    lax.fori_loop(0, pair_ref.shape[0] // QB, clear, 0)
    add_grads()
    lane = lax.broadcasted_iota(jnp.int32, (rows, LANES), 1)
    tall = lax.broadcasted_iota(jnp.int32, (CLIP, LANES), 1)

    def half(step, carry):
        part = lax.rem(t // per_half + step, 2)
        first, clip = block_clip(f, part, margin)
        length = lengths_ref[clip]
        for head in range(heads):
            pair = pair_ref[pl.ds(first, CLIP), head * LANES : (head + 1) * LANES].astype(f32)
            key_tiles[head] = head_tiles(pair, length).astype(bf16)
            value_tiles[head] = jnp.where(
                tall < HD, jnp.where(tall < 3, 1.0, 0.0), pair
            ).astype(bf16)
            turned_tiles[head] = pair.T.astype(bf16)

        def block(i, inner):
            within = lax.rem(lax.rem(t, per_half) + i, per_half)
            index = part * per_half + within

            @pl.when(index != t)
            def _():
                remote(
                    dspread_ref.at[0],
                    dcontext.at[index],
                    context_send.at[0],
                    context_recv.at[index],
                    f,
                    index,
                ).wait_recv()

            here = pl.ds(pl.multiple_of(index * rows, rows), rows)
            empty = jnp.zeros((rows, HD), f32)

            def two_tiles(ref, at):
                return (
                    ref[at + (slice(0, LANES),)].astype(f32),
                    jnp.concatenate(
                        [ref[at + (slice(LANES, LANES + HD),)].astype(f32), empty], axis=1
                    ),
                )

            upstream = two_tiles(dcontext, (index, slice(None)))
            forward = two_tiles(context_ref, (here,))
            queries = []
            for head in range(heads):
                tile = upstream[head // 2]
                odd = head % 2
                kept = jnp.where((lane >= HD) if odd else (lane < HD), tile * forward[head // 2], 0.0)
                delta = jnp.sum(kept, axis=1, keepdims=True) * scale
                high, middle, low = three_parts(delta)
                grad = (tile if odd else pltpu.roll(tile, HD, axis=1)) * scale
                grad = jnp.where(
                    lane >= HD,
                    grad,
                    jnp.where(
                        lane == 0,
                        -high,
                        jnp.where(lane == 1, -middle, jnp.where(lane == 2, -low, 0.0)),
                    ),
                ).astype(bf16)
                wide = wide_ref[head, here, :]
                probs = jnp.exp(contract_cols(key_tiles[head], wide))
                dscores = (probs * contract_cols(value_tiles[head], grad)).astype(bf16)
                both = jnp.concatenate([dscores, probs.astype(bf16)], axis=1)
                fold = jnp.concatenate(
                    [
                        jnp.where(lane < HD, wide.astype(f32), 0.0),
                        jnp.where(lane < HD, 0.0, grad.astype(f32)),
                    ],
                    axis=0,
                ).astype(bf16)
                totals[head, pl.ds(first, CLIP), :] += jnp.dot(
                    both, fold, preferred_element_type=f32
                )
                queries.append(
                    jnp.dot(turned_tiles[head], dscores, preferred_element_type=f32).T
                )
            dproj_ref[here, pair_width : pair_width + LANES] = jnp.where(
                lane < HD, queries[0], pltpu.roll(queries[1], HD, axis=1)
            ).astype(bf16)
            dproj_ref[here, pair_width + LANES :] = jnp.where(lane < HD, queries[2], 0.0).astype(
                bf16
            )
            return inner

        lax.fori_loop(0, per_half, block, 0)

        @pl.when(step == 0)
        def _():
            mixed_copy.start()

        return carry

    lax.fori_loop(0, 2, half, 0)
    mate_copy = remote(
        mate_out, mate_in, mate_send, mate_recv, f, lax.rem(t + tp_count // 2, tp_count)
    )

    def halo_copy(side, part):
        return remote(
            halo_out.at[side, part],
            halo_in.at[side, part],
            halo_send.at[side, part],
            halo_recv.at[side, part],
            f - 1 if side == 0 else f + 1,
            t,
        )

    halves = group // QB
    for part in range(halves):
        sends, _ = margin_plan(f, fsdp_count, part)
        for side in range(2):

            @pl.when(sends[side])
            def _(side=side, part=part):
                base = (0 if side == 0 else margin + group) + part * QB
                for head in range(heads):
                    halo_out[side, part, head] = totals[head, pl.ds(base, QB), :].astype(bf16)
                halo_copy(side, part).start()

    finish_grads((mate_total,))
    mate_out[...] = mate_total[...].astype(bf16)
    mate_copy.start()

    for part in range(halves):
        _, receives = margin_plan(f, fsdp_count, part)
        here = pl.ds(margin + part * QB, QB)
        for side in range(2):

            @pl.when(receives[side])
            def _(side=side, part=part, here=here):
                halo_copy(side, part).wait_recv()
                for head in range(heads):
                    totals[head, here, :] += halo_in[side, part, head].astype(f32)

        for head in range(heads):
            dproj_ref[part * QB : (part + 1) * QB, head * LANES : (head + 1) * LANES] = (
                totals[head, here, :] * (1.0 / scale)
            ).astype(bf16)

    def add_rows(i, carry):
        return carry + column_sum(dproj_ref[pl.ds(i * rows, rows), :].astype(f32))

    sums_ref[...] = lax.fori_loop(
        0, tp_count, add_rows, jnp.zeros((1, dproj_ref.shape[1]), f32)
    )
    mixed_copy.wait()

    def settle(j, carry):
        context_copy(j).wait_send()
        return carry

    lax.fori_loop(1, tp_count, settle, 0)
    for part in range(halves):
        sends, _ = margin_plan(f, fsdp_count, part)
        for side in range(2):

            @pl.when(sends[side])
            def _(side=side, part=part):
                halo_copy(side, part).wait_send()

    mate_copy.wait()


def attend_back(fsdp_count, tp_count, lengths, dspread, wide, pairs, context, mate_grad, mixed):
    bf16 = jnp.bfloat16
    f32 = jnp.float32
    heads, group, _ = wide.shape
    _, rows, width = dspread.shape
    count = fsdp_count // 2
    kinds, _, _, depth, features = mate_grad.shape
    dma = pltpu.SemaphoreType.DMA
    return pl.pallas_call(
        functools.partial(attend_back_kernel, fsdp_count, tp_count),
        out_shape=(
            jax.ShapeDtypeStruct((group, heads * LANES + 2 * LANES), bf16),
            jax.ShapeDtypeStruct((kinds, depth, features), bf16),
            jax.ShapeDtypeStruct(mixed.shape, bf16),
            jax.ShapeDtypeStruct((1, heads * LANES + 2 * LANES), f32),
        ),
        in_specs=[pl.BlockSpec(memory_space=pltpu.SMEM)] + whole_specs(6),
        out_specs=tuple(whole_specs(4)),
        scratch_shapes=[
            pltpu.VMEM((tp_count, rows, width), bf16),
            pltpu.VMEM((heads, CLIP, LANES), bf16),
            pltpu.VMEM((heads, CLIP, LANES), bf16),
            pltpu.VMEM((heads, LANES, CLIP), bf16),
            pltpu.VMEM((heads, pairs.shape[0], LANES), f32),
            pltpu.VMEM((2, group // QB, heads, QB, LANES), bf16),
            pltpu.VMEM((2, group // QB, heads, QB, LANES), bf16),
            pltpu.VMEM((kinds, count, depth, features), bf16),
            pltpu.VMEM((count, kinds, depth, features), bf16),
            pltpu.VMEM((kinds, depth, features), f32),
            pltpu.VMEM((kinds, depth, features), bf16),
            dma((tp_count,)),
            dma((tp_count,)),
            dma,
            dma,
            dma,
            dma,
            dma((2, group // QB)),
            dma((2, group // QB)),
            dma((1,)),
            dma((1,)),
            dma((count,)),
            dma((count,)),
        ],
        compiler_params=pltpu.CompilerParams(
            collective_id=5, has_side_effects=True, vmem_limit_bytes=VMEM_LIMIT
        ),
        name="attend_back",
    )(lengths, dspread, wide, pairs, context, mate_grad, mixed)


def reduce_copies(f, t, fsdp_count, tp_count, vector, by_fsdp, by_tp, sends, recvs):
    def fsdp_copy(i):
        return remote(
            vector, by_fsdp.at[f], sends.at[i], recvs.at[f], lax.rem(f + i, fsdp_count), t
        )

    def tp_copy(j):
        return remote(
            by_tp.at[t],
            by_tp.at[t],
            sends.at[fsdp_count + j],
            recvs.at[fsdp_count + t],
            f,
            lax.rem(t + j, tp_count),
        )

    def start():
        def body(i, carry):
            fsdp_copy(i).start()
            return carry

        by_fsdp[f] = vector[...]
        lax.fori_loop(1, fsdp_count, body, 0)

    def middle():
        def wait(i, carry):
            source = lax.rem(f + i, fsdp_count)
            remote(
                vector, by_fsdp.at[source], sends.at[i], recvs.at[source], source, t
            ).wait_recv()
            return carry

        def add(i, total):
            return total + by_fsdp[i]

        def body(j, carry):
            tp_copy(j).start()
            return carry

        lax.fori_loop(1, fsdp_count, wait, 0)
        by_tp[t] = lax.fori_loop(0, fsdp_count, add, jnp.zeros(vector.shape, jnp.float32))
        lax.fori_loop(1, tp_count, body, 0)

    def finish():
        def wait(j, carry):
            source = lax.rem(t + j, tp_count)
            remote(
                vector,
                by_tp.at[source],
                sends.at[fsdp_count + j],
                recvs.at[fsdp_count + source],
                f,
                source,
            ).wait_recv()
            tp_copy(j).wait_send()
            return carry

        def drain(i, carry):
            fsdp_copy(i).wait_send()
            return carry

        lax.fori_loop(1, tp_count, wait, 0)
        lax.fori_loop(1, fsdp_count, drain, 0)

    return (start, middle, finish)


def finish_kernel(
    fsdp_count,
    tp_count,
    x_ref,
    gain_ref,
    shift_ref,
    dproj_ref,
    full_ref,
    normed_ref,
    gradient_ref,
    partial_ref,
    mixed_ref,
    own_grad,
    heads_grad,
    mate_ref,
    sums_ref,
    bias_ref,
    proj_ref,
    inputs_grad,
    outputs_ref,
    key_total,
    value_total,
    query_total,
    up_total,
    down_total,
    heads_total,
    gain1_total,
    shift1_total,
    gain2_total,
    shift2_total,
    out_bias_total,
    last_bias_total,
    query_bias_total,
    value_bias_total,
    bias_total,
    weight_grad,
    weight_first,
    weight_second,
    weight_sum,
    weight_total,
    own_first,
    own_second,
    own_total,
    heads_first,
    heads_second,
    heads_sum,
    part_ref,
    row_out,
    row_in,
    heads_out,
    heads_in,
    early,
    early_fsdp,
    early_tp,
    row_send,
    row_recv,
    side_send,
    side_recv,
    one_send,
    one_recv,
    weight_send,
    weight_recv,
    two_send,
    two_recv,
    own_send,
    own_recv,
    three_send,
    three_recv,
    early_send,
    early_recv,
):
    f = lax.axis_index("fsdp")
    t = lax.axis_index("tp")
    bf16 = jnp.bfloat16
    f32 = jnp.float32
    rows, features = x_ref.shape
    proj_width = dproj_ref.shape[1]
    last = tp_count - 1
    sub = rows // 2
    units = bias_ref.shape[3]
    early[0:4, :] = sums_ref[...]
    early[4:5, :] = jnp.zeros((1, features), f32)
    early[4:5, 0:proj_width] = proj_ref[...]
    parts = jnp.concatenate([*three_parts(proj_ref[...]), jnp.zeros((5, proj_width), f32)], axis=0)
    early[7:8, :] = column_sum(contract_cols(parts.astype(bf16), full_ref[0]))
    for level in range(2):
        for c in range(bias_ref.shape[1]):
            early[5 + level : 6 + level, c * units : (c + 1) * units] = bias_ref[level, c]
    greet(fsdp_count, tp_count, f, t)
    start_own, add_own, finish_own = scatter_copies(
        f,
        t,
        fsdp_count,
        (own_grad, heads_grad),
        (own_first, heads_first),
        (own_second, heads_second),
        two_send,
        two_recv,
        (own_send, three_send),
        (own_recv, three_recv),
    )
    start_own()
    start_early, middle_early, finish_early = reduce_copies(
        f, t, fsdp_count, tp_count, early, early_fsdp, early_tp, early_send, early_recv
    )
    start_weights, add_weights, finish_weights = scatter_copies(
        f,
        t,
        fsdp_count,
        (weight_grad,),
        (weight_first,),
        (weight_second,),
        one_send,
        one_recv,
        (weight_send,),
        (weight_recv,),
    )

    def row_copy(piece, side):
        return remote(
            row_out.at[piece],
            row_in.at[side, piece],
            row_send.at[piece],
            row_recv.at[side, piece],
            f,
            t + 1 if side == 0 else t - 1,
        )

    def relay(unit, carry):
        k, low = (unit // 2, lax.rem(unit, 2))
        for side, (block, valid, inner) in enumerate(
            ((last - k, last - k > t, t > 0), (k, k < t, t < last))
        ):
            piece = 2 * block + low
            here = pl.ds(pl.multiple_of(low * sub, sub), sub)

            @pl.when(valid & (inner | (unit >= 2)))
            def _(side=side, block=block, inner=inner, piece=piece, here=here):
                @pl.when(inner)
                def _():
                    row_copy(piece, side).wait_recv()
                    row_out[piece] = (
                        part_ref[block, here, :] + row_in[side, piece].astype(f32)
                    ).astype(bf16)

                @pl.when(jnp.logical_not(inner))
                def _():
                    row_out[piece] = part_ref[block, here, :].astype(bf16)

                @pl.when(unit >= 2)
                def _():
                    row_copy(piece + 2 - 4 * side, side).wait_send()

                row_copy(piece, side).start()

        return carry

    def partial_rows(k, carry):
        block = jnp.where(t < tp_count // 2, last - k, k)
        part_ref[block] = contract_cols(
            dproj_ref[pl.ds(pl.multiple_of(block * rows, rows), rows), :], full_ref[0]
        )
        for side, (first, end) in enumerate(((last, 0), (0, last))):

            @pl.when((k == 0) & (t == end))
            def _(side=side, first=first):
                for low in range(2):
                    row_out[2 * first + low] = part_ref[
                        first, low * sub : (low + 1) * sub, :
                    ].astype(bf16)
                    row_copy(2 * first + low, side).start()

        return carry

    lax.fori_loop(0, tp_count, partial_rows, 0)
    depth = weight_grad.shape[3]
    tall = 256

    for c in range(features // tall):
        columns = slice(c * tall, (c + 1) * tall)
        total = jnp.zeros((tall, proj_width), f32)
        for block in range(tp_count):
            total = total + contract_rows(
                normed_ref[block, :, columns],
                dproj_ref[block * rows : (block + 1) * rows, :],
            )
        weight_sum[columns, :] = total.astype(bf16)
        along = jnp.sum(total * full_ref[0, columns, :].astype(f32), axis=1, keepdims=True)
        early[8:9, columns] = jnp.broadcast_to(along, (tall, LANES)).T[0:1, :]

    start_early()
    add_own()

    def arrange(i, carry):
        weight_grad[0, i // 2, lax.rem(i, 2)] = weight_sum[
            pl.ds(pl.multiple_of(i * depth, 8), depth), :
        ]
        return carry

    lax.fori_loop(0, fsdp_count, arrange, 0)
    start_weights()
    outputs_ref[...] = partial_ref[...] + mixed_ref[...].astype(f32)
    unit, spread, _ = normalize(x_ref[...], row_of(gain_ref), row_of(shift_ref))
    add_weights()

    lax.fori_loop(0, 2 * last, relay, 0)
    middle_early()
    finish_own((own_total, heads_sum))
    heads_out[...] = heads_sum[...].astype(bf16)

    def heads_copy(j):
        toward = lax.rem(t + j, tp_count)
        return remote(
            heads_out.at[toward],
            heads_in.at[t],
            side_send.at[j],
            side_recv.at[t],
            f,
            toward,
        )

    def heads_start(j, carry):
        heads_copy(j).start()
        return carry

    lax.fori_loop(1, tp_count, heads_start, 0)
    finish_weights((weight_total,))
    lane = lax.broadcasted_iota(jnp.int32, (depth, LANES), 1)
    tiles = [weight_total[0, :, j * LANES : (j + 1) * LANES] for j in range(5)]
    turned = [pltpu.roll(tile, HD, axis=1) for tile in tiles[:3]]
    key_total[:, 0:LANES] = jnp.where(lane < HD, tiles[0], turned[1])
    key_total[:, LANES:] = tiles[2][:, :HD]
    value_total[:, 0:LANES] = jnp.where(lane < HD, turned[0], tiles[1])
    value_total[:, LANES:] = turned[2][:, :HD]
    query_total[:, 0:LANES] = tiles[3]
    query_total[:, LANES:] = tiles[4][:, :HD]
    up_total[...] = own_total[0] + mate_ref[0].astype(f32)
    down_total[...] = own_total[1] + mate_ref[1].astype(f32)
    finish_early()
    for row, total in enumerate((gain2_total, shift2_total, out_bias_total, last_bias_total)):
        total[...] = jnp.sum(early_tp[:, row, :], axis=0)
    shift_sum = jnp.sum(early_tp[:, 7, :], axis=0, keepdims=True)
    product = jnp.sum(early_tp[:, 8, :], axis=0, keepdims=True)
    shift1_total[...] = shift_sum.reshape(-1)
    gain1_total[...] = ((product - row_of(shift_ref) * shift_sum) / row_of(gain_ref)).reshape(-1)
    heads = heads_grad.shape[4] // HD

    def piece(head, at, high):
        owner, index = (head // heads, head % heads)
        tile, odd = (index, 1) if at == 0 else (heads + index // 2, index % 2)
        row = early_tp[owner, 4:5, tile * LANES : (tile + 1) * LANES]
        return row if odd == high else swapped(row)

    for at, total in enumerate((value_bias_total, query_bias_total)):
        row = jnp.concatenate(
            [
                joined(piece(2 * i, at, 0), piece(2 * i + 1, at, 1))
                for i in range(tp_count * heads // 2)
            ],
            axis=1,
        )
        total[...] = row.reshape(-1)
    for j in range(tp_count):
        bias_total[j : j + 1, :] = (
            early_tp[j, 5:6, :] + early_tp[(j + tp_count // 2) % tp_count, 6:7, :]
        )

    for side, inner in enumerate((t > 0, t < last)):

        @pl.when(inner)
        def _(side=side):
            for low in range(2):
                row_copy(2 * t + low, side).wait_recv()
                part_ref[t, low * sub : (low + 1) * sub, :] += row_in[side, 2 * t + low].astype(
                    f32
                )

    dnorm = part_ref[t]
    inputs_grad[...] = gradient_ref[...] + norm_back(dnorm, unit, spread, row_of(gain_ref))

    for side, outer in enumerate((t < last, t > 0)):

        @pl.when(outer)
        def _(side=side):
            for low in range(2):
                row_copy(2 * (t + 1 - 2 * side) + low, side).wait_send()

    heads_total[...] = heads_sum[t]

    def heads_done(j, carry):
        source = lax.rem(t + j, tp_count)
        remote(
            heads_out.at[source],
            heads_in.at[source],
            side_send.at[j],
            side_recv.at[source],
            f,
            source,
        ).wait_recv()
        heads_total[...] += heads_in[source].astype(f32)
        heads_copy(j).wait_send()
        return carry

    lax.fori_loop(1, tp_count, heads_done, 0)


def finish(
    fsdp_count,
    tp_count,
    x,
    gain,
    shift,
    dproj,
    full,
    normed,
    gradient,
    partial,
    mixed,
    own_grad,
    heads_grad,
    mate,
    sums,
    bias,
    proj,
):
    bf16 = jnp.bfloat16
    f32 = jnp.float32
    rows, features = x.shape
    kinds = own_grad.shape[0]
    _, _, _, depth, width = heads_grad.shape
    proj_width = dproj.shape[1]
    count = fsdp_count // 2
    dma = pltpu.SemaphoreType.DMA
    peers = fsdp_count + tp_count
    return pl.pallas_call(
        functools.partial(finish_kernel, fsdp_count, tp_count),
        out_shape=(
            jax.ShapeDtypeStruct((rows, features), f32),
            jax.ShapeDtypeStruct((rows, features), f32),
            jax.ShapeDtypeStruct((depth, width), f32),
            jax.ShapeDtypeStruct((depth, width), f32),
            jax.ShapeDtypeStruct((depth, width), f32),
            jax.ShapeDtypeStruct((depth, features), f32),
            jax.ShapeDtypeStruct((depth, features), f32),
            jax.ShapeDtypeStruct((depth, width), f32),
            *[jax.ShapeDtypeStruct((features,), f32)] * 6,
            *[jax.ShapeDtypeStruct((tp_count * width,), f32)] * 2,
            jax.ShapeDtypeStruct((tp_count, features), f32),
        ),
        in_specs=whole_specs(15),
        out_specs=tuple(whole_specs(17)),
        scratch_shapes=[
            pltpu.VMEM((1, count, 2, depth, proj_width), bf16),
            pltpu.VMEM((1, count, depth, proj_width), bf16),
            pltpu.VMEM((count, 1, depth, proj_width), bf16),
            pltpu.VMEM((features, proj_width), bf16),
            pltpu.VMEM((1, depth, proj_width), f32),
            pltpu.VMEM((kinds, count, depth, features), bf16),
            pltpu.VMEM((count, kinds, depth, features), bf16),
            pltpu.VMEM((kinds, depth, features), f32),
            pltpu.VMEM((tp_count, count, depth, width), bf16),
            pltpu.VMEM((count, tp_count, depth, width), bf16),
            pltpu.VMEM((tp_count, depth, width), f32),
            pltpu.VMEM((tp_count, rows, features), f32),
            pltpu.VMEM((2 * tp_count, rows // 2, features), bf16),
            pltpu.VMEM((2, 2 * tp_count, rows // 2, features), bf16),
            pltpu.VMEM((tp_count, depth, width), bf16),
            pltpu.VMEM((tp_count, depth, width), bf16),
            pltpu.VMEM((9, features), f32),
            pltpu.VMEM((fsdp_count, 9, features), f32),
            pltpu.VMEM((tp_count, 9, features), f32),
            dma((2 * tp_count,)),
            dma((2, 2 * tp_count)),
            dma((tp_count,)),
            dma((tp_count,)),
            dma((1,)),
            dma((1,)),
            dma((count,)),
            dma((count,)),
            dma((2,)),
            dma((2,)),
            dma((count,)),
            dma((count,)),
            dma((count,)),
            dma((count,)),
            dma((peers,)),
            dma((peers,)),
        ],
        compiler_params=pltpu.CompilerParams(
            collective_id=6, has_side_effects=True, vmem_limit_bytes=VMEM_LIMIT
        ),
        name="finish",
    )(
        x,
        gain,
        shift,
        dproj,
        full,
        normed,
        gradient,
        partial,
        mixed,
        own_grad,
        heads_grad,
        mate,
        sums,
        bias,
        proj,
    )


def write_kernel(*refs):
    count = len(refs) // 2
    for source, target in zip(refs[:count], refs[count:]):
        target[...] = source[...]


def write_out(*values):
    return pl.pallas_call(
        write_kernel,
        out_shape=tuple(jax.ShapeDtypeStruct(v.shape, v.dtype) for v in values),
        in_specs=whole_specs(len(values)),
        out_specs=tuple(whole_specs(len(values))),
        compiler_params=pltpu.CompilerParams(vmem_limit_bytes=VMEM_LIMIT // 2),
        name="write_out",
    )(*values)


def on_device(
    inputs,
    out_cotangent,
    clip_lengths,
    norm1_gain,
    norm1_shift,
    query_weight,
    query_bias,
    key_weight,
    value_weight,
    value_bias,
    out_weight,
    out_bias,
    norm2_gain,
    norm2_shift,
    fc1_weight,
    fc1_bias,
    fc2_weight,
    fc2_bias,
):
    f32 = jnp.float32
    tp_count = lax.axis_size("tp")
    fsdp_count = lax.axis_size("fsdp")
    margin = CLIP - QB
    heads_here = query_weight.shape[1] // HD
    unit_count = fc1_weight.shape[0]
    query, pairs, normed, attention_w, mlp_w, out_parts, mlp_own = project(
        fsdp_count,
        tp_count,
        inputs,
        norm1_gain,
        norm1_shift,
        (key_weight, value_weight, query_weight),
        (value_bias, query_bias),
        (fc1_weight, fc2_weight),
        out_weight,
        margin,
    )
    spread, context, wide, mlp_other, out_full = attend(
        fsdp_count, tp_count, clip_lengths, query, pairs, mlp_own, out_parts, heads_here
    )
    unit_bias = jnp.swapaxes(fc1_bias.reshape(fsdp_count, tp_count, unit_count), 0, 1)
    (
        dhidden,
        outputs,
        mixed,
        dspread,
        own_grad,
        mate_grad,
        heads_grad,
        bias_part,
        sums,
    ) = by_rows(
        fsdp_count,
        tp_count,
        inputs,
        spread,
        out_full,
        (out_bias, norm2_gain, norm2_shift, fc2_bias),
        unit_bias.reshape(tp_count, -1, 1, 256),
        mlp_w,
        mlp_other,
        out_cotangent,
    )
    count = fsdp_count // 2
    by_owner = lambda grad: grad.reshape(grad.shape[0], count, 2, unit_count, -1)
    dproj, mate_total, mixed, proj_sums = attend_back(
        fsdp_count,
        tp_count,
        clip_lengths,
        dspread,
        wide,
        pairs,
        context,
        by_owner(mate_grad),
        mixed,
    )
    (
        inputs_grad,
        outputs,
        grad_key,
        grad_value,
        grad_query,
        grad_fc1,
        grad_fc2,
        grad_out,
        grad_gain1,
        grad_shift1,
        grad_gain2,
        grad_shift2,
        grad_obias,
        grad_b2,
        grad_qbias,
        grad_vbias,
        bias_total,
    ) = finish(
        fsdp_count,
        tp_count,
        inputs,
        norm1_gain,
        norm1_shift,
        dproj,
        attention_w,
        normed,
        dhidden,
        outputs,
        mixed,
        by_owner(own_grad),
        by_owner(heads_grad),
        mate_total,
        sums,
        bias_part,
        proj_sums,
    )
    grad_b1 = jnp.swapaxes(bias_total.reshape(tp_count, fsdp_count, unit_count), 0, 1).reshape(-1)
    return write_out(
        outputs,
        inputs_grad,
        grad_gain1,
        grad_shift1,
        grad_query,
        grad_qbias,
        grad_key,
        grad_value,
        grad_vbias,
        grad_out,
        grad_obias,
        grad_gain2,
        grad_shift2,
        grad_fc1,
        grad_b1,
        grad_fc2,
        grad_b2,
    )


def solution(mesh):
    in_specs = (
        P(("fsdp", "tp"), None),
        P("fsdp", None),
        P(),
        P(),
        P(),
        P("fsdp", "tp"),
        P(),
        P("fsdp", "tp"),
        P("fsdp", "tp"),
        P(),
        P("fsdp", "tp"),
        P(),
        P(),
        P(),
        P(("fsdp", "tp"), None),
        P(),
        P(("fsdp", "tp"), None),
        P(),
    )
    out_specs = (
        P(("fsdp", "tp"), None),
        P(("fsdp", "tp"), None),
        P(),
        P(),
        P("fsdp", "tp"),
        P(),
        P("fsdp", "tp"),
        P("fsdp", "tp"),
        P(),
        P("fsdp", "tp"),
        P(),
        P(),
        P(),
        P(("fsdp", "tp"), None),
        P(),
        P(("fsdp", "tp"), None),
        P(),
    )
    return jax.shard_map(
        on_device, mesh=mesh, in_specs=in_specs, out_specs=out_specs, check_vma=False
    )
```
